16 devices in a mesh: dp: 4 (over z, y), cp: 4 (over x, core).
Axes of the slice: x: 2, y: 2, z: 2, core: 2. Of those that a mesh axis runs over, the one named last changes fastest.
Arguments:
- x_in: bfloat16 [4, 2048, 1536], P('dp', 'cp'), parts along dimension 0
- ln_w: bfloat16 [1536], replicated
- ln_b: bfloat16 [1536], replicated
- w_q: bfloat16 [1536, 1536], replicated
- b_q: bfloat16 [1536], replicated
- w_k: bfloat16 [1536, 256], replicated
- b_k: bfloat16 [256], replicated
- w_v: bfloat16 [1536, 256], replicated
- b_v: bfloat16 [256], replicated
- w_o: bfloat16 [1536, 1536], replicated
- b_o: bfloat16 [1536], replicated
- long_factor: float32 [64], replicated
- dy_out: bfloat16 [4, 2048, 1536], P('dp', 'cp'), parts along dimension 0
Outputs:
- output 1: bfloat16 [4, 2048, 1536], P('dp', 'cp'), parts along dimension 0
- output 2: bfloat16 [4, 2048, 1536], P('dp', 'cp'), parts along dimension 0
- output 3: float32 [6144, 1536], P(('dp', 'cp')), parts along dimension 0
- output 4: float32 [6144, 256], P(('dp', 'cp')), parts along dimension 0
- output 5: float32 [6144, 256], P(('dp', 'cp')), parts along dimension 0
- output 6: float32 [6144, 1536], P(('dp', 'cp')), parts along dimension 0
- output 7: float32 [6144], P('dp'), parts along dimension 0
- output 8: float32 [6144], P('dp'), parts along dimension 0
- output 9: float32 [6144], P('dp'), parts along dimension 0
- output 10: float32 [1024], P('dp'), parts along dimension 0
- output 11: float32 [1024], P('dp'), parts along dimension 0
- output 12: float32 [6144], P('dp'), parts along dimension 0
There are 4 independent parts. The reference program is written for one: setup_inputs(seed, part) draws one part's arguments, and reference() takes and returns one part's arrays. A program takes and returns all parts, laid end to end along the dimension named above; an argument that names none is the same for every part.
All inputs are finite; a program needn't handle non-finite values.
Results may differ from the reference program's by a relative error of at most 0.02.
Values are sent between devices in bfloat16 or wider.
A program may use at most 1 GiB of HBM per device.

```python
import math
import jax
import jax.numpy as jnp
from jax import lax

D = 1536
HEADS = 12
KV_HEADS = 2
HEAD = 128
CP = 4
PIECE = 256
ORIG_CTX = 4096
MAX_CTX = 131072
SEQ = 2 * CP * PIECE
Q_WIDTH = HEADS * HEAD
KV_WIDTH = KV_HEADS * HEAD
GROUP_SIZE = HEADS // KV_HEADS
HALF_DIM = HEAD // 2
EPS = 1e-5
THETA = 10000.0
ROPE_SCALE = math.sqrt(1.0 + math.log(MAX_CTX / ORIG_CTX) / math.log(ORIG_CTX))


def setup_inputs(seed: int = 0, part: int = 0) -> dict:
    key = jax.random.key(seed)
    part_key = jax.random.fold_in(key, part)
    key_x, key_dy = jax.random.split(part_key, 2)
    keys = jax.random.split(key, 11)

    def normal(key_index, shape, spread):
        return (spread * jax.random.normal(keys[key_index], shape, jnp.float32)).astype(jnp.bfloat16)

    return {
        'x_in': jax.random.normal(key_x, (1, SEQ, D), jnp.float32).astype(jnp.bfloat16),
        'ln_w': (1.0 + 0.2 * jax.random.normal(keys[0], (D,), jnp.float32)).astype(jnp.bfloat16),
        'ln_b': normal(1, (D,), 0.2),
        'w_q': normal(2, (D, Q_WIDTH), 1.4 * D ** -0.5),
        'b_q': normal(3, (Q_WIDTH,), 0.5),
        'w_k': normal(4, (D, KV_WIDTH), 1.4 * D ** -0.5),
        'b_k': normal(5, (KV_WIDTH,), 1.0),
        'w_v': normal(6, (D, KV_WIDTH), D ** -0.5),
        'b_v': normal(7, (KV_WIDTH,), 0.5),
        'w_o': normal(8, (Q_WIDTH, D), Q_WIDTH ** -0.5),
        'b_o': normal(9, (D,), 0.5),
        'long_factor': jnp.exp(jax.random.uniform(keys[10], (HALF_DIM,), jnp.float32, 0.0, 3.5)),
        'dy_out': jax.random.normal(key_dy, (1, SEQ, D), jnp.float32).astype(jnp.bfloat16),
    }


def seq_positions():
    block_ids = jnp.arange(CP, dtype=jnp.int32)[:, None]
    offsets = jnp.arange(PIECE, dtype=jnp.int32)[None, :]
    both = jnp.concatenate([block_ids * PIECE + offsets, (2 * CP - 1 - block_ids) * PIECE + offsets], axis=1)
    return both.reshape(SEQ)


def rope_tables(positions, long_factor):
    exponent = jnp.arange(HALF_DIM, dtype=jnp.float32) * (1.0 / HALF_DIM)
    inv_freq = 1.0 / (long_factor * THETA ** exponent)
    angle = positions.astype(jnp.float32)[:, None] * inv_freq[None, :]
    return (jnp.cos(angle) * ROPE_SCALE)[:, None, :], (jnp.sin(angle) * ROPE_SCALE)[:, None, :]


def rope_apply(tensor, cos_t, sin_t):
    first = tensor[..., :HALF_DIM]
    second = tensor[..., HALF_DIM:]
    return jnp.concatenate([first * cos_t - second * sin_t, second * cos_t + first * sin_t], axis=-1)


def forward(x_in, ln_w, ln_b, w_q, b_q, w_k, b_k, w_v, b_v, w_o, b_o, long_factor):
    x_f = x_in[0].astype(jnp.float32)
    centered = x_f - jnp.mean(x_f, axis=-1, keepdims=True)
    inv_std = lax.rsqrt(jnp.mean(centered * centered, axis=-1, keepdims=True) + EPS)
    hidden = (centered * inv_std * ln_w + ln_b).astype(jnp.bfloat16).astype(jnp.float32)
    q_proj = (jnp.dot(hidden, w_q) + b_q).astype(jnp.bfloat16)
    k_proj = (jnp.dot(hidden, w_k) + b_k).astype(jnp.bfloat16)
    v_proj = (jnp.dot(hidden, w_v) + b_v).astype(jnp.bfloat16)
    positions = seq_positions()
    cos_t, sin_t = rope_tables(positions, long_factor)
    q_rot = rope_apply(q_proj.astype(jnp.float32).reshape(SEQ, HEADS, HEAD), cos_t, sin_t).astype(jnp.bfloat16)
    k_rot = rope_apply(k_proj.astype(jnp.float32).reshape(SEQ, KV_HEADS, HEAD), cos_t, sin_t).astype(jnp.bfloat16).astype(jnp.float32)
    v_heads = v_proj.reshape(SEQ, KV_HEADS, HEAD).astype(jnp.float32)
    q_blocks = q_rot.reshape(CP, 2 * PIECE, KV_HEADS, GROUP_SIZE, HEAD)
    pos_blocks = positions.reshape(CP, 2 * PIECE)

    def attend(block):
        q_blk, q_pos = block
        scores = jnp.einsum('tkgd,skd->tkgs', q_blk.astype(jnp.float32), k_rot) * (HEAD ** -0.5)
        visible = (positions[None, :] <= q_pos[:, None])[:, None, None, :]
        probs = jax.nn.softmax(jnp.where(visible, scores, -1e30), axis=-1)
        probs = probs.astype(jnp.bfloat16).astype(jnp.float32)
        return jnp.einsum('tkgs,skd->tkgd', probs, v_heads).astype(jnp.bfloat16)

    attn = lax.map(jax.checkpoint(attend), (q_blocks, pos_blocks)).reshape(SEQ, Q_WIDTH)
    z_out = jnp.dot(attn.astype(jnp.float32), w_o) + b_o
    return (x_f + z_out).astype(jnp.bfloat16)[None]


def reference(x_in, ln_w, ln_b, w_q, b_q, w_k, b_k, w_v, b_v, w_o, b_o, long_factor, dy_out):
    params = tuple(p.astype(jnp.float32) for p in (ln_w, ln_b, w_q, b_q, w_k, b_k, w_v, b_v, w_o, b_o))

    def layer_fn(x_val, *weights):
        return forward(x_val, *weights, long_factor)

    y_out, pullback = jax.vjp(layer_fn, x_in, *params)
    grads = pullback(dy_out)
    d_x = grads[0]
    d_lnw, d_lnb, d_wq, d_bq, d_wk, d_bk, d_wv, d_bv, d_wo, d_bo = grads[1:]
    return (y_out, d_x, d_wq, d_wk, d_wv, d_wo, d_lnw, d_lnb, d_bq, d_bk, d_bv, d_bo)
```

```python
import functools
import math
import jax
import jax.numpy as jnp
from jax import lax
from jax.experimental import pallas as pl
from jax.experimental.pallas import tpu as pltpu
from jax.sharding import PartitionSpec as P

EPS = 1e-5
THETA = 10000.0
ROPE_SCALE = math.sqrt(1.0 + math.log(32.0) / math.log(4096.0))
LOG2E = math.log2(math.e)
NEG = -1e30
F32 = jnp.float32
BF16 = jnp.bfloat16


def dot(a, b):
    return lax.dot_general(a, b, (((1,), (0,)), ((), ())), preferred_element_type=F32)


def dot_nt(a, b):
    return lax.dot_general(a, b, (((1,), (1,)), ((), ())), preferred_element_type=F32)


def dot_tn(a, b):
    return lax.dot_general(a, b, (((0,), (0,)), ((), ())), preferred_element_type=F32)


def rope_tables(positions, long_factor):
    half_dim = long_factor.shape[0]
    exponent = jnp.arange(half_dim, dtype=F32) * (1.0 / half_dim)
    inv_freq = 1.0 / (long_factor * THETA ** exponent)
    angle = positions.astype(F32)[:, None] * inv_freq[None, :]
    cos_t = jnp.cos(angle) * ROPE_SCALE
    sin_t = jnp.sin(angle) * ROPE_SCALE
    return jnp.concatenate([cos_t, cos_t], axis=1), jnp.concatenate([-sin_t, sin_t], axis=1)


def params(n, mib=48):
    return pltpu.CompilerParams(dimension_semantics=("arbitrary",) * n, vmem_limit_bytes=mib << 20)


def ln_body(x_ref, w_ref, b_ref, h_ref):
    x = x_ref[...].astype(F32)
    cen = x - jnp.mean(x, axis=-1, keepdims=True)
    inv = lax.rsqrt(jnp.mean(cen * cen, axis=-1, keepdims=True) + EPS)
    h_ref[...] = (cen * inv * w_ref[...].astype(F32) + b_ref[...].astype(F32)).astype(BF16)


def layer_norm(x, w, b, tm=256):
    rows, width = x.shape
    vec = pl.BlockSpec((1, width), lambda i: (0, 0))
    return pl.pallas_call(
        ln_body,
        grid=(rows // tm,),
        in_specs=[pl.BlockSpec((tm, width), lambda i: (i, 0)), vec, vec],
        out_specs=pl.BlockSpec((tm, width), lambda i: (i, 0)),
        out_shape=jax.ShapeDtypeStruct((rows, width), BF16),
        compiler_params=params(1, 24),
        cost_estimate=pl.CostEstimate(flops=rows * width * 12, bytes_accessed=rows * width * 4, transcendentals=0),
        name="ln_rows",
    )(x, w, b)


def qkv_body(nh, hd, c_ref, h_ref, wq_ref, wk_ref, wv_ref, bq_ref, bk_ref, bv_ref, cos_ref, sin_ref, q_ref, k_ref, v_ref):
    h = h_ref[...]
    cos_t = cos_ref[...]
    sin_t = sin_ref[...]

    def rope(t):
        t = t.astype(BF16).astype(F32)
        return (t * cos_t + pltpu.roll(t, hd // 2, 1) * sin_t).astype(BF16)

    k_ref[...] = rope(dot(h, wk_ref[...]) + bk_ref[...].astype(F32))
    v_ref[...] = (dot(h, wv_ref[...]) + bv_ref[...].astype(F32)).astype(BF16)
    qf = dot(h, wq_ref[...]) + bq_ref[...].astype(F32)
    for n in range(nh):
        q_ref[n] = rope(qf[:, n * hd:(n + 1) * hd])


def qkv_proj(core, h, wq, wk, wv, bq, bk, bv, cos_t, sin_t, nh, hd, tm=256):
    rows, width = h.shape
    qw = nh * hd
    row = pl.BlockSpec((tm, hd), lambda i, c: (i, 0))
    grid_spec = pltpu.PrefetchScalarGridSpec(
        num_scalar_prefetch=1,
        grid=(rows // tm,),
        in_specs=[
            pl.BlockSpec((tm, width), lambda i, c: (i, 0)),
            pl.BlockSpec((width, qw), lambda i, c: (0, c[0])),
            pl.BlockSpec((width, hd), lambda i, c: (0, c[0])),
            pl.BlockSpec((width, hd), lambda i, c: (0, c[0])),
            pl.BlockSpec((1, qw), lambda i, c: (0, c[0])),
            pl.BlockSpec((1, hd), lambda i, c: (0, c[0])),
            pl.BlockSpec((1, hd), lambda i, c: (0, c[0])),
            row, row],
        out_specs=[pl.BlockSpec((nh, tm, hd), lambda i, c: (0, i, 0)), row, row])
    return pl.pallas_call(
        functools.partial(qkv_body, nh, hd),
        grid_spec=grid_spec,
        out_shape=[jax.ShapeDtypeStruct((nh, rows, hd), BF16),
                   jax.ShapeDtypeStruct((rows, hd), BF16), jax.ShapeDtypeStruct((rows, hd), BF16)],
        compiler_params=params(1),
        cost_estimate=pl.CostEstimate(flops=2 * rows * width * (qw + 2 * hd), bytes_accessed=8 << 20, transcendentals=0),
        name="qkv_proj",
    )(core, h, wq, wk, wv, bq, bk, bv, cos_t, sin_t)


def do_body(nh, hd, c_ref, d_ref, wo_ref, o_ref):
    r = dot_nt(d_ref[...], wo_ref[...]).astype(BF16)
    for n in range(nh):
        o_ref[n] = r[:, n * hd:(n + 1) * hd]


def do_proj(core, d, wo, nh, hd, tm=256):
    rows, width = d.shape
    qw = nh * hd
    grid_spec = pltpu.PrefetchScalarGridSpec(
        num_scalar_prefetch=1,
        grid=(rows // tm,),
        in_specs=[pl.BlockSpec((tm, width), lambda i, c: (i, 0)),
                  pl.BlockSpec((qw, width), lambda i, c: (c[0], 0))],
        out_specs=pl.BlockSpec((nh, tm, hd), lambda i, c: (0, i, 0)))
    return pl.pallas_call(
        functools.partial(do_body, nh, hd),
        grid_spec=grid_spec,
        out_shape=jax.ShapeDtypeStruct((nh, rows, hd), BF16),
        compiler_params=params(1),
        cost_estimate=pl.CostEstimate(flops=2 * rows * width * qw, bytes_accessed=6 << 20, transcendentals=0),
        name="do_proj",
    )(core, d, wo)


def attn_body(nh, hd, tile, pieces, scale, ids, own, q_ref, do_ref, k_ref, v_ref, cos_ref, sin_ref, dki_ref, dvi_ref,
              o_ref, dq_ref, dk_ref, dv_ref, ks, vs, kt, vt, ps, dps, ms, pb, dsb, ot, dqt):
    step = pl.program_id(0)
    tq = nh * tile
    c = scale * LOG2E

    @pl.when(step == 0)
    def _():
        for s in range(pieces):
            p = ids[s]
            kv = k_ref[s * tile:(s + 1) * tile, :]
            vv = v_ref[s * tile:(s + 1) * tile, :]
            ks[p] = kv
            vs[p] = vv
            kt[p] = kv.T
            vt[p] = vv.T
        dk_ref[...] = dki_ref[...]
        dv_ref[...] = dvi_ref[...]

    i = own[step]

    def first(j, carry, diag):
        m, l, dl = carry
        kj = ks[j]
        vj = vs[j]
        m_new, l_new, d_new = [], [], []
        for n in range(nh):
            lanes = slice(n * tile, (n + 1) * tile)
            s = dot_nt(kj, q_ref[n]) * c
            if diag:
                key = lax.broadcasted_iota(jnp.int32, (tile, tile), 0)
                qry = lax.broadcasted_iota(jnp.int32, (tile, tile), 1)
                s = jnp.where(key <= qry, s, NEG)
            dpb = dot_nt(vj, do_ref[n]).astype(BF16)
            dps[j, :, lanes] = dpb
            mo = m[:, lanes]
            mn = jnp.maximum(mo, jnp.max(s, axis=0, keepdims=True))
            p = jnp.exp2(s - mn)
            ps[j, :, lanes] = p
            al = jnp.exp2(mo - mn)
            m_new.append(mn)
            l_new.append(l[:, lanes] * al + jnp.sum(p, axis=0, keepdims=True))
            d_new.append(dl[:, lanes] * al + jnp.sum(p * dpb.astype(F32), axis=0, keepdims=True))
        m = jnp.concatenate(m_new, axis=1)
        ms[j] = m
        return m, jnp.concatenate(l_new, axis=1), jnp.concatenate(d_new, axis=1)

    init = (jnp.full((1, tq), NEG, F32), jnp.zeros((1, tq), F32), jnp.zeros((1, tq), F32))
    carry = lax.fori_loop(0, i, lambda j, cr: first(j, cr, False), init)
    m, l, dl = first(i, carry, True)
    inv = 1.0 / l
    delta = dl * inv
    ot[...] = jnp.zeros_like(ot)
    dqt[...] = jnp.zeros_like(dqt)

    def second(j, carry):
        f = jnp.exp2(ms[j] - m) * inv
        for n in range(nh):
            lanes = slice(n * tile, (n + 1) * tile)
            p = ps[j, :, lanes] * f[:, lanes]
            pb[:, lanes] = p.astype(BF16)
            dsb[:, lanes] = (p * (dps[j, :, lanes].astype(F32) - delta[:, lanes])).astype(BF16)
        ot[...] += dot(vt[j], pb[...])
        dqt[...] += dot(kt[j], dsb[...])
        dv_ref[j] += dot(pb[...], do_ref[...].reshape(tq, hd))
        dk_ref[j] += dot(dsb[...], q_ref[...].reshape(tq, hd))
        return carry

    lax.fori_loop(0, i + 1, second, 0)
    cos_t = cos_ref[...]
    sin_t = sin_ref[...]
    for n in range(nh):
        lanes = slice(n * tile, (n + 1) * tile)
        cols = slice(n * hd, (n + 1) * hd)
        o_ref[:, cols] = ot[:, lanes].T.astype(BF16)
        g = (dqt[:, lanes].T * scale).astype(BF16).astype(F32)
        dq_ref[:, cols] = (g * cos_t - pltpu.roll(g, hd // 2, 1) * sin_t).astype(BF16)


def attention(ids, own, q, do, k, v, cos_t, sin_t, dk, dv, scale, tile):
    nh, rows, hd = q.shape
    pieces = k.shape[0] // tile
    whole = k.shape[0]
    tq = nh * tile
    full2 = pl.BlockSpec((whole, hd), lambda i, a, b: (0, 0))
    acc = pl.BlockSpec((pieces, tile, hd), lambda i, a, b: (0, 0, 0))
    heads = pl.BlockSpec((nh, tile, hd), lambda i, a, b: (0, i, 0))
    table = pl.BlockSpec((tile, hd), lambda i, a, b: (i, 0))
    out = pl.BlockSpec((tile, nh * hd), lambda i, a, b: (i, 0))
    grid_spec = pltpu.PrefetchScalarGridSpec(
        num_scalar_prefetch=2,
        grid=(rows // tile,),
        in_specs=[heads, heads, full2, full2, table, table, acc, acc],
        out_specs=[out, out, acc, acc],
        scratch_shapes=[
            pltpu.VMEM((pieces, tile, hd), BF16), pltpu.VMEM((pieces, tile, hd), BF16),
            pltpu.VMEM((pieces, hd, tile), BF16), pltpu.VMEM((pieces, hd, tile), BF16),
            pltpu.VMEM((pieces, tile, tq), F32), pltpu.VMEM((pieces, tile, tq), BF16),
            pltpu.VMEM((pieces, 1, tq), F32),
            pltpu.VMEM((tile, tq), BF16), pltpu.VMEM((tile, tq), BF16),
            pltpu.VMEM((hd, tq), F32), pltpu.VMEM((hd, tq), F32)])
    return pl.pallas_call(
        functools.partial(attn_body, nh, hd, tile, pieces, scale),
        grid_spec=grid_spec,
        out_shape=[jax.ShapeDtypeStruct((rows, nh * hd), BF16), jax.ShapeDtypeStruct((rows, nh * hd), BF16),
                   jax.ShapeDtypeStruct((pieces, tile, hd), F32), jax.ShapeDtypeStruct((pieces, tile, hd), F32)],
        compiler_params=params(1),
        cost_estimate=pl.CostEstimate(flops=rows * whole * nh * hd * 12, bytes_accessed=8 << 20,
                                      transcendentals=rows * whole * nh),
        name="attn_fwd_bwd",
    )(ids, own, q, do, k, v, cos_t, sin_t, dk, dv)


def solution(mesh):
    groups = mesh.shape['cp']
    row_spec = P('dp', 'cp', None)
    mat_spec = P(('dp', 'cp'), None)
    vec_spec = P('dp')
    near = [(i, i ^ 1) for i in range(groups)]
    far = [(i, i ^ 2) for i in range(groups)]

    def swap(v):
        return lax.ppermute(v, 'cp', near)

    def cross(v):
        return lax.ppermute(v, 'cp', far)

    def device_fn(x_in, ln_w, ln_b, w_q, b_q, w_k, b_k, w_v, b_v, w_o, b_o, long_factor, dy_out):
        rank = lax.axis_index('cp')
        core = rank % 2
        chip = rank // 2
        x_rows = x_in[0]
        d0 = dy_out[0]
        tokens, width = x_rows.shape
        piece = tokens // 2
        hd = 2 * long_factor.shape[0]
        kv_heads = w_k.shape[1] // hd
        nh = w_q.shape[1] // hd // kv_heads
        qw = nh * hd
        scale = hd ** -0.5
        core_v = jnp.reshape(core, (1,)).astype(jnp.int32)

        h0 = layer_norm(x_rows, ln_w[None], ln_b[None])
        h2 = cross(h0)
        d2 = cross(d0)
        h1 = swap(h0)
        d1 = swap(d0)
        h3 = swap(h2)
        d3 = swap(d2)

        blocks = jnp.stack([rank, rank ^ 1, rank ^ 2, rank ^ 3]).astype(jnp.int32)
        ids = jnp.stack([blocks, 2 * groups - 1 - blocks], axis=1).reshape(2 * groups)
        pos = (ids[:, None] * piece + jnp.arange(piece, dtype=jnp.int32)[None, :]).reshape(2 * groups * piece)
        cos_t, sin_t = rope_tables(pos, long_factor)
        half = 2 * tokens

        def project(h, t):
            return qkv_proj(core_v, h, w_q, w_k, w_v, b_q[None], b_k[None], b_v[None], cos_t[t], sin_t[t], nh, hd)

        lo = slice(0, half)
        hi = slice(half, 2 * half)
        h01 = jnp.concatenate([h0, h1], axis=0)
        d01 = jnp.concatenate([d0, d1], axis=0)
        h23 = jnp.concatenate([h2, h3], axis=0)
        d23 = jnp.concatenate([d2, d3], axis=0)
        q01, k01, v01 = project(h01, lo)
        do01 = do_proj(core_v, d01, w_o, nh, hd)
        q23, k23, v23 = project(h23, hi)
        k_all = jnp.concatenate([k01, k23], axis=0)
        v_all = jnp.concatenate([v01, v23], axis=0)
        zero = jnp.zeros((2 * groups, piece, hd), F32)
        o01, dq01, dk_a, dv_a = attention(ids, ids[:4], q01, do01, k_all, v_all, cos_t[lo], sin_t[lo], zero, zero, scale, piece)
        do23 = do_proj(core_v, d23, w_o, nh, hd)
        o23, dq23, dk_s, dv_s = attention(ids, ids[4:], q23, do23, k_all, v_all, cos_t[hi], sin_t[hi], dk_a, dv_a, scale, piece)

        both = jnp.stack([o01[tokens:], dq01[tokens:]])
        other = swap(both)
        first = core == 0

        def by_head(mine, theirs):
            return jnp.where(first, jnp.concatenate([mine, theirs], axis=1), jnp.concatenate([theirs, mine], axis=1))

        attn_rows = by_head(o01[:tokens], other[0])
        dq_rows = by_head(dq01[:tokens], other[1])
        y_rows = (x_rows.astype(F32) + dot(attn_rows, w_o) + b_o.astype(F32)).astype(BF16)

        dk_r = jnp.take(dk_s, ids, axis=0).reshape(2 * half, hd) * scale
        dv_r = jnp.take(dv_s, ids, axis=0).reshape(2 * half, hd)
        dk_r = dk_r.astype(BF16).astype(F32)
        dk_b = (dk_r * cos_t - jnp.roll(dk_r, hd // 2, axis=1) * sin_t).astype(BF16)
        dv_b = dv_r.astype(BF16)
        dkv_b = jnp.concatenate([dk_b, dv_b], axis=1)
        dkv_o = swap(dkv_b[tokens:half])
        dkv_m = dkv_b[:tokens]
        dk_rows = by_head(dkv_m[:, :hd], dkv_o[:, :hd])
        dv_rows = by_head(dkv_m[:, hd:], dkv_o[:, hd:])

        d_hid = (dot_nt(dq_rows, w_q) + dot_nt(dk_rows, w_k) + dot_nt(dv_rows, w_v)).astype(BF16).astype(F32)
        x_f = x_rows.astype(F32)
        cen = x_f - jnp.mean(x_f, axis=-1, keepdims=True)
        inv_std = lax.rsqrt(jnp.mean(cen * cen, axis=-1, keepdims=True) + EPS)
        x_hat = cen * inv_std
        a6 = d_hid * ln_w.astype(F32)
        d_x = inv_std * (a6 - jnp.mean(a6, axis=-1, keepdims=True) - x_hat * jnp.mean(a6 * x_hat, axis=-1, keepdims=True))
        dx_rows = (d0.astype(F32) + d_x).astype(BF16)

        h_cols = jnp.concatenate([lax.dynamic_slice(h, (0, chip * (width // 2)), (half, width // 2)) for h in (h01, h23)], axis=0)
        dqkv = jnp.concatenate([jnp.concatenate([dq01, dq23], axis=0), dkv_b], axis=1)
        d_w = dot_tn(h_cols, dqkv)
        part = width // groups
        mine = lax.dynamic_slice(d_w, (core * part, 0), (part, qw + 2 * hd))
        theirs = swap(lax.dynamic_slice(d_w, ((1 - core) * part, 0), (part, qw + 2 * hd)))
        d_wq = by_head(mine[:, :qw], theirs[:, :qw])
        d_wk = by_head(mine[:, qw:qw + hd], theirs[:, qw:qw + hd])
        d_wv = by_head(mine[:, qw + hd:], theirs[:, qw + hd:])

        o_all = jnp.concatenate([o01, o23], axis=0)
        o_mine = lax.dynamic_slice(o_all, (0, core * part), (2 * half, part))
        o_send = lax.dynamic_slice(o_all, (0, (1 - core) * part), (2 * half, part)).reshape(2, 2, tokens, part)
        o_got = swap(o_send[:, ::-1].reshape(2 * half, part))
        o_cols = jnp.where(core == chip, o_mine, o_got)
        d_wo = dot_tn(o_cols, jnp.concatenate([d01, d23], axis=0))

        sums = jnp.concatenate([jnp.sum(dq01.astype(F32), axis=0), jnp.sum(dkv_b[:half].astype(F32), axis=0)])
        gap = jnp.zeros_like(sums)
        sums = jnp.where(first, jnp.stack([sums, gap]), jnp.stack([gap, sums])).reshape(-1)
        vec = jnp.concatenate([jnp.sum(d_hid * x_hat, axis=0), jnp.sum(d_hid, axis=0), jnp.sum(d0.astype(F32), axis=0), sums])
        vec = vec + swap(vec)
        vec = vec + cross(vec)
        d_lnw = vec[:width]
        d_lnb = vec[width:2 * width]
        d_bo = vec[2 * width:3 * width]
        per = vec[3 * width:].reshape(kv_heads, qw + 2 * hd)
        d_bq = per[:, :qw].reshape(-1)
        d_bk = per[:, qw:qw + hd].reshape(-1)
        d_bv = per[:, qw + hd:].reshape(-1)
        return (y_rows[None], dx_rows[None], d_wq, d_wk, d_wv, d_wo, d_lnw, d_lnb, d_bq, d_bk, d_bv, d_bo)

    in_specs = (row_spec,) + (P(),) * 11 + (row_spec,)
    out_specs = (row_spec, row_spec) + (mat_spec,) * 4 + (vec_spec,) * 6
    return jax.shard_map(device_fn, mesh=mesh, in_specs=in_specs, out_specs=out_specs, check_vma=False)
```

```python
import functools
import math
import jax
import jax.numpy as jnp
from jax import lax
from jax.experimental import pallas as pl
from jax.experimental.pallas import tpu as pltpu
from jax.sharding import PartitionSpec as P


EPS = 1e-5
THETA = 10000.0
ROPE_SCALE = math.sqrt(1.0 + math.log(32.0) / math.log(4096.0))
LOG2E = math.log2(math.e)
NEG = -1e30
F32 = jnp.float32
BF16 = jnp.bfloat16


def dot(a, b):
    return lax.dot_general(a, b, (((1,), (0,)), ((), ())), preferred_element_type=F32)


def dot_nt(a, b):
    return lax.dot_general(a, b, (((1,), (1,)), ((), ())), preferred_element_type=F32)


def dot_tn(a, b):
    return lax.dot_general(a, b, (((0,), (0,)), ((), ())), preferred_element_type=F32)


def rope_tables(positions, long_factor):
    half_dim = long_factor.shape[0]
    exponent = jnp.arange(half_dim, dtype=F32) * (1.0 / half_dim)
    inv_freq = 1.0 / (long_factor * THETA ** exponent)
    angle = positions.astype(F32)[:, None] * inv_freq[None, :]
    cos_t = jnp.cos(angle) * ROPE_SCALE
    sin_t = jnp.sin(angle) * ROPE_SCALE
    return jnp.concatenate([cos_t, cos_t], axis=1), jnp.concatenate([-sin_t, sin_t], axis=1)


def params(n, mib=48):
    return pltpu.CompilerParams(dimension_semantics=("arbitrary",) * n, vmem_limit_bytes=mib << 20)


def ln_body(x_ref, w_ref, b_ref, ha_ref, hb_ref):
    x = x_ref[...].astype(F32)
    cen = x - jnp.mean(x, axis=-1, keepdims=True)
    inv = lax.rsqrt(jnp.mean(cen * cen, axis=-1, keepdims=True) + EPS)
    h = (cen * inv * w_ref[...].astype(F32) + b_ref[...].astype(F32)).astype(BF16)

    @pl.when(pl.program_id(0) == 0)
    def _():
        ha_ref[...] = h

    @pl.when(pl.program_id(0) == 1)
    def _():
        hb_ref[...] = h


def layer_norm(x, w, b):
    rows, width = x.shape
    tm = rows // 2
    vec = pl.BlockSpec((1, width), lambda i: (0, 0))
    half = pl.BlockSpec((tm, width), lambda i: (0, 0))
    return pl.pallas_call(
        ln_body,
        grid=(2,),
        in_specs=[pl.BlockSpec((tm, width), lambda i: (i, 0)), vec, vec],
        out_specs=[half, half],
        out_shape=[jax.ShapeDtypeStruct((tm, width), BF16)] * 2,
        compiler_params=params(1, 24),
        cost_estimate=pl.CostEstimate(flops=rows * width * 12, bytes_accessed=rows * width * 4, transcendentals=0),
        name="ln_rows",
    )(x, w, b)


def qkv_body(nh, hd, n_src, c_ref, t_ref, *refs):
    h_refs = refs[:n_src]
    wq_ref, wk_ref, wv_ref, bq_ref, bk_ref, bv_ref, cos_ref, sin_ref, q_ref, kv_ref = refs[n_src:]
    step = pl.program_id(0)
    h = h_refs[0][...]
    for n in range(1, n_src):
        h = jnp.where(step == n, h_refs[n][...], h)
    cos_t = cos_ref[...]
    sin_t = sin_ref[...]

    def rope(t):
        t = t.astype(BF16).astype(F32)
        return (t * cos_t + pltpu.roll(t, hd // 2, 1) * sin_t).astype(BF16)

    kv_ref[:, :hd] = rope(dot(h, wk_ref[...]) + bk_ref[...].astype(F32))
    kv_ref[:, hd:] = (dot(h, wv_ref[...]) + bv_ref[...].astype(F32)).astype(BF16)
    qf = dot(h, wq_ref[...]) + bq_ref[...].astype(F32)
    for n in range(nh):
        q_ref[n] = rope(qf[:, n * hd:(n + 1) * hd])


def qkv_proj(core, tids, hs, wq, wk, wv, bq, bk, bv, cos_t, sin_t, nh, hd):
    tm, width = hs[0].shape
    n_src = len(hs)
    rows = tm * n_src
    qw = nh * hd
    table = pl.BlockSpec((tm, hd), lambda i, c, t: (t[i], 0))
    grid_spec = pltpu.PrefetchScalarGridSpec(
        num_scalar_prefetch=2,
        grid=(n_src,),
        in_specs=[pl.BlockSpec((tm, width), lambda i, c, t: (0, 0))] * n_src + [
            pl.BlockSpec((width, qw), lambda i, c, t: (0, c[0])),
            pl.BlockSpec((width, hd), lambda i, c, t: (0, c[0])),
            pl.BlockSpec((width, hd), lambda i, c, t: (0, c[0])),
            pl.BlockSpec((1, qw), lambda i, c, t: (0, c[0])),
            pl.BlockSpec((1, hd), lambda i, c, t: (0, c[0])),
            pl.BlockSpec((1, hd), lambda i, c, t: (0, c[0])),
            table, table],
        out_specs=[pl.BlockSpec((nh, tm, hd), lambda i, c, t: (0, i, 0)),
                   pl.BlockSpec((tm, 2 * hd), lambda i, c, t: (i, 0))])
    return pl.pallas_call(
        functools.partial(qkv_body, nh, hd, n_src),
        grid_spec=grid_spec,
        out_shape=[jax.ShapeDtypeStruct((nh, rows, hd), BF16), jax.ShapeDtypeStruct((rows, 2 * hd), BF16)],
        compiler_params=params(1),
        cost_estimate=pl.CostEstimate(flops=2 * rows * width * (qw + 2 * hd), bytes_accessed=8 << 20, transcendentals=0),
        name="qkv_proj",
    )(core, tids, *hs, wq, wk, wv, bq, bk, bv, cos_t, sin_t)


def do_body(nh, hd, n_src, c_ref, *refs):
    d_refs = refs[:n_src]
    wo_ref, o_ref = refs[n_src:]
    d = d_refs[0][...]
    for n in range(1, n_src):
        d = jnp.where(pl.program_id(0) // (pl.num_programs(0) // n_src) == n, d_refs[n][...], d)
    r = dot_nt(d, wo_ref[...]).astype(BF16)
    for n in range(nh):
        o_ref[n] = r[:, n * hd:(n + 1) * hd]


def do_proj(core, ds, wo, nh, hd, tm):
    rows, width = ds[0].shape
    n_src = len(ds)
    per = rows // tm
    qw = nh * hd

    def src(n):
        return pl.BlockSpec((tm, width), lambda i, c: (jnp.clip(i - n * per, 0, per - 1), 0))

    grid_spec = pltpu.PrefetchScalarGridSpec(
        num_scalar_prefetch=1,
        grid=(n_src * per,),
        in_specs=[src(n) for n in range(n_src)] + [pl.BlockSpec((qw, width), lambda i, c: (c[0], 0))],
        out_specs=pl.BlockSpec((nh, tm, hd), lambda i, c: (0, i, 0)))
    return pl.pallas_call(
        functools.partial(do_body, nh, hd, n_src),
        grid_spec=grid_spec,
        out_shape=jax.ShapeDtypeStruct((nh, n_src * rows, hd), BF16),
        compiler_params=params(1),
        cost_estimate=pl.CostEstimate(flops=2 * n_src * rows * width * qw, bytes_accessed=6 << 20, transcendentals=0),
        name="do_proj",
    )(core, *ds, wo)


def prep_body(hd, tile, n_src, ids, *refs):
    kv_refs = refs[:n_src]
    ks, vs, kt, vt = refs[n_src:]
    s = 0
    for ref in kv_refs:
        for r in range(ref.shape[0] // tile):
            p = ids[s]
            k = ref[r * tile:(r + 1) * tile, :hd]
            v = ref[r * tile:(r + 1) * tile, hd:]
            ks[p] = k
            vs[p] = v
            kt[p] = k.T
            vt[p] = v.T
            s += 1


def kv_prep(ids, kvs, hd, tile):
    pieces = sum(a.shape[0] for a in kvs) // tile
    whole = lambda shape: pl.BlockSpec(shape, lambda i, a: (0,) * len(shape))
    out = [(pieces, tile, hd)] * 2 + [(pieces, hd, tile)] * 2
    return pl.pallas_call(
        functools.partial(prep_body, hd, tile, len(kvs)),
        grid_spec=pltpu.PrefetchScalarGridSpec(
            num_scalar_prefetch=1, grid=(1,),
            in_specs=[whole(a.shape) for a in kvs], out_specs=[whole(o) for o in out]),
        out_shape=[jax.ShapeDtypeStruct(o, BF16) for o in out],
        compiler_params=params(1, 24),
        cost_estimate=pl.CostEstimate(flops=1 << 20, bytes_accessed=3 << 20, transcendentals=0),
        name="kv_prep",
    )(ids, *kvs)


def attn_body(nh, hd, tile, pieces, scale, last, zero, n_out, ids, tids, rel, *refs):
    refs = list(refs)
    q_ref, do_ref, ks, vs, kt, vt, cos_ref, sin_ref = refs[:8]
    refs = refs[8:]
    if not zero:
        dki_ref, dvi_ref = refs[:2]
        refs = refs[2:]
    if last:
        call_ref, sall_ref = refs[:2]
        refs = refs[2:]
    o_refs = refs[:n_out]
    dq_refs = refs[n_out:2 * n_out]
    refs = refs[2 * n_out:]
    if last:
        dkv_ref, dkvp_ref, dk_ref, dv_ref = refs[:4]
        refs = refs[4:]
    else:
        dk_ref, dv_ref = refs[:2]
        refs = refs[2:]
    ps, dps, ms, pb, dsb, ot, dqt = refs
    step = pl.program_id(0)
    steps = pl.num_programs(0)
    tq = nh * tile
    c = scale * LOG2E

    @pl.when(step == 0)
    def _():
        dk_ref[...] = jnp.zeros_like(dk_ref) if zero else dki_ref[...]
        dv_ref[...] = jnp.zeros_like(dv_ref) if zero else dvi_ref[...]

    i = ids[step]

    def first(j, carry, diag):
        m, l, dl = carry
        kj = ks[j]
        vj = vs[j]
        m_new, l_new, d_new = [], [], []
        for n in range(nh):
            lanes = slice(n * tile, (n + 1) * tile)
            s = dot_nt(kj, q_ref[n]) * c
            if diag:
                key = lax.broadcasted_iota(jnp.int32, (tile, tile), 0)
                qry = lax.broadcasted_iota(jnp.int32, (tile, tile), 1)
                s = jnp.where(key <= qry, s, NEG)
            dpb = dot_nt(vj, do_ref[n]).astype(BF16)
            dps[j, :, lanes] = dpb
            mo = m[:, lanes]
            mn = jnp.maximum(mo, jnp.max(s, axis=0, keepdims=True))
            p = jnp.exp2(s - mn)
            ps[j, :, lanes] = p
            al = jnp.exp2(mo - mn)
            m_new.append(mn)
            l_new.append(l[:, lanes] * al + jnp.sum(p, axis=0, keepdims=True))
            d_new.append(dl[:, lanes] * al + jnp.sum(p * dpb.astype(F32), axis=0, keepdims=True))
        m = jnp.concatenate(m_new, axis=1)
        ms[j] = m
        return m, jnp.concatenate(l_new, axis=1), jnp.concatenate(d_new, axis=1)

    init = (jnp.full((1, tq), NEG, F32), jnp.zeros((1, tq), F32), jnp.zeros((1, tq), F32))
    carry = lax.fori_loop(0, i, lambda j, cr: first(j, cr, False), init)
    m, l, dl = first(i, carry, True)
    inv = 1.0 / l
    delta = dl * inv
    ot[...] = jnp.zeros_like(ot)
    dqt[...] = jnp.zeros_like(dqt)

    def second(j, carry):
        f = jnp.exp2(ms[j] - m) * inv
        for n in range(nh):
            lanes = slice(n * tile, (n + 1) * tile)
            p = ps[j, :, lanes] * f[:, lanes]
            pb[:, lanes] = p.astype(BF16)
            dsb[:, lanes] = (p * (dps[j, :, lanes].astype(F32) - delta[:, lanes])).astype(BF16)
        ot[...] += dot(vt[j], pb[...])
        dqt[...] += dot(kt[j], dsb[...])
        dv_ref[j] += dot(pb[...], do_ref[...].reshape(tq, hd))
        dk_ref[j] += dot(dsb[...], q_ref[...].reshape(tq, hd))
        return carry

    lax.fori_loop(0, i + 1, second, 0)
    cos_t = cos_ref[...]
    sin_t = sin_ref[...]

    def unrope(g, ct, st):
        g = g.astype(BF16).astype(F32)
        return (g * ct - pltpu.roll(g, hd // 2, 1) * st).astype(BF16)

    def write(o_ref, dq_ref):
        for n in range(nh):
            lanes = slice(n * tile, (n + 1) * tile)
            cols = slice(n * hd, (n + 1) * hd)
            o_ref[:, cols] = ot[:, lanes].T.astype(BF16)
            dq_ref[:, cols] = unrope(dqt[:, lanes].T * scale, cos_t, sin_t)

    if n_out == 1:
        write(o_refs[0], dq_refs[0])
    else:
        for k in range(n_out):
            pl.when(step // (steps // n_out) == k)(functools.partial(write, o_refs[k], dq_refs[k]))

    if last:
        @pl.when(step == steps - 1)
        def _():
            for s in range(pieces):
                rows = slice(s * tile, (s + 1) * tile)
                p = rel[s]
                gk = unrope(dk_ref[p] * scale, call_ref[rows, :], sall_ref[rows, :])
                gv = dv_ref[p].astype(BF16)
                dkv_ref[rows, :hd] = gk
                dkv_ref[rows, hd:] = gv
                if s // 2 == 1:
                    rows = slice((s - 2) * tile, (s - 1) * tile)
                    dkvp_ref[rows, :hd] = gk
                    dkvp_ref[rows, hd:] = gv


def attention(ids, tids, rel, q, do, keys, cos_t, sin_t, acc, scale, tile, n_out, last):
    nh, rows, hd = q.shape
    pieces = keys[0].shape[0]
    tq = nh * tile
    steps = rows // tile
    per = steps // n_out
    zero = acc is None

    def whole(shape):
        return pl.BlockSpec(shape, lambda i, a, b, c: (0,) * len(shape))

    heads = pl.BlockSpec((nh, tile, hd), lambda i, a, b, c: (0, i, 0))
    table = pl.BlockSpec((tile, hd), lambda i, a, b, c: (b[i], 0))

    def out(n):
        return pl.BlockSpec((tile, nh * hd), lambda i, a, b, c: (jnp.clip(i - n * per, 0, per - 1), 0))

    outs = [out(n) for n in range(n_out)] * 2
    shapes = [jax.ShapeDtypeStruct((per * tile, nh * hd), BF16)] * (2 * n_out)
    ins = [heads, heads] + [whole(a.shape) for a in keys] + [table, table]
    args = [q, do, *keys, cos_t, sin_t]
    sums = (pieces, tile, hd)
    if not zero:
        ins += [whole(sums), whole(sums)]
        args += list(acc)
    scratch = []
    if last:
        ins += [whole(cos_t.shape), whole(sin_t.shape)]
        args += [cos_t, sin_t]
        outs += [whole((pieces * tile, 2 * hd)), whole((2 * tile, 2 * hd))]
        shapes += [jax.ShapeDtypeStruct((pieces * tile, 2 * hd), BF16), jax.ShapeDtypeStruct((2 * tile, 2 * hd), BF16)]
        scratch += [pltpu.VMEM(sums, F32), pltpu.VMEM(sums, F32)]
    else:
        outs += [whole(sums), whole(sums)]
        shapes += [jax.ShapeDtypeStruct(sums, F32)] * 2
    scratch += [
        pltpu.VMEM((pieces, tile, tq), F32), pltpu.VMEM((pieces, tile, tq), BF16), pltpu.VMEM((pieces, 1, tq), F32),
        pltpu.VMEM((tile, tq), BF16), pltpu.VMEM((tile, tq), BF16), pltpu.VMEM((hd, tq), F32), pltpu.VMEM((hd, tq), F32)]
    return pl.pallas_call(
        functools.partial(attn_body, nh, hd, tile, pieces, scale, last, zero, n_out),
        grid_spec=pltpu.PrefetchScalarGridSpec(
            num_scalar_prefetch=3, grid=(steps,), in_specs=ins, out_specs=outs, scratch_shapes=scratch),
        out_shape=shapes,
        compiler_params=params(1),
        cost_estimate=pl.CostEstimate(flops=rows * pieces * tile * nh * hd * 12, bytes_accessed=8 << 20,
                                      transcendentals=rows * pieces * tile * nh),
        name="attn_fwd_bwd",
    )(ids, tids, rel, *args)


def y_body(c_ref, x_ref, om_ref, ot_ref, wm_ref, wt_ref, b_ref, y_ref):
    z = dot(om_ref[...], wm_ref[...]) + dot(ot_ref[...], wt_ref[...])
    y_ref[...] = (x_ref[...].astype(F32) + (z + b_ref[...].astype(F32))).astype(BF16)


def y_rows(core, x, o_mine, o_theirs, wo, bo, tm=256):
    rows, width = x.shape
    qw = o_mine.shape[1]
    row = pl.BlockSpec((tm, qw), lambda i, c: (i, 0))
    wide = pl.BlockSpec((tm, width), lambda i, c: (i, 0))
    return pl.pallas_call(
        y_body,
        grid_spec=pltpu.PrefetchScalarGridSpec(
            num_scalar_prefetch=1, grid=(rows // tm,),
            in_specs=[wide, row, row, pl.BlockSpec((qw, width), lambda i, c: (c[0], 0)),
                      pl.BlockSpec((qw, width), lambda i, c: (1 - c[0], 0)), pl.BlockSpec((1, width), lambda i, c: (0, 0))],
            out_specs=wide),
        out_shape=jax.ShapeDtypeStruct((rows, width), BF16),
        compiler_params=params(1),
        cost_estimate=pl.CostEstimate(flops=4 * rows * width * qw, bytes_accessed=8 << 20, transcendentals=0),
        name="y_rows",
    )(core, x, o_mine, o_theirs, wo, wo, bo)


def dx_body(hd, c_ref, x_ref, d_ref, qm_ref, qt_ref, km_ref, kt_ref, wqm, wqt, wkm, wkt, wvm, wvt, g_ref,
            dx_ref, v_ref, u_ref):
    @pl.when(pl.program_id(0) == 0)
    def _():
        v_ref[...] = jnp.zeros_like(v_ref)
        u_ref[...] = jnp.zeros_like(u_ref)

    qm = qm_ref[...]
    qt = qt_ref[...]
    km = km_ref[...]
    kt = kt_ref[...]
    dh = dot_nt(qm, wqm[...]) + dot_nt(qt, wqt[...])
    dh += dot_nt(km[:, :hd], wkm[...]) + dot_nt(kt[:, :hd], wkt[...])
    dh += dot_nt(km[:, hd:], wvm[...]) + dot_nt(kt[:, hd:], wvt[...])
    dh = dh.astype(BF16).astype(F32)
    x = x_ref[...].astype(F32)
    cen = x - jnp.mean(x, axis=-1, keepdims=True)
    inv = lax.rsqrt(jnp.mean(cen * cen, axis=-1, keepdims=True) + EPS)
    xh = cen * inv
    a = dh * g_ref[...].astype(F32)
    d = d_ref[...].astype(F32)
    dx = inv * (a - jnp.mean(a, axis=-1, keepdims=True) - xh * jnp.mean(a * xh, axis=-1, keepdims=True))
    dx_ref[...] = (d + dx).astype(BF16)

    def rows(t):
        return jnp.sum(t, axis=0, keepdims=True)

    v_ref[0:1, :] += rows(dh * xh)
    v_ref[1:2, :] += rows(dh)
    v_ref[2:3, :] += rows(d)
    qw = qm.shape[1]
    sides = ((c_ref[0], qm, km), (1 - c_ref[0], qt, kt))
    for side, q, k in sides:
        q = rows(q.astype(F32))
        k = rows(k.astype(F32))
        for h in range(2):
            @pl.when(side == h)
            def _():
                v_ref[3:4, h * qw:(h + 1) * qw] += q
                u_ref[0:1, h * hd:(h + 1) * hd] += k[:, :hd]
                u_ref[1:2, h * hd:(h + 1) * hd] += k[:, hd:]


def dx_rows(core, x, d, qm, qt, km, kt, wq, wk, wv, g, hd, tm=256):
    rows, width = x.shape
    qw = qm.shape[1]
    wide = pl.BlockSpec((tm, width), lambda i, c: (i, 0))
    row = pl.BlockSpec((tm, qw), lambda i, c: (i, 0))
    pair = pl.BlockSpec((tm, 2 * hd), lambda i, c: (i, 0))
    big = [pl.BlockSpec((width, qw), lambda i, c: (0, c[0])), pl.BlockSpec((width, qw), lambda i, c: (0, 1 - c[0]))]
    small = [pl.BlockSpec((width, hd), lambda i, c: (0, c[0])), pl.BlockSpec((width, hd), lambda i, c: (0, 1 - c[0]))]
    return pl.pallas_call(
        functools.partial(dx_body, hd),
        grid_spec=pltpu.PrefetchScalarGridSpec(
            num_scalar_prefetch=1, grid=(rows // tm,),
            in_specs=[wide, wide, row, row, pair, pair] + big + small + small + [pl.BlockSpec((1, width), lambda i, c: (0, 0))],
            out_specs=[wide, pl.BlockSpec((4, width), lambda i, c: (0, 0)), pl.BlockSpec((2, 2 * hd), lambda i, c: (0, 0))]),
        out_shape=[jax.ShapeDtypeStruct((rows, width), BF16), jax.ShapeDtypeStruct((4, width), F32),
                   jax.ShapeDtypeStruct((2, 2 * hd), F32)],
        compiler_params=params(1),
        cost_estimate=pl.CostEstimate(flops=4 * rows * width * (qw + 2 * hd), bytes_accessed=12 << 20, transcendentals=0),
        name="dx_rows",
    )(core, x, d, qm, qt, km, kt, wq, wq, wk, wk, wv, wv, g)


def dw_body(offs, merge, s_ref, *refs):
    refs = list(refs)
    h_offs, q_offs = offs
    n_h, n_q = len(h_offs), len(q_offs)
    h_refs = refs[:n_h]
    q_refs = refs[n_h:n_h + n_q]
    kv_ref = refs[n_h + n_q]
    refs = refs[n_h + n_q + 1:]
    if merge:
        gq_ref, gkv_ref, oq_ref, ok_ref, ov_ref, ht = refs
    else:
        oq_ref, okv_ref, ht = refs
    step = pl.program_id(0)

    @pl.when(step == 0)
    def _():
        for r, off in zip(h_refs, h_offs):
            ht[:, off:off + r.shape[0]] = r[...].T

    acc = None
    for r, off in zip(q_refs, q_offs):
        t = dot(ht[:, off:off + r.shape[0]], r[...])
        acc = t if acc is None else acc + t
    if not merge:
        oq_ref[...] = acc

        @pl.when(step == 0)
        def _():
            okv_ref[...] = dot(ht[...], kv_ref[...])
    else:
        core = s_ref[1]
        tn = acc.shape[1]
        steps = pl.num_programs(0)
        oq_ref[:, pl.ds(pl.multiple_of((core * steps + step) * tn, 128), tn)] = acc
        oq_ref[:, pl.ds(pl.multiple_of(((1 - core) * steps + step) * tn, 128), tn)] = gq_ref[...]

        @pl.when(step == 0)
        def _():
            kv = dot(ht[...], kv_ref[...])
            g = gkv_ref[...]
            hd = kv.shape[1] // 2
            mine = pl.ds(pl.multiple_of(core * hd, 128), hd)
            other = pl.ds(pl.multiple_of((1 - core) * hd, 128), hd)
            ok_ref[:, mine] = kv[:, :hd]
            ok_ref[:, other] = g[:, :hd]
            ov_ref[:, mine] = kv[:, hd:]
            ov_ref[:, other] = g[:, hd:]


def dw_rows(sel, hs, qs, kv, got, part, offs, tn=384):
    tokens = kv.shape[0]
    qw = qs[0].shape[1]
    kvw = kv.shape[1]
    merge = got is not None

    def whole(shape):
        return pl.BlockSpec(shape, lambda i, s: (0, 0))

    ins = [pl.BlockSpec((h.shape[0], part), lambda i, s: (0, s[0])) for h in hs]
    ins += [pl.BlockSpec((q.shape[0], tn), lambda i, s: (0, i)) for q in qs]
    ins += [whole(kv.shape)]
    args = [*hs, *qs, kv]
    if merge:
        ins += [pl.BlockSpec((part, tn), lambda i, s: (0, i)), whole((part, kvw))]
        args += list(got)
        dims = [(part, 2 * qw), (part, kvw), (part, kvw)]
        outs = [whole(d) for d in dims]
    else:
        dims = [(part, qw), (part, kvw)]
        outs = [pl.BlockSpec((part, tn), lambda i, s: (0, i)), whole((part, kvw))]
    return pl.pallas_call(
        functools.partial(dw_body, offs, merge),
        grid_spec=pltpu.PrefetchScalarGridSpec(
            num_scalar_prefetch=1, grid=(qw // tn,), in_specs=ins, out_specs=outs,
            scratch_shapes=[pltpu.VMEM((part, tokens), BF16)]),
        out_shape=[jax.ShapeDtypeStruct(d, F32) for d in dims],
        compiler_params=params(1),
        cost_estimate=pl.CostEstimate(flops=2 * part * tokens * (qw + kvw), bytes_accessed=8 << 20, transcendentals=0),
        name="dw_rows",
    )(sel, *args)


def dwo_body(n_src, offs, s_ref, *refs):
    om = refs[:n_src]
    og = refs[n_src:2 * n_src]
    d_refs = refs[2 * n_src:3 * n_src]
    out_ref, at = refs[3 * n_src:]

    @pl.when(pl.program_id(0) == 0)
    def _():
        for a, b, off in zip(om, og, offs):
            @pl.when(s_ref[1] == 1)
            def _():
                at[:, off:off + a.shape[0]] = a[...].T

            @pl.when(s_ref[1] == 0)
            def _():
                at[:, off:off + a.shape[0]] = b[...].T

    acc = None
    for r, off in zip(d_refs, offs):
        t = dot(at[:, off:off + r.shape[0]], r[...])
        acc = t if acc is None else acc + t
    out_ref[...] = acc


def dwo_rows(sel, o_mine, o_got, ds, part, offs, tn=384):
    width = ds[0].shape[1]
    tokens = sum(d.shape[0] for d in ds)
    n_src = len(ds)
    ins = [pl.BlockSpec((o.shape[0], part), lambda i, s: (0, s[0])) for o in o_mine + o_got]
    ins += [pl.BlockSpec((d.shape[0], tn), lambda i, s: (0, i)) for d in ds]
    return pl.pallas_call(
        functools.partial(dwo_body, n_src, offs),
        grid_spec=pltpu.PrefetchScalarGridSpec(
            num_scalar_prefetch=1, grid=(width // tn,), in_specs=ins,
            out_specs=pl.BlockSpec((part, tn), lambda i, s: (0, i)),
            scratch_shapes=[pltpu.VMEM((part, tokens), BF16)]),
        out_shape=jax.ShapeDtypeStruct((part, width), F32),
        compiler_params=params(1),
        cost_estimate=pl.CostEstimate(flops=2 * part * tokens * width, bytes_accessed=10 << 20, transcendentals=0),
        name="dwo_rows",
    )(sel, *o_mine, *o_got, *ds)


def after(values, *earlier):
    n = len(values)
    return lax.optimization_barrier(tuple(values) + tuple(earlier))[:n]


def solution(mesh):
    groups = mesh.shape['cp']
    row_spec = P('dp', 'cp', None)
    mat_spec = P(('dp', 'cp'), None)
    vec_spec = P('dp')
    near = [(i, i ^ 1) for i in range(groups)]
    far = [(i, i ^ 2) for i in range(groups)]

    def swap(v):
        return lax.ppermute(v, 'cp', near)

    def cross(v):
        return lax.ppermute(v, 'cp', far)

    def device_fn(x_in, ln_w, ln_b, w_q, b_q, w_k, b_k, w_v, b_v, w_o, b_o, long_factor, dy_out):
        rank = lax.axis_index('cp').astype(jnp.int32)
        core = rank & 1
        chip = rank >> 1
        x = x_in[0]
        d0 = dy_out[0]
        tokens, width = x.shape
        piece = tokens // 2
        hd = 2 * long_factor.shape[0]
        kv_heads = w_k.shape[1] // hd
        nh = w_q.shape[1] // hd // kv_heads
        scale = hd ** -0.5
        part = width // groups
        core_v = core[None]

        h0a, h0b = layer_norm(x, ln_w[None], ln_b[None])
        h1a = swap(h0a)
        h1b = swap(h0b)
        d1 = swap(d0)

        blocks = jnp.stack([rank, rank ^ 1, rank ^ 2, rank ^ 3])
        rel = jnp.stack([blocks, 2 * groups - 1 - blocks], axis=1).reshape(2 * groups)
        pos = (rel[:, None] * piece + jnp.arange(piece, dtype=jnp.int32)[None, :]).reshape(2 * groups * piece)
        cos_t, sin_t = rope_tables(pos, long_factor)

        def tile_ids(*t):
            return jnp.array(t, dtype=jnp.int32)

        def pieces_of(*t):
            return jnp.stack([rel[n] for n in t])

        def project(hs, *t):
            return qkv_proj(core_v, tile_ids(*t), hs, w_q, w_k, w_v, b_q[None], b_k[None], b_v[None], cos_t, sin_t, nh, hd)

        def attend(q, do, acc, n_out, last, *t):
            return attention(pieces_of(*t), tile_ids(*t), rel, q, do, keys, cos_t, sin_t, acc, scale, piece, n_out, last)

        q01, kv01 = project([h0a, h0b, h1a, h1b], 0, 1, 2, 3)
        kv23 = cross(kv01)
        h0b_s, d0_s = after((h0b, d0), kv01)
        h2b = cross(h0b_s)
        d2b = cross(d0_s[piece:])
        h0a_s, = after((h0a,), h0b_s)
        h2a = cross(h0a_s)
        d2a = cross(d0_s[:piece])
        do01 = do_proj(core_v, [d0, d1], w_o, nh, hd, piece)
        kv23, = after((kv23,), do01)
        keys = kv_prep(rel, [kv01, kv23], hd, piece)
        o0, o1, dq0, dq1, dk, dv = attend(q01, do01, None, 2, False, 0, 1, 2, 3)

        h2b, d2b = after((h2b, d2b), o0)
        h3b = swap(h2b)
        d3b = swap(d2b)
        o1_got = swap(o1)
        dq1_got = swap(dq1)
        o0_got = swap(o0)
        y = y_rows(core_v, x, o0, o1_got, w_o, b_o[None])
        q2, _ = project([h2b, h3b], 5, 7)
        do2 = do_proj(core_v, [d2b, d3b], w_o, nh, hd, piece)
        o2b, o3b, dq2b, dq3b, dk, dv = attend(q2, do2, (dk, dv), 2, False, 5, 7)

        h2a, d2a = after((h2a, d2a), o2b)
        h3a = swap(h2a)
        d3a = swap(d2a)
        o2b_got = swap(o2b)
        o3b_got = swap(o3b)
        q3, _ = project([h2a, h3a], 4, 6)
        do3 = do_proj(core_v, [d2a, d3a], w_o, nh, hd, piece)
        o2a, o3a, dq2a, dq3a, dkv, dkv_p = attend(q3, do3, (dk, dv), 2, True, 4, 6)
        dkv_got = swap(dkv_p)
        o2a_got = swap(o2a)
        o3a_got = swap(o3a)

        hs = [h0a, h0b, h1a, h1b, h2a, h2b, h3a, h3b]
        dqs = [dq0, dq1, dq2a, dq2b, dq3a, dq3b]
        h_offs = [n * piece for n in range(8)]
        offs = [0, tokens, 2 * tokens, 2 * tokens + piece, 3 * tokens, 3 * tokens + piece]
        hq = dw_rows(jnp.stack([rank ^ 1, core]), hs, dqs, dkv, None, part, (h_offs, offs))
        got_q = swap(hq[0])
        got_kv = swap(hq[1])
        dx, vec, small = dx_rows(core_v, x, d0, dq0, dq1_got, dkv[:tokens], dkv_got, w_q, w_k, w_v, ln_w[None], hd)
        vec = jnp.concatenate([vec.reshape(-1), small.reshape(-1)])
        vec = vec + swap(vec)
        vec_x = cross(vec)
        o_mine = [o0, o1, o2a, o2b, o3a, o3b]
        o_got = [o1_got, o0_got, o3a_got, o3b_got, o2a_got, o2b_got]
        d_wo = dwo_rows(jnp.stack([core, (core == chip).astype(jnp.int32)]), o_mine, o_got,
                        [d0, d1, d2a, d2b, d3a, d3b], part, offs)
        d_wq, d_wk, d_wv = dw_rows(jnp.stack([rank, core]), hs, dqs, dkv, (got_q, got_kv), part, (h_offs, offs))
        vec = vec + vec_x
        d_lnw, d_lnb, d_bo, d_bq = (vec[n * width:(n + 1) * width] for n in range(4))
        kvw = kv_heads * hd
        d_bk, d_bv = (vec[4 * width + n * kvw:4 * width + (n + 1) * kvw] for n in range(2))
        return (y[None], dx[None], d_wq, d_wk, d_wv, d_wo, d_lnw, d_lnb, d_bq, d_bk, d_bv, d_bo)

    in_specs = (row_spec,) + (P(),) * 11 + (row_spec,)
    out_specs = (row_spec, row_spec) + (mat_spec,) * 4 + (vec_spec,) * 6
    return jax.shard_map(device_fn, mesh=mesh, in_specs=in_specs, out_specs=out_specs, check_vma=False)
```

```python
import functools
import math
import jax
import jax.numpy as jnp
from jax import lax
from jax.experimental import pallas as pl
from jax.experimental.pallas import tpu as pltpu
from jax.sharding import PartitionSpec as P


EPS = 1e-5
THETA = 10000.0
ROPE_SCALE = math.sqrt(1.0 + math.log(32.0) / math.log(4096.0))
LOG2E = math.log2(math.e)
NEG = -1e30
F32 = jnp.float32
BF16 = jnp.bfloat16


def dot(a, b):
    return lax.dot_general(a, b, (((1,), (0,)), ((), ())), preferred_element_type=F32)


def dot_nt(a, b):
    return lax.dot_general(a, b, (((1,), (1,)), ((), ())), preferred_element_type=F32)


def dot_tn(a, b):
    return lax.dot_general(a, b, (((0,), (0,)), ((), ())), preferred_element_type=F32)


def rope_tables(starts, piece, long_factor):
    half_dim = long_factor.shape[0]
    exponent = jnp.arange(half_dim, dtype=F32) * (1.0 / half_dim)
    inv_freq = 1.0 / (long_factor * THETA ** exponent)
    positions = jnp.concatenate([jnp.arange(piece, dtype=jnp.int32), starts])
    angle = positions.astype(F32)[:, None] * inv_freq[None, :]
    cos_t = jnp.cos(angle)
    sin_t = jnp.sin(angle)
    return jnp.concatenate([cos_t, cos_t], axis=1), jnp.concatenate([-sin_t, sin_t], axis=1)


def tile_tables(cos_ref, sin_ref, piece, t):
    ca = cos_ref[pl.ds(piece + t, 1), :] * ROPE_SCALE
    sa = sin_ref[pl.ds(piece + t, 1), :] * ROPE_SCALE
    cb = cos_ref[:piece, :]
    sb = sin_ref[:piece, :]
    return ca * cb - sa * sb, sa * cb + ca * sb


def params(n, mib=40):
    return pltpu.CompilerParams(dimension_semantics=("arbitrary",) * n, vmem_limit_bytes=mib << 20)


def whole(shape):
    return pl.BlockSpec(shape, lambda *a: (0,) * len(shape))


def ln_body(x_ref, w_ref, b_ref, ha_ref, hb_ref):
    x = x_ref[...].astype(F32)
    cen = x - jnp.mean(x, axis=-1, keepdims=True)
    inv = lax.rsqrt(jnp.mean(cen * cen, axis=-1, keepdims=True) + EPS)
    h = (cen * inv * w_ref[...].astype(F32) + b_ref[...].astype(F32)).astype(BF16)

    @pl.when(pl.program_id(0) == 0)
    def _():
        ha_ref[...] = h

    @pl.when(pl.program_id(0) == 1)
    def _():
        hb_ref[...] = h


def layer_norm(x, w, b):
    rows, width = x.shape
    tm = rows // 2
    vec = pl.BlockSpec((1, width), lambda i: (0, 0))
    half = pl.BlockSpec((tm, width), lambda i: (0, 0))
    return pl.pallas_call(
        ln_body,
        grid=(2,),
        in_specs=[pl.BlockSpec((tm, width), lambda i: (i, 0)), vec, vec],
        out_specs=[half, half],
        out_shape=[jax.ShapeDtypeStruct((tm, width), BF16)] * 2,
        compiler_params=params(1, 24),
        cost_estimate=pl.CostEstimate(flops=rows * width * 12, bytes_accessed=rows * width * 4, transcendentals=0),
        name="ln_rows",
    )(x, w, b)


def qkv_body(hd, n_src, with_kv, c_ref, t_ref, *refs):
    h_refs = refs[:n_src]
    refs = refs[n_src:]
    wq_ref, bq_ref, cos_ref, sin_ref = refs[:4]
    refs = refs[4:]
    if with_kv:
        wk_ref, wv_ref, bk_ref, bv_ref, q_ref, kv_ref, tc, ts, wkv = refs
    else:
        q_ref, tc, ts = refs
    tm = h_refs[0].shape[0]

    def rope(t, rows):
        t = t.astype(BF16).astype(F32)
        return (t * tc[rows, :] + pltpu.roll(t, hd // 2, 1) * ts[rows, :]).astype(BF16)

    @pl.when(pl.program_id(0) == 0)
    def _():
        for n in range(n_src):
            rows = slice(n * tm, (n + 1) * tm)
            tc[rows, :], ts[rows, :] = tile_tables(cos_ref, sin_ref, tm, t_ref[n])
        if with_kv:
            wkv[:, :hd] = wk_ref[...]
            wkv[:, hd:] = wv_ref[...]
            for n in range(n_src):
                rows = slice(n * tm, (n + 1) * tm)
                kv = dot(h_refs[n][...], wkv[...])
                kv_ref[rows, :hd] = rope(kv[:, :hd] + bk_ref[...].astype(F32), rows)
                kv_ref[rows, hd:] = (kv[:, hd:] + bv_ref[...].astype(F32)).astype(BF16)

    for n in range(n_src):
        rows = slice(n * tm, (n + 1) * tm)
        q = dot(h_refs[n][...], wq_ref[...]) + bq_ref[...].astype(F32)
        for k in range(q_ref.shape[0]):
            q_ref[k, rows, :] = rope(q[:, k * hd:(k + 1) * hd], rows)


def qkv_proj(core, tids, hs, wq, bq, kv, cos_t, sin_t, nh, hd, per=2):
    tm, width = hs[0].shape
    n_src = len(hs)
    rows = tm * n_src
    steps = nh // per
    ins = [whole((tm, width))] * n_src
    ins += [pl.BlockSpec((width, per * hd), lambda i, c, t: (0, c[0] * steps + i)),
            pl.BlockSpec((1, per * hd), lambda i, c, t: (0, c[0] * steps + i)), whole(cos_t.shape), whole(sin_t.shape)]
    args = [*hs, wq, bq, cos_t, sin_t]
    outs = [pl.BlockSpec((per, rows, hd), lambda i, c, t: (i, 0, 0))]
    shapes = [jax.ShapeDtypeStruct((nh, rows, hd), BF16)]
    scratch = [pltpu.VMEM((rows, hd), F32), pltpu.VMEM((rows, hd), F32)]
    if kv is not None:
        ins += [pl.BlockSpec((width, hd), lambda i, c, t: (0, c[0]))] * 2
        ins += [pl.BlockSpec((1, hd), lambda i, c, t: (0, c[0]))] * 2
        args += list(kv)
        outs += [whole((rows, 2 * hd))]
        shapes += [jax.ShapeDtypeStruct((rows, 2 * hd), BF16)]
        scratch += [pltpu.VMEM((width, 2 * hd), BF16)]
    return pl.pallas_call(
        functools.partial(qkv_body, hd, n_src, kv is not None),
        grid_spec=pltpu.PrefetchScalarGridSpec(
            num_scalar_prefetch=2, grid=(steps,), in_specs=ins, out_specs=outs, scratch_shapes=scratch),
        out_shape=shapes,
        compiler_params=params(1, 32),
        cost_estimate=pl.CostEstimate(flops=2 * rows * width * nh * hd, bytes_accessed=8 << 20, transcendentals=0),
        name="qkv_proj",
    )(core, tids, *args)


def do_body(hd, n_src, c_ref, *refs):
    d_refs = refs[:n_src]
    wo_ref, o_ref = refs[n_src:]
    off = 0
    for d in d_refs:
        rows = slice(off, off + d.shape[0])
        r = dot_nt(d[...], wo_ref[...]).astype(BF16)
        for k in range(o_ref.shape[0]):
            o_ref[k, rows, :] = r[:, k * hd:(k + 1) * hd]
        off += d.shape[0]


def do_proj(core, ds, wo, nh, hd, per=2):
    width = ds[0].shape[1]
    rows = sum(d.shape[0] for d in ds)
    steps = nh // per
    return pl.pallas_call(
        functools.partial(do_body, hd, len(ds)),
        grid_spec=pltpu.PrefetchScalarGridSpec(
            num_scalar_prefetch=1, grid=(steps,),
            in_specs=[whole(d.shape) for d in ds] + [pl.BlockSpec((per * hd, width), lambda i, c: (c[0] * steps + i, 0))],
            out_specs=pl.BlockSpec((per, rows, hd), lambda i, c: (i, 0, 0))),
        out_shape=jax.ShapeDtypeStruct((nh, rows, hd), BF16),
        compiler_params=params(1, 32),
        cost_estimate=pl.CostEstimate(flops=2 * rows * width * nh * hd, bytes_accessed=6 << 20, transcendentals=0),
        name="do_proj",
    )(core, *ds, wo)


def prep_body(hd, tile, n_src, ids, *refs):
    kv_refs = refs[:n_src]
    ks, vs, kt, vt = refs[n_src:]
    s = 0
    for ref in kv_refs:
        for r in range(ref.shape[0] // tile):
            p = ids[s]
            k = ref[r * tile:(r + 1) * tile, :hd]
            v = ref[r * tile:(r + 1) * tile, hd:]
            ks[p] = k
            vs[p] = v
            kt[p] = k.T
            vt[p] = v.T
            s += 1


def kv_prep(ids, kvs, hd, tile):
    pieces = sum(a.shape[0] for a in kvs) // tile
    out = [(pieces, tile, hd)] * 2 + [(pieces, hd, tile)] * 2
    return pl.pallas_call(
        functools.partial(prep_body, hd, tile, len(kvs)),
        grid_spec=pltpu.PrefetchScalarGridSpec(
            num_scalar_prefetch=1, grid=(1,),
            in_specs=[whole(a.shape) for a in kvs], out_specs=[whole(o) for o in out]),
        out_shape=[jax.ShapeDtypeStruct(o, BF16) for o in out],
        compiler_params=params(1, 24),
        cost_estimate=pl.CostEstimate(flops=1 << 20, bytes_accessed=3 << 20, transcendentals=0),
        name="kv_prep",
    )(ids, *kvs)


def attn_body(nh, hd, tile, pieces, scale, last, zero, natural, n_out, ids, tids, rel, *refs):
    refs = list(refs)

    def take(n):
        got = refs[:n]
        del refs[:n]
        return got

    q_ref, do_ref, ks, vs, kt, vt, cos_ref, sin_ref = take(8)
    if not zero:
        dki_ref, dvi_ref = take(2)
    keep_refs = take(n_out)
    send_refs = take(n_out)
    dqt_refs = take(n_out)
    if natural:
        o_refs = take(n_out)
        dq_refs = take(n_out)
    if last:
        dkvt_ref, dkv0_ref, dkv1_ref = take(3)
    dk_ref, dv_ref = take(2)
    ps, dps, ms, pb, dsb, ot, dqt = refs
    step = pl.program_id(0)
    steps = pl.num_programs(0)
    tq = nh * tile
    c = scale * LOG2E

    @pl.when(step == 0)
    def _():
        dk_ref[...] = jnp.zeros_like(dk_ref) if zero else dki_ref[...]
        dv_ref[...] = jnp.zeros_like(dv_ref) if zero else dvi_ref[...]

    i = ids[step]

    def first(j, carry, diag):
        m, l, dl = carry
        kj = ks[j]
        vj = vs[j]
        m_new, l_new, d_new = [], [], []
        for n in range(nh):
            lanes = slice(n * tile, (n + 1) * tile)
            s = dot_nt(kj, q_ref[n]) * c
            if diag:
                key = lax.broadcasted_iota(jnp.int32, (tile, tile), 0)
                qry = lax.broadcasted_iota(jnp.int32, (tile, tile), 1)
                s = jnp.where(key <= qry, s, NEG)
            dpb = dot_nt(vj, do_ref[n]).astype(BF16)
            dps[j, :, lanes] = dpb
            mo = m[:, lanes]
            mn = jnp.maximum(mo, jnp.max(s, axis=0, keepdims=True))
            p = jnp.exp2(s - mn)
            ps[j, :, lanes] = p
            al = jnp.exp2(mo - mn)
            m_new.append(mn)
            l_new.append(l[:, lanes] * al + jnp.sum(p, axis=0, keepdims=True))
            d_new.append(dl[:, lanes] * al + jnp.sum(p * dpb.astype(F32), axis=0, keepdims=True))
        m = jnp.concatenate(m_new, axis=1)
        ms[j] = m
        return m, jnp.concatenate(l_new, axis=1), jnp.concatenate(d_new, axis=1)

    init = (jnp.full((1, tq), NEG, F32), jnp.zeros((1, tq), F32), jnp.zeros((1, tq), F32))
    carry = lax.fori_loop(0, i, lambda j, cr: first(j, cr, False), init)
    m, l, dl = first(i, carry, True)
    inv = 1.0 / l
    delta = dl * inv
    ot[...] = jnp.zeros_like(ot)
    dqt[...] = jnp.zeros_like(dqt)

    def second(j, carry):
        f = jnp.exp2(ms[j] - m) * inv
        for n in range(nh):
            lanes = slice(n * tile, (n + 1) * tile)
            p = ps[j, :, lanes] * f[:, lanes]
            pb[:, lanes] = p.astype(BF16)
            dsb[:, lanes] = (p * (dps[j, :, lanes].astype(F32) - delta[:, lanes])).astype(BF16)
        ot[...] += dot(vt[j], pb[...])
        dqt[...] += dot(kt[j], dsb[...])
        dv_ref[j] += dot(pb[...], do_ref[...].reshape(tq, hd))
        dk_ref[j] += dot(dsb[...], q_ref[...].reshape(tq, hd))
        return carry

    lax.fori_loop(0, i + 1, second, 0)
    tc, ts = tile_tables(cos_ref, sin_ref, tile, tids[step])
    cos_t = tc.T[:hd // 2]
    sin_t = ts.T[hd // 2:]
    core = rel[pieces]

    def write(k):
        for n in range(nh):
            lanes = slice(n * tile, (n + 1) * tile)
            o_t = ot[:, lanes].astype(BF16)
            half = slice((n % (nh // 2)) * hd, (n % (nh // 2) + 1) * hd)

            @pl.when(core == n // (nh // 2))
            def _():
                keep_refs[k][half, :] = o_t

            @pl.when(core != n // (nh // 2))
            def _():
                send_refs[k][half, :] = o_t

            g = (dqt[:, lanes] * scale).astype(BF16).astype(F32)
            a = g[:hd // 2]
            e = g[hd // 2:]
            g = jnp.concatenate([a * cos_t + e * sin_t, e * cos_t - a * sin_t], axis=0).astype(BF16)
            cols = slice(n * hd, (n + 1) * hd)
            dqt_refs[k][cols, :] = g
            if natural:
                o_refs[k][:, cols] = o_t.T
                dq_refs[k][:, cols] = g.T

    if n_out == 1:
        write(0)
    else:
        for k in range(n_out):
            pl.when(step // (steps // n_out) == k)(functools.partial(write, k))

    if last:
        @pl.when(step == steps - 1)
        def _():
            for s in range(pieces):
                cols = slice(s * tile, (s + 1) * tile)
                p = rel[s]
                ct, st = tile_tables(cos_ref, sin_ref, tile, s)
                g = (dk_ref[p] * scale).astype(BF16).astype(F32)
                gk = (g * ct - pltpu.roll(g, hd // 2, 1) * st).astype(BF16)
                gv = dv_ref[p].astype(BF16)
                dkvt_ref[:hd, cols] = gk.T
                dkvt_ref[hd:, cols] = gv.T
                if s < 4:
                    rows = slice((s % 2) * tile, (s % 2 + 1) * tile)
                    out = (dkv0_ref, dkv1_ref)[s // 2]
                    out[rows, :hd] = gk
                    out[rows, hd:] = gv


def attention(ids, tids, rel, q, do, keys, cos_t, sin_t, acc, scale, tile, n_out, last, natural):
    nh, rows, hd = q.shape
    pieces = keys[0].shape[0]
    tq = nh * tile
    steps = rows // tile
    per = steps // n_out
    zero = acc is None
    heads = pl.BlockSpec((nh, tile, hd), lambda i, a, b, c: (0, i, 0))

    def clip(i, n):
        return jnp.clip(i - n * per, 0, per - 1)

    def cols(n, r):
        return pl.BlockSpec((r, tile), lambda i, a, b, c: (0, clip(i, n)))

    def out(n):
        return pl.BlockSpec((tile, nh * hd), lambda i, a, b, c: (clip(i, n), 0))

    def shape(*dims):
        return jax.ShapeDtypeStruct(dims, BF16)

    outs = [cols(n, nh * hd // 2) for n in range(n_out)] * 2 + [cols(n, nh * hd) for n in range(n_out)]
    shapes = [shape(nh * hd // 2, per * tile)] * (2 * n_out) + [shape(nh * hd, per * tile)] * n_out
    if natural:
        outs += [out(n) for n in range(n_out)] * 2
        shapes += [shape(per * tile, nh * hd)] * (2 * n_out)
    ins = [heads, heads] + [whole(a.shape) for a in keys] + [whole(cos_t.shape), whole(sin_t.shape)]
    args = [q, do, *keys, cos_t, sin_t]
    sums = (pieces, tile, hd)
    if not zero:
        ins += [whole(sums), whole(sums)]
        args += list(acc)
    scratch = []
    if last:
        dims = [(2 * hd, pieces * tile), (2 * tile, 2 * hd), (2 * tile, 2 * hd)]
        outs += [whole(d) for d in dims]
        shapes += [shape(*d) for d in dims]
        scratch += [pltpu.VMEM(sums, F32), pltpu.VMEM(sums, F32)]
    else:
        outs += [whole(sums), whole(sums)]
        shapes += [jax.ShapeDtypeStruct(sums, F32)] * 2
    scratch += [
        pltpu.VMEM((pieces, tile, tq), F32), pltpu.VMEM((pieces, tile, tq), BF16), pltpu.VMEM((pieces, 1, tq), F32),
        pltpu.VMEM((tile, tq), BF16), pltpu.VMEM((tile, tq), BF16), pltpu.VMEM((hd, tq), F32), pltpu.VMEM((hd, tq), F32)]
    return pl.pallas_call(
        functools.partial(attn_body, nh, hd, tile, pieces, scale, last, zero, natural, n_out),
        grid_spec=pltpu.PrefetchScalarGridSpec(
            num_scalar_prefetch=3, grid=(steps,), in_specs=ins, out_specs=outs, scratch_shapes=scratch),
        out_shape=shapes,
        compiler_params=params(1, 44),
        cost_estimate=pl.CostEstimate(flops=rows * pieces * tile * nh * hd * 12, bytes_accessed=8 << 20,
                                      transcendentals=rows * pieces * tile * nh),
        name="attn_fwd_bwd",
    )(ids, tids, rel, *args)


def y_body(x_ref, om_ref, ot_ref, w_ref, b_ref, y_ref, z_ref):
    @pl.when(pl.program_id(0) == 0)
    def _():
        z_ref[...] = dot(om_ref[...], w_ref[...])

    @pl.when(pl.program_id(0) == 1)
    def _():
        z = z_ref[...] + dot(ot_ref[...], w_ref[...])
        y_ref[...] = (x_ref[...].astype(F32) + (z + b_ref[...].astype(F32))).astype(BF16)


def y_rows(core, x, o_mine, o_theirs, wo, bo):
    rows, width = x.shape
    qw = o_mine.shape[1]
    return pl.pallas_call(
        lambda c, *refs: y_body(*refs),
        grid_spec=pltpu.PrefetchScalarGridSpec(
            num_scalar_prefetch=1, grid=(2,),
            in_specs=[whole((rows, width)), whole((rows, qw)), whole((rows, qw)),
                      pl.BlockSpec((qw, width), lambda i, c: (c[0] + i - 2 * c[0] * i, 0)), whole((1, width))],
            out_specs=whole((rows, width)),
            scratch_shapes=[pltpu.VMEM((rows, width), F32)]),
        out_shape=jax.ShapeDtypeStruct((rows, width), BF16),
        compiler_params=params(1, 32),
        cost_estimate=pl.CostEstimate(flops=4 * rows * width * qw, bytes_accessed=8 << 20, transcendentals=0),
        name="y_rows",
    )(core, x, o_mine, o_theirs, wo, bo)


def dx_body(hd, c_ref, x_ref, d_ref, qm_ref, qt_ref, km_ref, kt_ref, wq_ref, wk_ref, wv_ref, g_ref, dx_ref, v_ref, acc):
    step = pl.program_id(0)
    qw = qm_ref.shape[1]

    def rows(t):
        return jnp.sum(t, axis=0, keepdims=True)

    def put(side, q, k):
        q = rows(q.astype(F32))
        k = rows(k.astype(F32))
        for h in range(2):
            @pl.when(side == h)
            def _():
                v_ref[3:4, h * qw:(h + 1) * qw] = q
                v_ref[4:5, h * hd:(h + 1) * hd] = k[:, :hd]
                v_ref[5:6, h * hd:(h + 1) * hd] = k[:, hd:]

    @pl.when(step == 0)
    def _():
        v_ref[...] = jnp.zeros_like(v_ref)
        acc[...] = dot_nt(qm_ref[...], wq_ref[...])
        put(c_ref[0], qm_ref[...], km_ref[...])

    @pl.when(step == 1)
    def _():
        acc[...] += dot_nt(qt_ref[...], wq_ref[...])
        put(1 - c_ref[0], qt_ref[...], kt_ref[...])
        mine = pl.ds(pl.multiple_of(c_ref[0] * hd, 128), hd)
        other = pl.ds(pl.multiple_of((1 - c_ref[0]) * hd, 128), hd)
        km = km_ref[...]
        kt = kt_ref[...]
        tm = 128
        for r in range(0, acc.shape[0], tm):
            s = slice(r, r + tm)
            dh = acc[s, :] + (dot_nt(km[s, :hd], wk_ref[:, mine]) + dot_nt(kt[s, :hd], wk_ref[:, other])
                              + dot_nt(km[s, hd:], wv_ref[:, mine]) + dot_nt(kt[s, hd:], wv_ref[:, other]))
            dh = dh.astype(BF16).astype(F32)
            x = x_ref[s, :].astype(F32)
            cen = x - jnp.mean(x, axis=-1, keepdims=True)
            inv = lax.rsqrt(jnp.mean(cen * cen, axis=-1, keepdims=True) + EPS)
            xh = cen * inv
            a = dh * g_ref[...].astype(F32)
            d = d_ref[s, :].astype(F32)
            dx = inv * (a - jnp.mean(a, axis=-1, keepdims=True) - xh * jnp.mean(a * xh, axis=-1, keepdims=True))
            dx_ref[s, :] = (d + dx).astype(BF16)
            v_ref[0:1, :] += rows(dh * xh)
            v_ref[1:2, :] += rows(dh)
            v_ref[2:3, :] += rows(d)


def dx_rows(core, x, d, qm, qt, km, kt, wq, wk, wv, g, hd):
    rows, width = x.shape
    qw = qm.shape[1]
    kvw = wk.shape[1]
    return pl.pallas_call(
        functools.partial(dx_body, hd),
        grid_spec=pltpu.PrefetchScalarGridSpec(
            num_scalar_prefetch=1, grid=(2,),
            in_specs=[whole((rows, width))] * 2 + [whole((rows, qw))] * 2 + [whole((rows, 2 * hd))] * 2 + [
                pl.BlockSpec((width, qw), lambda i, c: (0, c[0] + i - 2 * c[0] * i)),
                whole((width, kvw)), whole((width, kvw)), whole((1, width))],
            out_specs=[whole((rows, width)), whole((8, width))],
            scratch_shapes=[pltpu.VMEM((rows, width), F32)]),
        out_shape=[jax.ShapeDtypeStruct((rows, width), BF16), jax.ShapeDtypeStruct((8, width), F32)],
        compiler_params=params(1),
        cost_estimate=pl.CostEstimate(flops=4 * rows * width * (qw + 2 * hd), bytes_accessed=12 << 20, transcendentals=0),
        name="dx_rows",
    )(core, x, d, qm, qt, km, kt, wq, wk, wv, g)


def dw_body(h_offs, q_offs, s_ref, *refs):
    refs = list(refs)
    n_h, n_q = len(h_offs), len(q_offs)
    h_refs = refs[:n_h]
    q_refs = refs[n_h:n_h + n_q]
    kv_ref, o_ref = refs[n_h + n_q:]
    steps = pl.num_programs(0)
    part = h_refs[0].shape[1] // 2

    def run(lhs):
        acc = None
        for r, off in zip(h_refs, h_offs):
            t = dot(lhs(off, r.shape[0]), r[...])
            acc = t if acc is None else acc + t
        o_ref[0] = acc[:, :part].T
        o_ref[1] = acc[:, part:].T

    def from_q(off, n):
        for r, o in zip(q_refs, q_offs):
            if o <= off < o + r.shape[1]:
                return r[:, off - o:off - o + n]

    @pl.when(pl.program_id(0) < steps - 1)
    def _():
        run(from_q)

    @pl.when(pl.program_id(0) == steps - 1)
    def _():
        run(lambda off, n: kv_ref[:, off:off + n])


def dw_rows(sel, hs, qts, kvt, part, h_offs, q_offs, tn=256):
    kvw, tokens = kvt.shape
    qw = qts[0].shape[0]
    steps = qw // tn
    ins = [pl.BlockSpec((h.shape[0], 2 * part), lambda i, s: (0, s[0])) for h in hs]
    ins += [pl.BlockSpec((tn, q.shape[1]), lambda i, s: (jnp.minimum(i, steps - 1), 0)) for q in qts]
    ins += [whole(kvt.shape)]
    return pl.pallas_call(
        functools.partial(dw_body, h_offs, q_offs),
        grid_spec=pltpu.PrefetchScalarGridSpec(
            num_scalar_prefetch=1, grid=(steps + 1,), in_specs=ins,
            out_specs=pl.BlockSpec((2, part, tn), lambda i, s: (0, 0, i))),
        out_shape=jax.ShapeDtypeStruct((2, part, qw + kvw), F32),
        compiler_params=params(1),
        cost_estimate=pl.CostEstimate(flops=4 * part * tokens * (qw + kvw), bytes_accessed=12 << 20, transcendentals=0),
        name="dw_rows",
    )(sel, *hs, *qts, kvt)


def merge_body(s_ref, m_ref, t_ref, q_ref, k_ref, v_ref):
    core = s_ref[0]
    qw = q_ref.shape[1] // 2
    hd = k_ref.shape[1] // 2
    for side, r in ((core, m_ref), (1 - core, t_ref)):
        for h in range(2):
            @pl.when(side == h)
            def _():
                q_ref[:, h * qw:(h + 1) * qw] = r[0, :, :qw]
                k_ref[:, h * hd:(h + 1) * hd] = r[0, :, qw:qw + hd]
                v_ref[:, h * hd:(h + 1) * hd] = r[0, :, qw + hd:]


def merge_cols(core, both, got, qw, hd, tm=128):
    part, cols = got.shape[1:]
    outs = [(part, 2 * qw), (part, 2 * hd), (part, 2 * hd)]
    return pl.pallas_call(
        merge_body,
        grid_spec=pltpu.PrefetchScalarGridSpec(
            num_scalar_prefetch=1, grid=(part // tm,),
            in_specs=[pl.BlockSpec((1, tm, cols), lambda i, s: (s[0], i, 0)), pl.BlockSpec((1, tm, cols), lambda i, s: (0, i, 0))],
            out_specs=[pl.BlockSpec((tm, o[1]), lambda i, s: (i, 0)) for o in outs]),
        out_shape=[jax.ShapeDtypeStruct(o, F32) for o in outs],
        compiler_params=params(1, 24),
        cost_estimate=pl.CostEstimate(flops=1 << 20, bytes_accessed=6 << 20, transcendentals=0),
        name="merge_cols",
    )(core, both, got)


def dwo_body(offs, s_ref, *refs):
    n_src = len(offs)
    om = refs[:n_src]
    og = refs[n_src:2 * n_src]
    d_refs = refs[2 * n_src:3 * n_src]
    out_ref, at = refs[3 * n_src:]

    @pl.when(pl.program_id(0) == 0)
    def _():
        for a, b, off in zip(om, og, offs):
            at[:, off:off + a.shape[1]] = jnp.where(s_ref[0] == 1, a[...], b[...])

    acc = None
    for r, off in zip(d_refs, offs):
        t = dot(at[:, off:off + r.shape[0]], r[...])
        acc = t if acc is None else acc + t
    out_ref[...] = acc


def dwo_rows(sel, o_mine, o_got, ds, offs, tn=512):
    part = o_mine[0].shape[0]
    width = ds[0].shape[1]
    tokens = sum(d.shape[0] for d in ds)
    ins = [whole(o.shape) for o in o_mine + o_got]
    ins += [pl.BlockSpec((d.shape[0], tn), lambda i, s: (0, i)) for d in ds]
    return pl.pallas_call(
        functools.partial(dwo_body, offs),
        grid_spec=pltpu.PrefetchScalarGridSpec(
            num_scalar_prefetch=1, grid=(width // tn,), in_specs=ins,
            out_specs=pl.BlockSpec((part, tn), lambda i, s: (0, i)),
            scratch_shapes=[pltpu.VMEM((part, tokens), BF16)]),
        out_shape=jax.ShapeDtypeStruct((part, width), F32),
        compiler_params=params(1),
        cost_estimate=pl.CostEstimate(flops=2 * part * tokens * width, bytes_accessed=10 << 20, transcendentals=0),
        name="dwo_rows",
    )(sel, *o_mine, *o_got, *ds)


def after(values, *earlier):
    n = len(values)
    return lax.optimization_barrier(tuple(values) + tuple(earlier))[:n]


def solution(mesh):
    groups = mesh.shape['cp']
    row_spec = P('dp', 'cp', None)
    mat_spec = P(('dp', 'cp'), None)
    vec_spec = P('dp')
    near = [(i, i ^ 1) for i in range(groups)]
    far = [(i, i ^ 2) for i in range(groups)]

    def swap(v):
        return lax.ppermute(v, 'cp', near)

    def cross(v):
        return lax.ppermute(v, 'cp', far)

    def device_fn(x_in, ln_w, ln_b, w_q, b_q, w_k, b_k, w_v, b_v, w_o, b_o, long_factor, dy_out):
        rank = lax.axis_index('cp').astype(jnp.int32)
        core = rank & 1
        chip = rank >> 1
        x = x_in[0]
        d0 = dy_out[0]
        tokens, width = x.shape
        piece = tokens // 2
        hd = 2 * long_factor.shape[0]
        kv_heads = w_k.shape[1] // hd
        nh = w_q.shape[1] // hd // kv_heads
        scale = hd ** -0.5
        part = width // groups
        core_v = core[None]

        h0a, h0b = layer_norm(x, ln_w[None], ln_b[None])
        h1a = swap(h0a)
        h1b = swap(h0b)
        d1 = swap(d0)

        blocks = jnp.stack([rank, rank ^ 1, rank ^ 2, rank ^ 3])
        rel = jnp.stack([blocks, 2 * groups - 1 - blocks], axis=1).reshape(2 * groups)
        cos_t, sin_t = rope_tables(rel * piece, piece, long_factor)
        rel = jnp.concatenate([rel, core_v])

        def tile_ids(*t):
            return jnp.array(t, dtype=jnp.int32)

        def pieces_of(*t):
            return jnp.stack([rel[n] for n in t])

        def project(hs, kv, *t):
            return qkv_proj(core_v, tile_ids(*t), hs, w_q, b_q[None], kv, cos_t, sin_t, nh, hd)

        def attend(q, do, acc, last, natural, *t):
            return attention(pieces_of(*t), tile_ids(*t), rel, q, do, keys, cos_t, sin_t, acc, scale, piece, 2, last, natural)

        q01, kv01 = project([h0a, h0b, h1a, h1b], (w_k, w_v, b_k[None], b_v[None]), 0, 1, 2, 3)
        kv23 = cross(kv01)
        h0b_s, d0_s = after((h0b, d0), kv01)
        h2b = cross(h0b_s)
        d2b = cross(d0_s[piece:])
        h0a_s, = after((h0a,), h0b_s)
        h2a = cross(h0a_s)
        d2a = cross(d0_s[:piece])
        do01 = do_proj(core_v, [d0, d1], w_o, nh, hd)
        kv23, = after((kv23,), do01)
        keys = kv_prep(rel, [kv01, kv23], hd, piece)
        k0, k1, s0, s1, qt0, qt1, o0, o1, dq0, dq1, dk, dv = attend(q01, do01, None, False, True, 0, 1, 2, 3)

        h2b, d2b = after((h2b, d2b), o0)
        h3b = swap(h2b)
        d3b = swap(d2b)
        o1_got = swap(o1)
        dq1_got = swap(dq1)
        g0 = swap(s1)
        g1 = swap(s0)
        q2, = project([h2b, h3b], None, 5, 7)
        do2 = do_proj(core_v, [d2b, d3b], w_o, nh, hd)
        k2b, k3b, s2b, s3b, qt2b, qt3b, dk, dv = attend(q2, do2, (dk, dv), False, False, 5, 7)

        h2a, d2a = after((h2a, d2a), k2b)
        h3a = swap(h2a)
        d3a = swap(d2a)
        g2b = swap(s3b)
        g3b = swap(s2b)
        q3, = project([h2a, h3a], None, 4, 6)
        do3 = do_proj(core_v, [d2a, d3a], w_o, nh, hd)
        k2a, k3a, s2a, s3a, qt2a, qt3a, dkv_t, dkv0, dkv1 = attend(q3, do3, (dk, dv), True, False, 4, 6)
        dkv_got = swap(dkv1)
        g2a = swap(s3a)
        g3a = swap(s2a)

        hs = [h0a, h0b, h1a, h1b, h2a, h2b, h3a, h3b]
        h_offs = [n * piece for n in range(8)]
        offs = [0, tokens, 2 * tokens, 2 * tokens + piece, 3 * tokens, 3 * tokens + piece]
        d_w = dw_rows(chip[None], hs, [qt0, qt1, qt2a, qt2b, qt3a, qt3b], dkv_t, part, h_offs, offs)
        got = swap(lax.dynamic_slice(d_w, (1 - core, 0, 0), (1, part, d_w.shape[2])))
        dkv_got, = after((dkv_got,), d_w)
        dx, vec = dx_rows(core_v, x, d0, dq0, dq1_got, dkv0, dkv_got, w_q, w_k, w_v, ln_w[None], hd)
        vec = vec + swap(vec)
        vec_x = cross(vec)
        g2a, g3a = after((g2a, g3a), dx)
        d_wo = dwo_rows((core == chip).astype(jnp.int32)[None], [k0, k1, k2a, k2b, k3a, k3b], [g0, g1, g2a, g2b, g3a, g3b],
                        [d0, d1, d2a, d2b, d3a, d3b], offs)
        y = y_rows(core_v, x, o0, o1_got, w_o, b_o[None])
        got, = after((got,), d_wo)
        d_wq, d_wk, d_wv = merge_cols(core_v, d_w, got, nh * hd, hd)
        vec = vec + vec_x
        kvw = kv_heads * hd
        d_lnw, d_lnb, d_bo, d_bq = (vec[n] for n in range(4))
        d_bk, d_bv = (vec[n, :kvw] for n in (4, 5))
        return (y[None], dx[None], d_wq, d_wk, d_wv, d_wo, d_lnw, d_lnb, d_bq, d_bk, d_bv, d_bo)

    in_specs = (row_spec,) + (P(),) * 11 + (row_spec,)
    out_specs = (row_spec, row_spec) + (mat_spec,) * 4 + (vec_spec,) * 6
    return jax.shard_map(device_fn, mesh=mesh, in_specs=in_specs, out_specs=out_specs, check_vma=False)
```

```python
import functools
import math
import jax
import jax.numpy as jnp
from jax import lax
from jax.experimental import pallas as pl
from jax.experimental.pallas import tpu as pltpu
from jax.sharding import PartitionSpec as P


EPS = 1e-5
THETA = 10000.0
ROPE_SCALE = math.sqrt(1.0 + math.log(32.0) / math.log(4096.0))
LOG2E = math.log2(math.e)
NEG = -1e30
F32 = jnp.float32
BF16 = jnp.bfloat16


def dot(a, b):
    return lax.dot_general(a, b, (((1,), (0,)), ((), ())), preferred_element_type=F32)


def dot_nt(a, b):
    return lax.dot_general(a, b, (((1,), (1,)), ((), ())), preferred_element_type=F32)


def dot_tn(a, b):
    return lax.dot_general(a, b, (((0,), (0,)), ((), ())), preferred_element_type=F32)


def rope_tables(starts, piece, long_factor):
    half_dim = long_factor.shape[0]
    exponent = jnp.arange(half_dim, dtype=F32) * (1.0 / half_dim)
    inv_freq = 1.0 / (long_factor * THETA ** exponent)
    positions = jnp.concatenate([jnp.arange(piece, dtype=jnp.int32), starts])
    angle = positions.astype(F32)[:, None] * inv_freq[None, :]
    cos_t = jnp.cos(angle)
    sin_t = jnp.sin(angle)
    return jnp.concatenate([cos_t, cos_t], axis=1), jnp.concatenate([-sin_t, sin_t], axis=1)


def tile_tables(cos_ref, sin_ref, piece, t):
    ca = cos_ref[pl.ds(piece + t, 1), :] * ROPE_SCALE
    sa = sin_ref[pl.ds(piece + t, 1), :] * ROPE_SCALE
    cb = cos_ref[:piece, :]
    sb = sin_ref[:piece, :]
    return ca * cb - sa * sb, sa * cb + ca * sb


def params(n, mib=64):
    return pltpu.CompilerParams(dimension_semantics=("arbitrary",) * n, vmem_limit_bytes=67043328)


def whole(shape):
    return pl.BlockSpec(shape, lambda *a: (0,) * len(shape))


def ln_body(x_ref, w_ref, b_ref, ha_ref, hb_ref):
    x = x_ref[...].astype(F32)
    cen = x - jnp.mean(x, axis=-1, keepdims=True)
    inv = lax.rsqrt(jnp.mean(cen * cen, axis=-1, keepdims=True) + EPS)
    h = (cen * inv * w_ref[...].astype(F32) + b_ref[...].astype(F32)).astype(BF16)

    @pl.when(pl.program_id(0) == 0)
    def _():
        ha_ref[...] = h

    @pl.when(pl.program_id(0) == 1)
    def _():
        hb_ref[...] = h


def layer_norm(x, w, b):
    rows, width = x.shape
    tm = rows // 2
    vec = pl.BlockSpec((1, width), lambda i: (0, 0))
    half = pl.BlockSpec((tm, width), lambda i: (0, 0))
    return pl.pallas_call(
        ln_body,
        grid=(2,),
        in_specs=[pl.BlockSpec((tm, width), lambda i: (i, 0)), vec, vec],
        out_specs=[half, half],
        out_shape=[jax.ShapeDtypeStruct((tm, width), BF16)] * 2,
        compiler_params=params(1, 24),
        cost_estimate=pl.CostEstimate(flops=rows * width * 12, bytes_accessed=rows * width * 4, transcendentals=0),
        name="ln_rows",
    )(x, w, b)


def qkv_body(hd, n_src, with_kv, c_ref, t_ref, *refs):
    h_refs = refs[:n_src]
    refs = refs[n_src:]
    wq_ref, bq_ref, cos_ref, sin_ref = refs[:4]
    refs = refs[4:]
    if with_kv:
        wk_ref, wv_ref, bk_ref, bv_ref, q_ref, kv_ref, tc, ts, wkv = refs
    else:
        q_ref, tc, ts = refs
    tm = h_refs[0].shape[0]

    def rope(t, rows):
        t = t.astype(BF16).astype(F32)
        return (t * tc[rows, :] + pltpu.roll(t, hd // 2, 1) * ts[rows, :]).astype(BF16)

    @pl.when(pl.program_id(0) == 0)
    def _():
        for n in range(n_src):
            rows = slice(n * tm, (n + 1) * tm)
            tc[rows, :], ts[rows, :] = tile_tables(cos_ref, sin_ref, tm, t_ref[n])
        if with_kv:
            wkv[:, :hd] = wk_ref[...]
            wkv[:, hd:] = wv_ref[...]
            for n in range(n_src):
                rows = slice(n * tm, (n + 1) * tm)
                kv = dot(h_refs[n][...], wkv[...])
                kv_ref[rows, :hd] = rope(kv[:, :hd] + bk_ref[...].astype(F32), rows)
                kv_ref[rows, hd:] = (kv[:, hd:] + bv_ref[...].astype(F32)).astype(BF16)

    for n in range(n_src):
        rows = slice(n * tm, (n + 1) * tm)
        q = dot(h_refs[n][...], wq_ref[...]) + bq_ref[...].astype(F32)
        for k in range(q_ref.shape[0]):
            q_ref[k, rows, :] = rope(q[:, k * hd:(k + 1) * hd], rows)


def qkv_proj(core, tids, hs, wq, bq, kv, cos_t, sin_t, nh, hd, per=2):
    tm, width = hs[0].shape
    n_src = len(hs)
    rows = tm * n_src
    steps = nh // per
    ins = [whole((tm, width))] * n_src
    ins += [pl.BlockSpec((width, per * hd), lambda i, c, t: (0, c[0] * steps + i)),
            pl.BlockSpec((1, per * hd), lambda i, c, t: (0, c[0] * steps + i)), whole(cos_t.shape), whole(sin_t.shape)]
    args = [*hs, wq, bq, cos_t, sin_t]
    outs = [pl.BlockSpec((per, rows, hd), lambda i, c, t: (i, 0, 0))]
    shapes = [jax.ShapeDtypeStruct((nh, rows, hd), BF16)]
    scratch = [pltpu.VMEM((rows, hd), F32), pltpu.VMEM((rows, hd), F32)]
    if kv is not None:
        ins += [pl.BlockSpec((width, hd), lambda i, c, t: (0, c[0]))] * 2
        ins += [pl.BlockSpec((1, hd), lambda i, c, t: (0, c[0]))] * 2
        args += list(kv)
        outs += [whole((rows, 2 * hd))]
        shapes += [jax.ShapeDtypeStruct((rows, 2 * hd), BF16)]
        scratch += [pltpu.VMEM((width, 2 * hd), BF16)]
    return pl.pallas_call(
        functools.partial(qkv_body, hd, n_src, kv is not None),
        grid_spec=pltpu.PrefetchScalarGridSpec(
            num_scalar_prefetch=2, grid=(steps,), in_specs=ins, out_specs=outs, scratch_shapes=scratch),
        out_shape=shapes,
        compiler_params=params(1, 32),
        cost_estimate=pl.CostEstimate(flops=2 * rows * width * nh * hd, bytes_accessed=8 << 20, transcendentals=0),
        name="qkv_proj",
    )(core, tids, *args)


def do_body(hd, n_src, c_ref, *refs):
    d_refs = refs[:n_src]
    wo_ref, o_ref = refs[n_src:]
    off = 0
    for d in d_refs:
        rows = slice(off, off + d.shape[0])
        r = dot_nt(d[...], wo_ref[...]).astype(BF16)
        for k in range(o_ref.shape[0]):
            o_ref[k, rows, :] = r[:, k * hd:(k + 1) * hd]
        off += d.shape[0]


def do_proj(core, ds, wo, nh, hd, per=2):
    width = ds[0].shape[1]
    rows = sum(d.shape[0] for d in ds)
    steps = nh // per
    return pl.pallas_call(
        functools.partial(do_body, hd, len(ds)),
        grid_spec=pltpu.PrefetchScalarGridSpec(
            num_scalar_prefetch=1, grid=(steps,),
            in_specs=[whole(d.shape) for d in ds] + [pl.BlockSpec((per * hd, width), lambda i, c: (c[0] * steps + i, 0))],
            out_specs=pl.BlockSpec((per, rows, hd), lambda i, c: (i, 0, 0))),
        out_shape=jax.ShapeDtypeStruct((nh, rows, hd), BF16),
        compiler_params=params(1, 32),
        cost_estimate=pl.CostEstimate(flops=2 * rows * width * nh * hd, bytes_accessed=6 << 20, transcendentals=0),
        name="do_proj",
    )(core, *ds, wo)


def prep_body(hd, tile, n_src, ids, *refs):
    kv_refs = refs[:n_src]
    ks, vs, kt, vt = refs[n_src:]
    s = 0
    for ref in kv_refs:
        for r in range(ref.shape[0] // tile):
            p = ids[s]
            k = ref[r * tile:(r + 1) * tile, :hd]
            v = ref[r * tile:(r + 1) * tile, hd:]
            ks[p] = k
            vs[p] = v
            kt[p] = k.T
            vt[p] = v.T
            s += 1


def kv_prep(ids, kvs, hd, tile):
    pieces = sum(a.shape[0] for a in kvs) // tile
    out = [(pieces, tile, hd)] * 2 + [(pieces, hd, tile)] * 2
    return pl.pallas_call(
        functools.partial(prep_body, hd, tile, len(kvs)),
        grid_spec=pltpu.PrefetchScalarGridSpec(
            num_scalar_prefetch=1, grid=(1,),
            in_specs=[whole(a.shape) for a in kvs], out_specs=[whole(o) for o in out]),
        out_shape=[jax.ShapeDtypeStruct(o, BF16) for o in out],
        compiler_params=params(1, 24),
        cost_estimate=pl.CostEstimate(flops=1 << 20, bytes_accessed=3 << 20, transcendentals=0),
        name="kv_prep",
    )(ids, *kvs)


def attn_body(nh, hd, tile, pieces, scale, last, zero, natural, n_out, ids, tids, rel, *refs):
    refs = list(refs)

    def take(n):
        got = refs[:n]
        del refs[:n]
        return got

    q_ref, do_ref, ks, vs, kt, vt, cos_ref, sin_ref = take(8)
    if not zero:
        dki_ref, dvi_ref = take(2)
    keep_refs = take(n_out)
    send_refs = take(n_out)
    dqt_refs = take(n_out)
    if natural:
        o_refs = take(n_out)
        dq_refs = take(n_out)
    if last:
        dkvt_ref, dkv0_ref, dkv1_ref = take(3)
    dk_ref, dv_ref = take(2)
    ps, dps, ms, pb, dsb, ot, dqt = refs
    step = pl.program_id(0)
    steps = pl.num_programs(0)
    tq = nh * tile
    c = scale * LOG2E

    @pl.when(step == 0)
    def _():
        dk_ref[...] = jnp.zeros_like(dk_ref) if zero else dki_ref[...]
        dv_ref[...] = jnp.zeros_like(dv_ref) if zero else dvi_ref[...]

    i = ids[step]

    def first(j, carry, diag):
        m, l, dl = carry
        kj = ks[j]
        vj = vs[j]
        m_new, l_new, d_new = [], [], []
        for n in range(nh):
            lanes = slice(n * tile, (n + 1) * tile)
            s = dot_nt(kj, q_ref[n]) * c
            if diag:
                key = lax.broadcasted_iota(jnp.int32, (tile, tile), 0)
                qry = lax.broadcasted_iota(jnp.int32, (tile, tile), 1)
                s = jnp.where(key <= qry, s, NEG)
            dpb = dot_nt(vj, do_ref[n]).astype(BF16)
            dps[j, :, lanes] = dpb
            mo = m[:, lanes]
            mn = jnp.maximum(mo, jnp.max(s, axis=0, keepdims=True))
            p = jnp.exp2(s - mn)
            ps[j, :, lanes] = p
            al = jnp.exp2(mo - mn)
            m_new.append(mn)
            l_new.append(l[:, lanes] * al + jnp.sum(p, axis=0, keepdims=True))
            d_new.append(dl[:, lanes] * al + jnp.sum(p * dpb.astype(F32), axis=0, keepdims=True))
        m = jnp.concatenate(m_new, axis=1)
        ms[j] = m
        return m, jnp.concatenate(l_new, axis=1), jnp.concatenate(d_new, axis=1)

    init = (jnp.full((1, tq), NEG, F32), jnp.zeros((1, tq), F32), jnp.zeros((1, tq), F32))
    carry = lax.fori_loop(0, i, lambda j, cr: first(j, cr, False), init)
    m, l, dl = first(i, carry, True)
    inv = 1.0 / l
    delta = dl * inv
    ot[...] = jnp.zeros_like(ot)
    dqt[...] = jnp.zeros_like(dqt)

    def second(j, carry):
        f = jnp.exp2(ms[j] - m) * inv
        for n in range(nh):
            lanes = slice(n * tile, (n + 1) * tile)
            p = ps[j, :, lanes] * f[:, lanes]
            pb[:, lanes] = p.astype(BF16)
            dsb[:, lanes] = (p * (dps[j, :, lanes].astype(F32) - delta[:, lanes])).astype(BF16)
        ot[...] += dot(vt[j], pb[...])
        dqt[...] += dot(kt[j], dsb[...])
        dv_ref[j] += dot(pb[...], do_ref[...].reshape(tq, hd))
        dk_ref[j] += dot(dsb[...], q_ref[...].reshape(tq, hd))
        return carry

    lax.fori_loop(0, i + 1, second, 0)
    tc, ts = tile_tables(cos_ref, sin_ref, tile, tids[step])
    cos_t = tc.T[:hd // 2]
    sin_t = ts.T[hd // 2:]
    core = rel[pieces]

    def write(k):
        for n in range(nh):
            lanes = slice(n * tile, (n + 1) * tile)
            o_t = ot[:, lanes].astype(BF16)
            half = slice((n % (nh // 2)) * hd, (n % (nh // 2) + 1) * hd)

            @pl.when(core == n // (nh // 2))
            def _():
                keep_refs[k][half, :] = o_t

            @pl.when(core != n // (nh // 2))
            def _():
                send_refs[k][half, :] = o_t

            g = (dqt[:, lanes] * scale).astype(BF16).astype(F32)
            a = g[:hd // 2]
            e = g[hd // 2:]
            g = jnp.concatenate([a * cos_t + e * sin_t, e * cos_t - a * sin_t], axis=0).astype(BF16)
            cols = slice(n * hd, (n + 1) * hd)
            dqt_refs[k][cols, :] = g
            if natural:
                o_refs[k][:, cols] = o_t.T
                dq_refs[k][:, cols] = g.T

    if n_out == 1:
        write(0)
    else:
        for k in range(n_out):
            pl.when(step // (steps // n_out) == k)(functools.partial(write, k))

    if last:
        @pl.when(step == steps - 1)
        def _():
            for s in range(pieces):
                cols = slice(s * tile, (s + 1) * tile)
                p = rel[s]
                ct, st = tile_tables(cos_ref, sin_ref, tile, s)
                g = (dk_ref[p] * scale).astype(BF16).astype(F32)
                gk = (g * ct - pltpu.roll(g, hd // 2, 1) * st).astype(BF16)
                gv = dv_ref[p].astype(BF16)
                dkvt_ref[:hd, cols] = gk.T
                dkvt_ref[hd:, cols] = gv.T
                if s < 4:
                    rows = slice((s % 2) * tile, (s % 2 + 1) * tile)
                    out = (dkv0_ref, dkv1_ref)[s // 2]
                    out[rows, :hd] = gk
                    out[rows, hd:] = gv


def attention(ids, tids, rel, q, do, keys, cos_t, sin_t, acc, scale, tile, n_out, last, natural):
    nh, rows, hd = q.shape
    pieces = keys[0].shape[0]
    tq = nh * tile
    steps = rows // tile
    per = steps // n_out
    zero = acc is None
    heads = pl.BlockSpec((nh, tile, hd), lambda i, a, b, c: (0, i, 0))

    def clip(i, n):
        return jnp.clip(i - n * per, 0, per - 1)

    def cols(n, r):
        return pl.BlockSpec((r, tile), lambda i, a, b, c: (0, clip(i, n)))

    def out(n):
        return pl.BlockSpec((tile, nh * hd), lambda i, a, b, c: (clip(i, n), 0))

    def shape(*dims):
        return jax.ShapeDtypeStruct(dims, BF16)

    outs = [cols(n, nh * hd // 2) for n in range(n_out)] * 2 + [cols(n, nh * hd) for n in range(n_out)]
    shapes = [shape(nh * hd // 2, per * tile)] * (2 * n_out) + [shape(nh * hd, per * tile)] * n_out
    if natural:
        outs += [out(n) for n in range(n_out)] * 2
        shapes += [shape(per * tile, nh * hd)] * (2 * n_out)
    ins = [heads, heads] + [whole(a.shape) for a in keys] + [whole(cos_t.shape), whole(sin_t.shape)]
    args = [q, do, *keys, cos_t, sin_t]
    sums = (pieces, tile, hd)
    if not zero:
        ins += [whole(sums), whole(sums)]
        args += list(acc)
    scratch = []
    if last:
        dims = [(2 * hd, pieces * tile), (2 * tile, 2 * hd), (2 * tile, 2 * hd)]
        outs += [whole(d) for d in dims]
        shapes += [shape(*d) for d in dims]
        scratch += [pltpu.VMEM(sums, F32), pltpu.VMEM(sums, F32)]
    else:
        outs += [whole(sums), whole(sums)]
        shapes += [jax.ShapeDtypeStruct(sums, F32)] * 2
    scratch += [
        pltpu.VMEM((pieces, tile, tq), F32), pltpu.VMEM((pieces, tile, tq), BF16), pltpu.VMEM((pieces, 1, tq), F32),
        pltpu.VMEM((tile, tq), BF16), pltpu.VMEM((tile, tq), BF16), pltpu.VMEM((hd, tq), F32), pltpu.VMEM((hd, tq), F32)]
    return pl.pallas_call(
        functools.partial(attn_body, nh, hd, tile, pieces, scale, last, zero, natural, n_out),
        grid_spec=pltpu.PrefetchScalarGridSpec(
            num_scalar_prefetch=3, grid=(steps,), in_specs=ins, out_specs=outs, scratch_shapes=scratch),
        out_shape=shapes,
        compiler_params=params(1, 44),
        cost_estimate=pl.CostEstimate(flops=rows * pieces * tile * nh * hd * 12, bytes_accessed=8 << 20,
                                      transcendentals=rows * pieces * tile * nh),
        name="attn_fwd_bwd",
    )(ids, tids, rel, *args)


def y_body(x_ref, om_ref, ot_ref, w_ref, b_ref, y_ref, z_ref):
    @pl.when(pl.program_id(0) == 0)
    def _():
        z_ref[...] = dot(om_ref[...], w_ref[...])

    @pl.when(pl.program_id(0) == 1)
    def _():
        z = z_ref[...] + dot(ot_ref[...], w_ref[...])
        y_ref[...] = (x_ref[...].astype(F32) + (z + b_ref[...].astype(F32))).astype(BF16)


def y_rows(core, x, o_mine, o_theirs, wo, bo):
    rows, width = x.shape
    qw = o_mine.shape[1]
    return pl.pallas_call(
        lambda c, *refs: y_body(*refs),
        grid_spec=pltpu.PrefetchScalarGridSpec(
            num_scalar_prefetch=1, grid=(2,),
            in_specs=[whole((rows, width)), whole((rows, qw)), whole((rows, qw)),
                      pl.BlockSpec((qw, width), lambda i, c: (c[0] + i - 2 * c[0] * i, 0)), whole((1, width))],
            out_specs=whole((rows, width)),
            scratch_shapes=[pltpu.VMEM((rows, width), F32)]),
        out_shape=jax.ShapeDtypeStruct((rows, width), BF16),
        compiler_params=params(1, 32),
        cost_estimate=pl.CostEstimate(flops=4 * rows * width * qw, bytes_accessed=8 << 20, transcendentals=0),
        name="y_rows",
    )(core, x, o_mine, o_theirs, wo, bo)


def dx_body(hd, c_ref, x_ref, d_ref, qm_ref, qt_ref, km_ref, kt_ref, wq_ref, wk_ref, wv_ref, g_ref, dx_ref, v_ref, acc):
    step = pl.program_id(0)
    qw = qm_ref.shape[1]

    def rows(t):
        return jnp.sum(t, axis=0, keepdims=True)

    def put(side, q, k):
        q = rows(q.astype(F32))
        k = rows(k.astype(F32))
        for h in range(2):
            @pl.when(side == h)
            def _():
                v_ref[3:4, h * qw:(h + 1) * qw] = q
                v_ref[4:5, h * hd:(h + 1) * hd] = k[:, :hd]
                v_ref[5:6, h * hd:(h + 1) * hd] = k[:, hd:]

    @pl.when(step == 0)
    def _():
        v_ref[...] = jnp.zeros_like(v_ref)
        acc[...] = dot_nt(qm_ref[...], wq_ref[...])
        put(c_ref[0], qm_ref[...], km_ref[...])

    @pl.when(step == 1)
    def _():
        acc[...] += dot_nt(qt_ref[...], wq_ref[...])
        put(1 - c_ref[0], qt_ref[...], kt_ref[...])
        mine = pl.ds(pl.multiple_of(c_ref[0] * hd, 128), hd)
        other = pl.ds(pl.multiple_of((1 - c_ref[0]) * hd, 128), hd)
        km = km_ref[...]
        kt = kt_ref[...]
        tm = 128
        for r in range(0, acc.shape[0], tm):
            s = slice(r, r + tm)
            dh = acc[s, :] + (dot_nt(km[s, :hd], wk_ref[:, mine]) + dot_nt(kt[s, :hd], wk_ref[:, other])
                              + dot_nt(km[s, hd:], wv_ref[:, mine]) + dot_nt(kt[s, hd:], wv_ref[:, other]))
            dh = dh.astype(BF16).astype(F32)
            x = x_ref[s, :].astype(F32)
            cen = x - jnp.mean(x, axis=-1, keepdims=True)
            inv = lax.rsqrt(jnp.mean(cen * cen, axis=-1, keepdims=True) + EPS)
            xh = cen * inv
            a = dh * g_ref[...].astype(F32)
            d = d_ref[s, :].astype(F32)
            dx = inv * (a - jnp.mean(a, axis=-1, keepdims=True) - xh * jnp.mean(a * xh, axis=-1, keepdims=True))
            dx_ref[s, :] = (d + dx).astype(BF16)
            v_ref[0:1, :] += rows(dh * xh)
            v_ref[1:2, :] += rows(dh)
            v_ref[2:3, :] += rows(d)


def dx_rows(core, x, d, qm, qt, km, kt, wq, wk, wv, g, hd):
    rows, width = x.shape
    qw = qm.shape[1]
    kvw = wk.shape[1]
    return pl.pallas_call(
        functools.partial(dx_body, hd),
        grid_spec=pltpu.PrefetchScalarGridSpec(
            num_scalar_prefetch=1, grid=(2,),
            in_specs=[whole((rows, width))] * 2 + [whole((rows, qw))] * 2 + [whole((rows, 2 * hd))] * 2 + [
                pl.BlockSpec((width, qw), lambda i, c: (0, c[0] + i - 2 * c[0] * i)),
                whole((width, kvw)), whole((width, kvw)), whole((1, width))],
            out_specs=[whole((rows, width)), whole((8, width))],
            scratch_shapes=[pltpu.VMEM((rows, width), F32)]),
        out_shape=[jax.ShapeDtypeStruct((rows, width), BF16), jax.ShapeDtypeStruct((8, width), F32)],
        compiler_params=params(1),
        cost_estimate=pl.CostEstimate(flops=4 * rows * width * (qw + 2 * hd), bytes_accessed=12 << 20, transcendentals=0),
        name="dx_rows",
    )(core, x, d, qm, qt, km, kt, wq, wk, wv, g)


def dw_body(h_offs, q_offs, s_ref, *refs):
    refs = list(refs)
    n_h, n_q = len(h_offs), len(q_offs)
    h_refs = refs[:n_h]
    q_refs = refs[n_h:n_h + n_q]
    kv_ref, o_ref = refs[n_h + n_q:]
    steps = pl.num_programs(0)
    part = h_refs[0].shape[1] // 2

    def run(lhs):
        acc = None
        for r, off in zip(h_refs, h_offs):
            t = dot(lhs(off, r.shape[0]), r[...])
            acc = t if acc is None else acc + t
        o_ref[0] = acc[:, :part].T
        o_ref[1] = acc[:, part:].T

    def from_q(off, n):
        for r, o in zip(q_refs, q_offs):
            if o <= off < o + r.shape[1]:
                return r[:, off - o:off - o + n]

    @pl.when(pl.program_id(0) < steps - 1)
    def _():
        run(from_q)

    @pl.when(pl.program_id(0) == steps - 1)
    def _():
        run(lambda off, n: kv_ref[:, off:off + n])


def dw_rows(sel, hs, qts, kvt, part, h_offs, q_offs, tn=256):
    kvw, tokens = kvt.shape
    qw = qts[0].shape[0]
    steps = qw // tn
    ins = [pl.BlockSpec((h.shape[0], 2 * part), lambda i, s: (0, s[0])) for h in hs]
    ins += [pl.BlockSpec((tn, q.shape[1]), lambda i, s: (jnp.minimum(i, steps - 1), 0)) for q in qts]
    ins += [whole(kvt.shape)]
    return pl.pallas_call(
        functools.partial(dw_body, h_offs, q_offs),
        grid_spec=pltpu.PrefetchScalarGridSpec(
            num_scalar_prefetch=1, grid=(steps + 1,), in_specs=ins,
            out_specs=pl.BlockSpec((2, part, tn), lambda i, s: (0, 0, i))),
        out_shape=jax.ShapeDtypeStruct((2, part, qw + kvw), F32),
        compiler_params=params(1),
        cost_estimate=pl.CostEstimate(flops=4 * part * tokens * (qw + kvw), bytes_accessed=12 << 20, transcendentals=0),
        name="dw_rows",
    )(sel, *hs, *qts, kvt)


def merge_body(s_ref, m_ref, t_ref, q_ref, k_ref, v_ref):
    core = s_ref[0]
    qw = q_ref.shape[1] // 2
    hd = k_ref.shape[1] // 2
    for side, r in ((core, m_ref), (1 - core, t_ref)):
        for h in range(2):
            @pl.when(side == h)
            def _():
                q_ref[:, h * qw:(h + 1) * qw] = r[0, :, :qw]
                k_ref[:, h * hd:(h + 1) * hd] = r[0, :, qw:qw + hd]
                v_ref[:, h * hd:(h + 1) * hd] = r[0, :, qw + hd:]


def merge_cols(core, both, got, qw, hd, tm=128):
    part, cols = got.shape[1:]
    outs = [(part, 2 * qw), (part, 2 * hd), (part, 2 * hd)]
    return pl.pallas_call(
        merge_body,
        grid_spec=pltpu.PrefetchScalarGridSpec(
            num_scalar_prefetch=1, grid=(part // tm,),
            in_specs=[pl.BlockSpec((1, tm, cols), lambda i, s: (s[0], i, 0)), pl.BlockSpec((1, tm, cols), lambda i, s: (0, i, 0))],
            out_specs=[pl.BlockSpec((tm, o[1]), lambda i, s: (i, 0)) for o in outs]),
        out_shape=[jax.ShapeDtypeStruct(o, F32) for o in outs],
        compiler_params=params(1, 24),
        cost_estimate=pl.CostEstimate(flops=1 << 20, bytes_accessed=6 << 20, transcendentals=0),
        name="merge_cols",
    )(core, both, got)


def dwo_body(offs, s_ref, *refs):
    n_src = len(offs)
    om = refs[:n_src]
    og = refs[n_src:2 * n_src]
    d_refs = refs[2 * n_src:3 * n_src]
    out_ref, at = refs[3 * n_src:]

    @pl.when(pl.program_id(0) == 0)
    def _():
        for a, b, off in zip(om, og, offs):
            at[:, off:off + a.shape[1]] = jnp.where(s_ref[0] == 1, a[...], b[...])

    acc = None
    for r, off in zip(d_refs, offs):
        t = dot(at[:, off:off + r.shape[0]], r[...])
        acc = t if acc is None else acc + t
    out_ref[...] = acc


def dwo_rows(sel, o_mine, o_got, ds, offs, tn=512):
    part = o_mine[0].shape[0]
    width = ds[0].shape[1]
    tokens = sum(d.shape[0] for d in ds)
    ins = [whole(o.shape) for o in o_mine + o_got]
    ins += [pl.BlockSpec((d.shape[0], tn), lambda i, s: (0, i)) for d in ds]
    return pl.pallas_call(
        functools.partial(dwo_body, offs),
        grid_spec=pltpu.PrefetchScalarGridSpec(
            num_scalar_prefetch=1, grid=(width // tn,), in_specs=ins,
            out_specs=pl.BlockSpec((part, tn), lambda i, s: (0, i)),
            scratch_shapes=[pltpu.VMEM((part, tokens), BF16)]),
        out_shape=jax.ShapeDtypeStruct((part, width), F32),
        compiler_params=params(1),
        cost_estimate=pl.CostEstimate(flops=2 * part * tokens * width, bytes_accessed=10 << 20, transcendentals=0),
        name="dwo_rows",
    )(sel, *o_mine, *o_got, *ds)


def after(values, *earlier):
    n = len(values)
    return lax.optimization_barrier(tuple(values) + tuple(earlier))[:n]


def solution(mesh):
    groups = mesh.shape['cp']
    row_spec = P('dp', 'cp', None)
    mat_spec = P(('dp', 'cp'), None)
    vec_spec = P('dp')
    near = [(i, i ^ 1) for i in range(groups)]
    far = [(i, i ^ 2) for i in range(groups)]

    def swap(v):
        return lax.ppermute(v, 'cp', near)

    def cross(v):
        return lax.ppermute(v, 'cp', far)

    def device_fn(x_in, ln_w, ln_b, w_q, b_q, w_k, b_k, w_v, b_v, w_o, b_o, long_factor, dy_out):
        rank = lax.axis_index('cp').astype(jnp.int32)
        core = rank & 1
        chip = rank >> 1
        x = x_in[0]
        d0 = dy_out[0]
        tokens, width = x.shape
        piece = tokens // 2
        hd = 2 * long_factor.shape[0]
        kv_heads = w_k.shape[1] // hd
        nh = w_q.shape[1] // hd // kv_heads
        scale = hd ** -0.5
        part = width // groups
        core_v = core[None]

        h0a, h0b = layer_norm(x, ln_w[None], ln_b[None])
        h1a = swap(h0a)
        h1b = swap(h0b)
        d1 = swap(d0)

        blocks = jnp.stack([rank, rank ^ 1, rank ^ 2, rank ^ 3])
        rel = jnp.stack([blocks, 2 * groups - 1 - blocks], axis=1).reshape(2 * groups)
        cos_t, sin_t = rope_tables(rel * piece, piece, long_factor)
        rel = jnp.concatenate([rel, core_v])

        def tile_ids(*t):
            return jnp.array(t, dtype=jnp.int32)

        def pieces_of(*t):
            return jnp.stack([rel[n] for n in t])

        def project(hs, kv, *t):
            return qkv_proj(core_v, tile_ids(*t), hs, w_q, b_q[None], kv, cos_t, sin_t, nh, hd)

        def attend(q, do, acc, last, natural, *t):
            return attention(pieces_of(*t), tile_ids(*t), rel, q, do, keys, cos_t, sin_t, acc, scale, piece, 2, last, natural)

        q01, kv01 = project([h0a, h0b, h1a, h1b], (w_k, w_v, b_k[None], b_v[None]), 0, 1, 2, 3)
        kv23 = cross(kv01)
        h0b_s, d0_s = after((h0b, d0), kv01)
        h2b = cross(h0b_s)
        d2b = cross(d0_s[piece:])
        h0a_s, = after((h0a,), h0b_s)
        h2a = cross(h0a_s)
        d2a = cross(d0_s[:piece])
        do01 = do_proj(core_v, [d0, d1], w_o, nh, hd)
        kv23, = after((kv23,), do01)
        keys = kv_prep(rel, [kv01, kv23], hd, piece)
        k0, k1, s0, s1, qt0, qt1, o0, o1, dq0, dq1, dk, dv = attend(q01, do01, None, False, True, 0, 1, 2, 3)

        h2b, d2b = after((h2b, d2b), o0)
        h3b = swap(h2b)
        d3b = swap(d2b)
        o1_got = swap(o1)
        dq1_got = swap(dq1)
        g0 = swap(s1)
        g1 = swap(s0)
        q2, = project([h2b, h3b], None, 5, 7)
        do2 = do_proj(core_v, [d2b, d3b], w_o, nh, hd)
        k2b, k3b, s2b, s3b, qt2b, qt3b, dk, dv = attend(q2, do2, (dk, dv), False, False, 5, 7)

        h2a, d2a = after((h2a, d2a), k2b)
        h3a = swap(h2a)
        d3a = swap(d2a)
        g2b = swap(s3b)
        g3b = swap(s2b)
        q3, = project([h2a, h3a], None, 4, 6)
        do3 = do_proj(core_v, [d2a, d3a], w_o, nh, hd)
        k2a, k3a, s2a, s3a, qt2a, qt3a, dkv_t, dkv0, dkv1 = attend(q3, do3, (dk, dv), True, False, 4, 6)
        dkv_got = swap(dkv1)
        g2a = swap(s3a)
        g3a = swap(s2a)

        hs = [h0a, h0b, h1a, h1b, h2a, h2b, h3a, h3b]
        h_offs = [n * piece for n in range(8)]
        offs = [0, tokens, 2 * tokens, 2 * tokens + piece, 3 * tokens, 3 * tokens + piece]
        d_w = dw_rows(chip[None], hs, [qt0, qt1, qt2a, qt2b, qt3a, qt3b], dkv_t, part, h_offs, offs)
        got = swap(lax.dynamic_slice(d_w, (1 - core, 0, 0), (1, part, d_w.shape[2])))
        dkv_got, = after((dkv_got,), d_w)
        dx, vec = dx_rows(core_v, x, d0, dq0, dq1_got, dkv0, dkv_got, w_q, w_k, w_v, ln_w[None], hd)
        vec = vec + swap(vec)
        vec_x = cross(vec)
        g2a, g3a = after((g2a, g3a), dx)
        d_wo = dwo_rows((core == chip).astype(jnp.int32)[None], [k0, k1, k2a, k2b, k3a, k3b], [g0, g1, g2a, g2b, g3a, g3b],
                        [d0, d1, d2a, d2b, d3a, d3b], offs)
        y = y_rows(core_v, x, o0, o1_got, w_o, b_o[None])
        got, = after((got,), d_wo)
        d_wq, d_wk, d_wv = merge_cols(core_v, d_w, got, nh * hd, hd)
        vec = vec + vec_x
        kvw = kv_heads * hd
        d_lnw, d_lnb, d_bo, d_bq = (vec[n] for n in range(4))
        d_bk, d_bv = (vec[n, :kvw] for n in (4, 5))
        return (y[None], dx[None], d_wq, d_wk, d_wv, d_wo, d_lnw, d_lnb, d_bq, d_bk, d_bv, d_bo)

    in_specs = (row_spec,) + (P(),) * 11 + (row_spec,)
    out_specs = (row_spec, row_spec) + (mat_spec,) * 4 + (vec_spec,) * 6
    return jax.shard_map(device_fn, mesh=mesh, in_specs=in_specs, out_specs=out_specs, check_vma=False)
```

```python
import functools
import math
import jax
import jax.numpy as jnp
from jax import lax
from jax.experimental import pallas as pl
from jax.experimental.pallas import tpu as pltpu
from jax.sharding import PartitionSpec as P

EPS = 1e-5
THETA = 10000.0
ROPE_SCALE = math.sqrt(1.0 + math.log(32.0) / math.log(4096.0))
LOG2E = math.log2(math.e)
NEG = -1e30
F32 = jnp.float32
BF16 = jnp.bfloat16


def dot(a, b):
    return lax.dot_general(a, b, (((1,), (0,)), ((), ())), preferred_element_type=F32)


def dot_nt(a, b):
    return lax.dot_general(a, b, (((1,), (1,)), ((), ())), preferred_element_type=F32)


def dot_tn(a, b):
    return lax.dot_general(a, b, (((0,), (0,)), ((), ())), preferred_element_type=F32)


def rope_tables(starts, piece, long_factor):
    half_dim = long_factor.shape[0]
    exponent = jnp.arange(half_dim, dtype=F32) * (1.0 / half_dim)
    inv_freq = 1.0 / (long_factor * THETA ** exponent)
    positions = jnp.concatenate([jnp.arange(piece, dtype=jnp.int32), starts])
    angle = positions.astype(F32)[:, None] * inv_freq[None, :]
    cos_t = jnp.cos(angle)
    sin_t = jnp.sin(angle)
    return jnp.concatenate([cos_t, cos_t], axis=1), jnp.concatenate([-sin_t, sin_t], axis=1)


def tile_tables(cos_ref, sin_ref, piece, t):
    ca = cos_ref[pl.ds(piece + t, 1), :] * ROPE_SCALE
    sa = sin_ref[pl.ds(piece + t, 1), :] * ROPE_SCALE
    cb = cos_ref[:piece, :]
    sb = sin_ref[:piece, :]
    return ca * cb - sa * sb, sa * cb + ca * sb


MESH = pl.DeviceIdType.MESH


def mega_body(nh, hd, tile, scale,
              x_hbm, d_hbm, wq_hbm, wk_hbm, wv_hbm, wo_hbm, lnw1, lnb1, bq1, bo1, bk1, bv1, cos_ref, sin_ref,
              y_hbm, dx_hbm, dwq_hbm, dwk_hbm, dwv_hbm, dwo_hbm, vec_ref,
              H, D, KV, KT, VT, WQ, WO, WKV, DK, DV, KEEP, SEND, GOT, DWT, ONA, ONS, ONR, DQA, DQS, DQR, DKA, DKS, DKR,
              DWR, VS, VR, SM, fs, fr, ns, nr, ls):
    rank = lax.axis_index('cp')
    core = rank % 2
    chip = rank // 2
    near = rank + 1 - 2 * core
    far = rank + 2 - 4 * chip
    tq = nh * tile
    qw = nh * hd
    width = H.shape[2]
    part = width // 4
    third = nh // 2
    lnw, lnb, bq, bo, bk, bv = (SM.at[n:n + 1, :] for n in range(6))
    for n, r in enumerate((lnw1, lnb1, bq1, bo1, bk1, bv1)):
        SM[n:n + 1, :r.shape[0]] = r[...].astype(F32).reshape(1, r.shape[0])

    def local(src, dst, n):
        return pltpu.make_async_copy(src, dst, ls.at[n])

    def remote(src, dst, send, recv, n, to):
        return pltpu.make_async_remote_copy(src_ref=src, dst_ref=dst, send_sem=send.at[n], recv_sem=recv.at[n],
                                            device_id={'cp': to}, device_id_type=MESH)

    def lanes_of(i, n):
        return pl.ds(pl.multiple_of(i * n, 128), n)

    def piece_of(t):
        k = t // 2
        b = (rank % 2 + k % 2) % 2 + 2 * ((rank // 2 + k // 2) % 2)
        return b + (t % 2) * (7 - 2 * b)

    def tile_of(p):
        up = p // 4
        b = p + up * (7 - 2 * p)
        k = (rank % 2 + b % 2) % 2 + 2 * ((rank // 2 + b // 2) % 2)
        return 2 * k + up

    def start_loads(X):
        mine = lanes_of(core, hd)
        return [local(x_hbm, X, 0), local(wk_hbm.at[:, mine], WKV.at[:, :hd], 1), local(wv_hbm.at[:, mine], WKV.at[:, hd:], 2),
                local(d_hbm, D.at[0:2], 3), local(wq_hbm.at[:, lanes_of(core, qw)], WQ, 4),
                local(wo_hbm.at[lanes_of(core, qw), :], WO, 5)]

    n_h = remote(H.at[0:2], H.at[2:4], ns, nr, 0, near)
    n_d = remote(D.at[0:2], D.at[2:4], ns, nr, 1, near)
    f_kv = remote(KV.at[0:4], KV.at[4:8], fs, fr, 0, far)
    f_h1 = remote(H.at[1], H.at[5], fs, fr, 1, far)
    f_d1 = remote(D.at[1], D.at[5], fs, fr, 2, far)
    f_h0 = remote(H.at[0], H.at[4], fs, fr, 3, far)
    f_d0 = remote(D.at[0], D.at[4], fs, fr, 4, far)
    n_h5 = remote(H.at[5], H.at[7], ns, nr, 2, near)
    n_d5 = remote(D.at[5], D.at[7], ns, nr, 3, near)
    n_h4 = remote(H.at[4], H.at[6], ns, nr, 4, near)
    n_d4 = remote(D.at[4], D.at[6], ns, nr, 5, near)
    n_o = remote(ONS, ONR, ns, nr, 6, near)
    n_q = remote(DQS, DQR, ns, nr, 7, near)
    n_k = remote(DKS, DKR, ns, nr, 8, near)
    n_v = remote(VS.at[0], VR.at[0], ns, nr, 10, near)
    f_v = remote(VS.at[1], VR.at[1], fs, fr, 5, far)

    def swapped(t):
        return t + 2 - 4 * ((t // 2) % 2)

    def n_s(t):
        return remote(SEND.at[t], GOT.at[swapped(t)], ns, nr, 11 + t, near)

    def n_s_in(t):
        return remote(SEND.at[swapped(t)], GOT.at[t], ns, nr, 11 + swapped(t), near)

    def head_phase(X):
        loads = start_loads(X)
        for c in loads:
            c.start()
        barrier = pltpu.get_barrier_semaphore()
        for to in (near, far):
            pl.semaphore_signal(barrier, inc=1, device_id={'cp': to}, device_id_type=MESH)
        pl.semaphore_wait(barrier, 2)
        loads[0].wait()
        gain = lnw[...]
        shift = lnb[...]

        def norm(r, _):
            rows = pl.ds(pl.multiple_of((r % 4) * 64, 64), 64)
            x = X[r // 4, rows, :].astype(F32)
            cen = x - jnp.mean(x, axis=-1, keepdims=True)
            inv = lax.rsqrt(jnp.mean(cen * cen, axis=-1, keepdims=True) + EPS)
            H[r // 4, rows, :] = (cen * inv * gain + shift).astype(BF16)
            return _

        lax.fori_loop(0, 8, norm, 0)
        n_h.start()
        loads[3].wait()
        n_d.start()
        loads[1].wait()
        loads[2].wait()
        loads[4].wait()
        loads[5].wait()

    pl.run_scoped(head_phase, pltpu.VMEM((2, tile, width), BF16))

    def attention_phase(Q, DO, PS, DPS, MS, PB, DSB, OT, DQT, DQTT):
        c = scale * LOG2E

        def rope(t, ct, st):
            t = t.astype(BF16).astype(F32)
            return (t * ct + pltpu.roll(t, hd // 2, 1) * st).astype(BF16)

        def kv_tile(t, _):
            ct, st = tile_tables(cos_ref, sin_ref, tile, t)
            kv = dot(H[t], WKV[...])
            KV[t, :, :hd] = rope(kv[:, :hd] + bk[0:1, lanes_of(core, hd)], ct, st)
            KV[t, :, hd:] = (kv[:, hd:] + bv[0:1, lanes_of(core, hd)]).astype(BF16)
            return _

        def project(t, slot):
            ct, st = tile_tables(cos_ref, sin_ref, tile, t)
            q = dot(H[t], WQ[...]) + bq[0:1, lanes_of(core, qw)]
            for n in range(nh):
                Q[slot, n] = rope(q[:, n * hd:(n + 1) * hd], ct, st)
            r = dot_nt(D[t], WO[...]).astype(BF16)
            for n in range(nh):
                DO[slot, n] = r[:, n * hd:(n + 1) * hd]

        def turn(t, _):
            KT[t] = KV[t, :, :hd].T
            VT[t] = KV[t, :, hd:].T
            return _

        lax.fori_loop(0, 2, kv_tile, 0)
        n_h.wait_recv()
        lax.fori_loop(2, 4, kv_tile, 0)
        f_kv.start()
        f_h1.start()
        f_d1.start()
        f_h0.start()
        f_d0.start()
        n_d.wait_recv()

        def first_four(t, _):
            project(t, t)
            return _

        lax.fori_loop(0, 4, first_four, 0)
        lax.fori_loop(0, 4, turn, 0)
        DK[...] = jnp.zeros_like(DK)
        DV[...] = jnp.zeros_like(DV)
        DWT[...] = jnp.zeros_like(DWT)
        f_kv.wait_recv()
        lax.fori_loop(4, 8, turn, 0)

        def one_tile(s, same):
            late = s // 4
            u = s % 4
            t = (1 - late) * ((u + 2) % 4) + late * (4 + (u % 2) * 2 + 1 - u // 2)
            slot = (1 - late) * t + late * u

            @pl.when(s == 3)
            def _():
                f_h1.wait_recv()
                f_d1.wait_recv()
                n_h5.start()
                n_d5.start()

            @pl.when(s == 5)
            def _():
                n_h5.wait_recv()
                n_d5.wait_recv()

            @pl.when(s == 6)
            def _():
                f_h0.wait_recv()
                f_d0.wait_recv()
                n_h4.start()
                n_d4.start()

            @pl.when(s == 7)
            def _():
                n_h4.wait_recv()
                n_d4.wait_recv()

            @pl.when(late == 1)
            def _():
                project(t, slot)

            i = piece_of(t)

            def first(j, carry, diag):
                m, l, dl = carry
                g = tile_of(j)
                kj = KV[g, :, :hd]
                vj = KV[g, :, hd:]
                m_new, l_new, d_new = [], [], []
                for n in range(nh):
                    lanes = slice(n * tile, (n + 1) * tile)
                    sc = dot_nt(kj, Q[slot, n]) * c
                    if diag:
                        key = lax.broadcasted_iota(jnp.int32, (tile, tile), 0)
                        qry = lax.broadcasted_iota(jnp.int32, (tile, tile), 1)
                        sc = jnp.where(key <= qry, sc, NEG)
                    dpb = dot_nt(vj, DO[slot, n]).astype(BF16)
                    DPS[j, :, lanes] = dpb
                    mo = m[:, lanes]
                    mn = jnp.maximum(mo, jnp.max(sc, axis=0, keepdims=True))
                    p = jnp.exp2(sc - mn)
                    PS[j, :, lanes] = p
                    al = jnp.exp2(mo - mn)
                    m_new.append(mn)
                    l_new.append(l[:, lanes] * al + jnp.sum(p, axis=0, keepdims=True))
                    d_new.append(dl[:, lanes] * al + jnp.sum(p * dpb.astype(F32), axis=0, keepdims=True))
                m = jnp.concatenate(m_new, axis=1)
                MS[j] = m
                return m, jnp.concatenate(l_new, axis=1), jnp.concatenate(d_new, axis=1)

            init = (jnp.full((1, tq), NEG, F32), jnp.zeros((1, tq), F32), jnp.zeros((1, tq), F32))
            carry = lax.fori_loop(0, i, lambda j, cr: first(j, cr, False), init)
            m, l, dl = first(i, carry, True)
            inv = 1.0 / l
            delta = dl * inv
            OT[...] = jnp.zeros_like(OT)
            DQT[...] = jnp.zeros_like(DQT)

            def second(j, carry):
                g = tile_of(j)
                f = jnp.exp2(MS[j] - m) * inv
                for n in range(nh):
                    lanes = slice(n * tile, (n + 1) * tile)
                    p = PS[j, :, lanes] * f[:, lanes]
                    PB[:, lanes] = p.astype(BF16)
                    DSB[:, lanes] = (p * (DPS[j, :, lanes].astype(F32) - delta[:, lanes])).astype(BF16)
                OT[...] += dot(VT[g], PB[...])
                DQT[...] += dot(KT[g], DSB[...])
                DV[g] += dot(PB[...], DO[slot].reshape(tq, hd))
                DK[g] += dot(DSB[...], Q[slot].reshape(tq, hd))
                return carry

            lax.fori_loop(0, i + 1, second, 0)
            ct, st = tile_tables(cos_ref, sin_ref, tile, t)
            cos_t = ct.T[:hd // 2]
            sin_t = st.T[hd // 2:]
            for n in range(nh):
                lanes = slice(n * tile, (n + 1) * tile)
                o_t = OT[:, lanes].astype(BF16)
                rows = slice((n % third) * hd, (n % third + 1) * hd)

                @pl.when(core == n // third)
                def _():
                    KEEP[t, rows, :] = o_t

                @pl.when(core != n // third)
                def _():
                    SEND[t, rows, :] = o_t

                gr = (DQT[:, lanes] * scale).astype(BF16).astype(F32)
                a = gr[:hd // 2]
                e = gr[hd // 2:]
                gr = jnp.concatenate([a * cos_t + e * sin_t, e * cos_t - a * sin_t], axis=0).astype(BF16)
                cols = slice(n * hd, (n + 1) * hd)
                DQTT[cols, :] = gr

                @pl.when(t // 2 == 0)
                def _():
                    ONA[t % 2, :, cols] = o_t.T
                    DQA[t % 2, :, cols] = gr.T

                @pl.when(t // 2 == 1)
                def _():
                    ONS[t % 2, :, cols] = o_t.T
                    DQS[t % 2, :, cols] = gr.T

            n_s(t).start()

            @pl.when(s == 1)
            def _():
                n_o.start()
                n_q.start()

            DWT[...] += dot(DQTT[...], H[t, :, lanes_of(chip, 2 * part)])
            return same

        lax.fori_loop(0, 8, one_tile, 0)

    pl.run_scoped(attention_phase,
                  pltpu.VMEM((4, nh, tile, hd), BF16), pltpu.VMEM((4, nh, tile, hd), BF16),
                  pltpu.VMEM((8, tile, tq), F32), pltpu.VMEM((8, tile, tq), BF16), pltpu.VMEM((8, 1, tq), F32),
                  pltpu.VMEM((tile, tq), BF16), pltpu.VMEM((tile, tq), BF16), pltpu.VMEM((hd, tq), F32), pltpu.VMEM((hd, tq), F32),
                  pltpu.VMEM((qw, tile), BF16))

    def tail_phase(DWS, X, WQO, WOO, WKVO, DKVT, DWK, DWM, ACC, AT, OUT, YB, XB):
        n_w = remote(DWS, DWR, ns, nr, 9, near)
        other = lanes_of(1 - core, hd)
        loads = [local(wq_hbm.at[:, lanes_of(1 - core, qw)], WQO, 0), local(wk_hbm.at[:, other], WKVO.at[:, :hd], 1),
                 local(wv_hbm.at[:, other], WKVO.at[:, hd:], 2), local(x_hbm, X, 3),
                 local(wo_hbm.at[lanes_of(1 - core, qw), :], WOO, 4)]
        for cp in loads:
            cp.start()

        def finish(t, same):
            ct, st = tile_tables(cos_ref, sin_ref, tile, t)
            g = (DK[t] * scale).astype(BF16).astype(F32)
            gk = (g * ct - pltpu.roll(g, hd // 2, 1) * st).astype(BF16)
            gv = DV[t].astype(BF16)
            DKVT[t, :hd, :] = gk.T
            DKVT[t, hd:, :] = gv.T

            @pl.when(t // 2 == 0)
            def _():
                DKA[t % 2, :, :hd] = gk
                DKA[t % 2, :, hd:] = gv

            @pl.when(t // 2 == 1)
            def _():
                DKS[t % 2, :, :hd] = gk
                DKS[t % 2, :, hd:] = gv

            return same

        lax.fori_loop(0, 4, finish, 0)
        n_k.start()
        lax.fori_loop(4, 8, finish, 0)

        DWK[...] = jnp.zeros_like(DWK)

        def kv_grad(t, _):
            DWK[...] += dot(DKVT[t], H[t, :, lanes_of(chip, 2 * part)])
            return _

        lax.fori_loop(0, 8, kv_grad, 0)
        theirs = lanes_of(1 - core, part)
        mine = lanes_of(core, part)
        for n in range(qw // tile):
            cols = slice(n * tile, (n + 1) * tile)
            DWS[:, cols] = DWT[cols, theirs].T
        DWS[:, qw:] = DWK[:, theirs].T
        n_w.start()
        for n in range(qw // tile):
            cols = slice(n * tile, (n + 1) * tile)
            DWM[:, cols] = DWT[cols, mine].T
        DWM[:, qw:] = DWK[:, mine].T
        outs = [local(DWM.at[:, :qw], dwq_hbm.at[:, lanes_of(core, qw)], 5),
                local(DWM.at[:, qw:qw + hd], dwk_hbm.at[:, lanes_of(core, hd)], 6),
                local(DWM.at[:, qw + hd:], dwv_hbm.at[:, lanes_of(core, hd)], 7)]
        for cp in outs:
            cp.start()

        for cp in loads[:4]:
            cp.wait()
        n_q.wait_recv()
        n_k.wait_recv()

        def rowsum(v):
            return jnp.sum(v, axis=0, keepdims=True)

        VS[0] = jnp.zeros_like(VS[0])
        gain = lnw[...]
        for t in range(2):
            ACC[...] = (dot_nt(DQA[t], WQ[...]) + dot_nt(DQR[t], WQO[...])
                        + dot_nt(DKA[t], WKV[...]) + dot_nt(DKR[t], WKVO[...]))

            def back(r, _):
                rows = pl.ds(pl.multiple_of(r * 64, 64), 64)
                dh = ACC[rows, :].astype(BF16).astype(F32)
                x = X[t, rows, :].astype(F32)
                cen = x - jnp.mean(x, axis=-1, keepdims=True)
                inv = lax.rsqrt(jnp.mean(cen * cen, axis=-1, keepdims=True) + EPS)
                xh = cen * inv
                a = dh * gain
                d = D[t, rows, :].astype(F32)
                dx = inv * (a - jnp.mean(a, axis=-1, keepdims=True) - xh * jnp.mean(a * xh, axis=-1, keepdims=True))
                XB[t, rows, :] = (d + dx).astype(BF16)
                VS[0, 0:1, :] += rowsum(dh * xh)
                VS[0, 1:2, :] += rowsum(dh)
                VS[0, 2:3, :] += rowsum(d)
                return _

            lax.fori_loop(0, tile // 64, back, 0)
            for side, q, k in ((core, DQA, DKA), (1 - core, DQR, DKR)):
                qs = rowsum(q[t].astype(F32))
                ks = rowsum(k[t].astype(F32))
                for h in range(2):
                    @pl.when(side == h)
                    def _():
                        VS[0, 3:4, h * qw:(h + 1) * qw] += qs
                        VS[0, 4:5, h * hd:(h + 1) * hd] += ks[:, :hd]
                        VS[0, 5:6, h * hd:(h + 1) * hd] += ks[:, hd:]
        n_v.start()
        outs.append(local(XB, dx_hbm, 8))
        outs[-1].start()

        loads[4].wait()
        n_o.wait_recv()
        for t in range(2):
            z = dot(ONA[t], WO[...]) + dot(ONR[t], WOO[...])
            YB[t] = (X[t].astype(F32) + (z + bo[...])).astype(BF16)
        outs.append(local(YB, y_hbm, 9))
        outs[-1].start()
        n_v.wait_recv()
        VS[1] = VS[0] + VR[0]
        f_v.start()

        def pick(t, _):
            n_s_in(t).wait_recv()
            AT[:, pl.ds(pl.multiple_of(t * tile, tile), tile)] = jnp.where(core == chip, KEEP[t], GOT[t])
            return _

        lax.fori_loop(0, 8, pick, 0)
        tn = 512
        for n in range(width // tn):
            OUT[:, n * tn:(n + 1) * tn] = dot(AT[...], D[:, :, n * tn:(n + 1) * tn].reshape(8 * tile, tn))
        outs.append(local(OUT, dwo_hbm, 10))
        outs[-1].start()
        n_w.wait_recv()
        outs += [local(DWR.at[:, :qw], dwq_hbm.at[:, lanes_of(1 - core, qw)], 11),
                 local(DWR.at[:, qw:qw + hd], dwk_hbm.at[:, lanes_of(1 - core, hd)], 12),
                 local(DWR.at[:, qw + hd:], dwv_hbm.at[:, lanes_of(1 - core, hd)], 13)]
        for cp in outs[-3:]:
            cp.start()
        f_v.wait_recv()
        vec_ref[...] = VS[1] + VR[1]
        for cp in outs:
            cp.wait()
        n_w.wait_send()

    pl.run_scoped(tail_phase,
                  pltpu.VMEM((part, qw + 2 * hd), F32), pltpu.VMEM((2, tile, width), BF16), pltpu.VMEM((width, qw), BF16), pltpu.VMEM((qw, width), BF16),
                  pltpu.VMEM((width, 2 * hd), BF16), pltpu.VMEM((8, 2 * hd, tile), BF16), pltpu.VMEM((2 * hd, 2 * part), F32),
                  pltpu.VMEM((part, qw + 2 * hd), F32), pltpu.VMEM((tile, width), F32), pltpu.VMEM((part, 8 * tile), BF16),
                  pltpu.VMEM((part, width), F32), pltpu.VMEM((2, tile, width), BF16), pltpu.VMEM((2, tile, width), BF16))

    for cp in (n_h, n_d, f_kv, f_h1, f_d1, f_h0, f_d0, n_h5, n_d5, n_h4, n_d4, n_o, n_q, n_k, n_v, f_v):
        cp.wait_send()

    def sent(t, _):
        n_s(t).wait_send()
        return _

    lax.fori_loop(0, 8, sent, 0)


def mega(x, d, wq, wk, wv, wo, small, cos_t, sin_t, nh, hd, scale):
    _, tile, width = x.shape
    qw = nh * hd
    part = width // 4
    anywhere = pl.BlockSpec(memory_space=pltpu.HBM)
    vmem = pl.BlockSpec(memory_space=pltpu.VMEM)
    rows = (2, tile, width)

    def vm(*shape, dtype=BF16):
        return pltpu.VMEM(shape, dtype)

    return pl.pallas_call(
        functools.partial(mega_body, nh, hd, tile, scale),
        in_specs=[anywhere] * 6 + [vmem] * 8,
        out_specs=[anywhere] * 6 + [vmem],
        out_shape=[jax.ShapeDtypeStruct(rows, BF16), jax.ShapeDtypeStruct(rows, BF16),
                   jax.ShapeDtypeStruct((part, 2 * qw), F32), jax.ShapeDtypeStruct((part, 2 * hd), F32),
                   jax.ShapeDtypeStruct((part, 2 * hd), F32), jax.ShapeDtypeStruct((part, width), F32),
                   jax.ShapeDtypeStruct((8, width), F32)],
        scratch_shapes=[
            vm(8, tile, width), vm(8, tile, width), vm(8, tile, 2 * hd), vm(8, hd, tile), vm(8, hd, tile),
            vm(width, qw), vm(qw, width), vm(width, 2 * hd),
            vm(8, tile, hd, dtype=F32), vm(8, tile, hd, dtype=F32),
            vm(8, part, tile), vm(8, part, tile), vm(8, part, tile), vm(qw, 2 * part, dtype=F32),
            vm(2, tile, qw), vm(2, tile, qw), vm(2, tile, qw), vm(2, tile, qw), vm(2, tile, qw), vm(2, tile, qw),
            vm(2, tile, 2 * hd), vm(2, tile, 2 * hd), vm(2, tile, 2 * hd),
            vm(part, qw + 2 * hd, dtype=F32),
            vm(2, 8, width, dtype=F32), vm(2, 8, width, dtype=F32), vm(8, width, dtype=F32),
            pltpu.SemaphoreType.DMA((6,)), pltpu.SemaphoreType.DMA((6,)),
            pltpu.SemaphoreType.DMA((19,)), pltpu.SemaphoreType.DMA((19,)), pltpu.SemaphoreType.DMA((14,))],
        compiler_params=pltpu.CompilerParams(collective_id=0, has_side_effects=True, vmem_limit_bytes=67043328),
        name="sublayer",
    )(x, d, wq, wk, wv, wo, *small, cos_t, sin_t)


def solution(mesh):
    groups = mesh.shape['cp']
    row_spec = P('dp', 'cp', None)
    mat_spec = P(('dp', 'cp'), None)
    vec_spec = P('dp')

    def device_fn(x_in, ln_w, ln_b, w_q, b_q, w_k, b_k, w_v, b_v, w_o, b_o, long_factor, dy_out):
        rank = lax.axis_index('cp').astype(jnp.int32)
        tokens, width = x_in.shape[1:]
        piece = tokens // 2
        hd = 2 * long_factor.shape[0]
        kvw = w_k.shape[1]
        nh = w_q.shape[1] // kvw
        blocks = jnp.stack([rank, rank ^ 1, rank ^ 2, rank ^ 3])
        rel = jnp.stack([blocks, 2 * groups - 1 - blocks], axis=1).reshape(2 * groups)
        cos_t, sin_t = rope_tables(rel * piece, piece, long_factor)
        small = (ln_w, ln_b, b_q, b_o, b_k, b_v)
        y, dx, d_wq, d_wk, d_wv, d_wo, vec = mega(
            x_in.reshape(2, piece, width), dy_out.reshape(2, piece, width), w_q, w_k, w_v, w_o,
            small, cos_t, sin_t, nh, hd, hd ** -0.5)
        d_lnw, d_lnb, d_bo, d_bq = (vec[n] for n in range(4))
        d_bk, d_bv = (vec[n, :kvw] for n in (4, 5))
        shape = (1, tokens, width)
        return (y.reshape(shape), dx.reshape(shape), d_wq, d_wk, d_wv, d_wo, d_lnw, d_lnb, d_bq, d_bk, d_bv, d_bo)

    in_specs = (row_spec,) + (P(),) * 11 + (row_spec,)
    out_specs = (row_spec, row_spec) + (mat_spec,) * 4 + (vec_spec,) * 6
    return jax.shard_map(device_fn, mesh=mesh, in_specs=in_specs, out_specs=out_specs, check_vma=False)
```

```python
import functools
import math
import jax
import jax.numpy as jnp
from jax import lax
from jax.experimental import pallas as pl
from jax.experimental.pallas import tpu as pltpu
from jax.sharding import PartitionSpec as P

EPS = 1e-5
THETA = 10000.0
ROPE_SCALE = math.sqrt(1.0 + math.log(32.0) / math.log(4096.0))
LOG2E = math.log2(math.e)
NEG = -1e30
F32 = jnp.float32
BF16 = jnp.bfloat16


def dot(a, b):
    return lax.dot_general(a, b, (((1,), (0,)), ((), ())), preferred_element_type=F32)


def dot_nt(a, b):
    return lax.dot_general(a, b, (((1,), (1,)), ((), ())), preferred_element_type=F32)


def dot_tn(a, b):
    return lax.dot_general(a, b, (((0,), (0,)), ((), ())), preferred_element_type=F32)


def rope_tables(starts, piece, long_factor):
    half_dim = long_factor.shape[0]
    exponent = jnp.arange(half_dim, dtype=F32) * (1.0 / half_dim)
    inv_freq = 1.0 / (long_factor * THETA ** exponent)
    positions = jnp.concatenate([jnp.arange(piece, dtype=jnp.int32), starts])
    angle = positions.astype(F32)[:, None] * inv_freq[None, :]
    cos_t = jnp.cos(angle)
    sin_t = jnp.sin(angle)
    return jnp.concatenate([cos_t, cos_t], axis=1), jnp.concatenate([-sin_t, sin_t], axis=1)


def tile_tables(cos_ref, sin_ref, piece, t):
    ca = cos_ref[pl.ds(piece + t, 1), :] * ROPE_SCALE
    sa = sin_ref[pl.ds(piece + t, 1), :] * ROPE_SCALE
    cb = cos_ref[:piece, :]
    sb = sin_ref[:piece, :]
    return ca * cb - sa * sb, sa * cb + ca * sb


MESH = pl.DeviceIdType.MESH


def mega_body(nh, hd, tile, scale,
              x_hbm, d_hbm, wq_hbm, wk_hbm, wv_hbm, wo_hbm, lnw1, lnb1, bq1, bo1, bk1, bv1, cos_ref, sin_ref,
              y_hbm, dx_hbm, dwq_hbm, dwk_hbm, dwv_hbm, dwo_hbm, vec_ref,
              H, D, KV, KT, VT, WQ, WO, WKV, DK, DV, AT, SEND, DWT, ONA, ONS, ONR, DQA, DQS, DQR, DKA, DKS, DKR,
              DWR, VS, VR, SM, fs, fr, ns, nr, ls):
    rank = lax.axis_index('cp')
    core = rank % 2
    chip = rank // 2
    near = rank + 1 - 2 * core
    far = rank + 2 - 4 * chip
    tq = nh * tile
    qw = nh * hd
    width = H.shape[2]
    part = width // 4
    third = nh // 2
    lnw, lnb, bq, bo, bk, bv = (SM.at[n:n + 1, :] for n in range(6))
    for n, r in enumerate((lnw1, lnb1, bq1, bo1, bk1, bv1)):
        SM[n:n + 1, :r.shape[0]] = r[...].astype(F32).reshape(1, r.shape[0])

    def local(src, dst, n):
        return pltpu.make_async_copy(src, dst, ls.at[n])

    def remote(src, dst, send, recv, n, to):
        return pltpu.make_async_remote_copy(src_ref=src, dst_ref=dst, send_sem=send.at[n], recv_sem=recv.at[n],
                                            device_id={'cp': to}, device_id_type=MESH)

    def lanes_of(i, n):
        return pl.ds(pl.multiple_of(i * n, 128), n)

    def piece_of(t):
        k = t // 2
        b = (rank % 2 + k % 2) % 2 + 2 * ((rank // 2 + k // 2) % 2)
        return b + (t % 2) * (7 - 2 * b)

    def tile_of(p):
        up = p // 4
        b = p + up * (7 - 2 * p)
        k = (rank % 2 + b % 2) % 2 + 2 * ((rank // 2 + b // 2) % 2)
        return 2 * k + up

    def start_loads(X):
        mine = lanes_of(core, hd)
        return [local(x_hbm, X, 0), local(wk_hbm.at[:, mine], WKV.at[:, :hd], 1), local(wv_hbm.at[:, mine], WKV.at[:, hd:], 2),
                local(d_hbm, D.at[0:2], 3), local(wq_hbm.at[:, lanes_of(core, qw)], WQ, 4),
                local(wo_hbm.at[lanes_of(core, qw), :], WO, 5)]

    n_h = remote(H.at[0:2], H.at[2:4], ns, nr, 0, near)
    n_d = remote(D.at[0:2], D.at[2:4], ns, nr, 1, near)
    f_kv = remote(KV.at[0:2], KV.at[4:6], fs, fr, 0, far)
    f_kw = remote(KV.at[2:4], KV.at[6:8], fs, fr, 6, far)
    f_h1 = remote(H.at[1], H.at[5], fs, fr, 1, far)
    f_d1 = remote(D.at[1, :tile // 2], D.at[5, :tile // 2], fs, fr, 2, far)
    f_e1 = remote(D.at[1, tile // 2:], D.at[5, tile // 2:], fs, fr, 7, far)
    f_h0 = remote(H.at[0], H.at[4], fs, fr, 3, far)
    f_d0 = remote(D.at[0], D.at[4], fs, fr, 4, far)
    n_h5 = remote(H.at[5], H.at[7], ns, nr, 2, near)
    n_d5 = remote(D.at[5], D.at[7], ns, nr, 3, near)
    n_h4 = remote(H.at[4], H.at[6], ns, nr, 4, near)
    n_d4 = remote(D.at[4], D.at[6], ns, nr, 5, near)
    n_o = remote(ONS, ONR, ns, nr, 6, near)
    n_q = remote(DQS, DQR, ns, nr, 7, near)
    n_k = remote(DKS, DKR, ns, nr, 8, near)
    n_v = remote(VS.at[0], VR.at[0], ns, nr, 10, near)
    f_v = remote(VS.at[1], VR.at[1], fs, fr, 5, far)

    def swapped(t):
        return t + 2 - 4 * ((t // 2) % 2)

    holds = core == chip

    def n_s(t, s):
        return remote(SEND.at[s % 2], AT.at[swapped(t)], ns, nr, 11 + t, near)

    def n_s_in(t):
        return remote(SEND.at[0], AT.at[t], ns, nr, 11 + swapped(t), near)

    def tile_at(s):
        late = s // 4
        u = s % 4
        return (1 - late) * ((u + 2) % 4) + late * (4 + (u % 2) * 2 + 1 - u // 2)

    def head_phase(X):
        loads = start_loads(X)
        for c in loads:
            c.start()
        barrier = pltpu.get_barrier_semaphore()
        for to in (near, far):
            pl.semaphore_signal(barrier, inc=1, device_id={'cp': to}, device_id_type=MESH)
        pl.semaphore_wait(barrier, 2)
        loads[3].wait()
        f_d1.start()
        loads[0].wait()
        gain = lnw[...]
        shift = lnb[...]

        def norm(r, _):
            rows = pl.ds(pl.multiple_of((r % 4) * 64, 64), 64)
            x = X[r // 4, rows, :].astype(F32)
            cen = x - jnp.mean(x, axis=-1, keepdims=True)
            inv = lax.rsqrt(jnp.mean(cen * cen, axis=-1, keepdims=True) + EPS)
            H[r // 4, rows, :] = (cen * inv * gain + shift).astype(BF16)
            return _

        lax.fori_loop(0, 8, norm, 0)
        n_h.start()
        n_d.start()
        loads[1].wait()
        loads[2].wait()
        loads[4].wait()
        loads[5].wait()

    pl.run_scoped(head_phase, pltpu.VMEM((2, tile, width), BF16))

    def attention_phase(Q, DO, PS, DPS, MS, PB, DSB, OT, DQT, DQTT):
        c = scale * LOG2E

        def rope(t, ct, st):
            t = t.astype(BF16).astype(F32)
            return (t * ct + pltpu.roll(t, hd // 2, 1) * st).astype(BF16)

        def kv_tile(t, _):
            ct, st = tile_tables(cos_ref, sin_ref, tile, t)
            kv = dot(H[t], WKV[...])
            KV[t, :, :hd] = rope(kv[:, :hd] + bk[0:1, lanes_of(core, hd)], ct, st)
            KV[t, :, hd:] = (kv[:, hd:] + bv[0:1, lanes_of(core, hd)]).astype(BF16)
            return _

        def project(t, slot):
            ct, st = tile_tables(cos_ref, sin_ref, tile, t)
            q = dot(H[t], WQ[...]) + bq[0:1, lanes_of(core, qw)]
            for n in range(nh):
                Q[slot, n] = rope(q[:, n * hd:(n + 1) * hd], ct, st)
            r = dot_nt(D[t], WO[...]).astype(BF16)
            for n in range(nh):
                DO[slot, n] = r[:, n * hd:(n + 1) * hd]

        def turn(t, _):
            KT[t] = KV[t, :, :hd].T
            VT[t] = KV[t, :, hd:].T
            return _

        lax.fori_loop(0, 2, kv_tile, 0)
        f_kv.start()
        n_h.wait_recv()
        lax.fori_loop(2, 4, kv_tile, 0)
        f_kw.start()
        f_h1.start()
        f_e1.start()
        f_h0.start()
        f_d0.start()
        n_d.wait_recv()

        def first_four(t, _):
            project(t, t)
            return _

        lax.fori_loop(0, 4, first_four, 0)
        lax.fori_loop(0, 4, turn, 0)
        DK[...] = jnp.zeros_like(DK)
        DV[...] = jnp.zeros_like(DV)
        DWT[...] = jnp.zeros_like(DWT)
        f_kv.wait_recv()
        lax.fori_loop(4, 6, turn, 0)
        f_kw.wait_recv()
        lax.fori_loop(6, 8, turn, 0)

        def one_tile(s, same):
            late = s // 4
            u = s % 4
            t = tile_at(s)
            slot = (1 - late) * t + late * u

            @pl.when(s == 4)
            def _():
                f_h1.wait_recv()
                f_d1.wait_recv()
                f_e1.wait_recv()
                n_h5.start()
                n_d5.start()

            @pl.when(s == 5)
            def _():
                n_h5.wait_recv()
                n_d5.wait_recv()

            @pl.when(s == 6)
            def _():
                f_h0.wait_recv()
                f_d0.wait_recv()
                n_h4.start()
                n_d4.start()

            @pl.when(s == 7)
            def _():
                n_h4.wait_recv()
                n_d4.wait_recv()

            @pl.when(late == 1)
            def _():
                project(t, slot)

            i = piece_of(t)

            def first(j, carry, diag):
                m, l, dl = carry
                g = tile_of(j)
                kj = KV[g, :, :hd]
                vj = KV[g, :, hd:]
                m_new, l_new, d_new = [], [], []
                for n in range(nh):
                    lanes = slice(n * tile, (n + 1) * tile)
                    sc = dot_nt(kj, Q[slot, n]) * c
                    if diag:
                        key = lax.broadcasted_iota(jnp.int32, (tile, tile), 0)
                        qry = lax.broadcasted_iota(jnp.int32, (tile, tile), 1)
                        sc = jnp.where(key <= qry, sc, NEG)
                    dpb = dot_nt(vj, DO[slot, n]).astype(BF16)
                    DPS[j, :, lanes] = dpb
                    mo = m[:, lanes]
                    mn = jnp.maximum(mo, jnp.max(sc, axis=0, keepdims=True))
                    p = jnp.exp2(sc - mn)
                    PS[j, :, lanes] = p
                    al = jnp.exp2(mo - mn)
                    m_new.append(mn)
                    l_new.append(l[:, lanes] * al + jnp.sum(p, axis=0, keepdims=True))
                    d_new.append(dl[:, lanes] * al + jnp.sum(p * dpb.astype(F32), axis=0, keepdims=True))
                m = jnp.concatenate(m_new, axis=1)
                MS[j] = m
                return m, jnp.concatenate(l_new, axis=1), jnp.concatenate(d_new, axis=1)

            init = (jnp.full((1, tq), NEG, F32), jnp.zeros((1, tq), F32), jnp.zeros((1, tq), F32))
            carry = lax.fori_loop(0, i // 2, lambda h, cr: first(2 * h + 1, first(2 * h, cr, False), False), init)
            carry = lax.fori_loop(2 * (i // 2), i, lambda j, cr: first(j, cr, False), carry)
            m, l, dl = first(i, carry, True)
            inv = 1.0 / l
            delta = dl * inv
            OT[...] = jnp.zeros_like(OT)
            DQT[...] = jnp.zeros_like(DQT)

            def weigh(j, k):
                f = jnp.exp2(MS[j] - m) * inv
                for n in range(nh):
                    lanes = slice(n * tile, (n + 1) * tile)
                    p = PS[j, :, lanes] * f[:, lanes]
                    PB[k, :, lanes] = p.astype(BF16)
                    DSB[k, :, lanes] = (p * (DPS[j, :, lanes].astype(F32) - delta[:, lanes])).astype(BF16)

            def second(js, carry):
                gs = [tile_of(j) for j in js]
                for k, j in enumerate(js):
                    weigh(j, k)
                o = dot(VT[gs[0]], PB[0])
                dq = dot(KT[gs[0]], DSB[0])
                for k in range(1, len(js)):
                    o += dot(VT[gs[k]], PB[k])
                    dq += dot(KT[gs[k]], DSB[k])
                OT[...] += o
                DQT[...] += dq
                for k, g in enumerate(gs):
                    DV[g] += dot(PB[k], DO[slot].reshape(tq, hd))
                    DK[g] += dot(DSB[k], Q[slot].reshape(tq, hd))
                return carry

            pairs = (i + 1) // 2
            lax.fori_loop(0, pairs, lambda h, cr: second((2 * h, 2 * h + 1), cr), 0)
            lax.fori_loop(2 * pairs, i + 1, lambda j, cr: second((j,), cr), 0)
            ct, st = tile_tables(cos_ref, sin_ref, tile, t)
            cos_t = ct.T[:hd // 2]

            @pl.when(jnp.logical_and(holds, s >= 2))
            def _():
                n_s(tile_at(s - 2), s).wait_send()

            sin_t = st.T[hd // 2:]
            for n in range(nh):
                lanes = slice(n * tile, (n + 1) * tile)
                o_t = OT[:, lanes].astype(BF16)
                rows = slice((n % third) * hd, (n % third + 1) * hd)

                @pl.when(jnp.logical_and(holds, core == n // third))
                def _():
                    AT[t, rows, :] = o_t

                @pl.when(jnp.logical_and(holds, core != n // third))
                def _():
                    SEND[s % 2, rows, :] = o_t

                gr = (DQT[:, lanes] * scale).astype(BF16).astype(F32)
                a = gr[:hd // 2]
                e = gr[hd // 2:]
                gr = jnp.concatenate([a * cos_t + e * sin_t, e * cos_t - a * sin_t], axis=0).astype(BF16)
                cols = slice(n * hd, (n + 1) * hd)
                DQTT[cols, :] = gr

                @pl.when(t // 2 == 0)
                def _():
                    ONA[t % 2, :, cols] = o_t.T
                    DQA[t % 2, :, cols] = gr.T

                @pl.when(t // 2 == 1)
                def _():
                    ONS[t % 2, :, cols] = o_t.T
                    DQS[t % 2, :, cols] = gr.T

            @pl.when(holds)
            def _():
                n_s(t, s).start()

            @pl.when(s == 1)
            def _():
                n_o.start()
                n_q.start()

            DWT[...] += dot(DQTT[...], H[t, :, lanes_of(chip, 2 * part)])
            return same

        lax.fori_loop(0, 8, one_tile, 0)

    pl.run_scoped(attention_phase,
                  pltpu.VMEM((4, nh, tile, hd), BF16), pltpu.VMEM((4, nh, tile, hd), BF16),
                  pltpu.VMEM((8, tile, tq), F32), pltpu.VMEM((8, tile, tq), BF16), pltpu.VMEM((8, 1, tq), F32),
                  pltpu.VMEM((2, tile, tq), BF16), pltpu.VMEM((2, tile, tq), BF16), pltpu.VMEM((hd, tq), F32), pltpu.VMEM((hd, tq), F32),
                  pltpu.VMEM((qw, tile), BF16))

    def tail_phase(DWS, X, WQO, WOO, WKVO, DKVT, DWK, DWM, ACC, OUT, YB, XB):
        n_w = remote(DWS, DWR, ns, nr, 9, near)
        other = lanes_of(1 - core, hd)
        loads = [local(wq_hbm.at[:, lanes_of(1 - core, qw)], WQO, 0), local(wk_hbm.at[:, other], WKVO.at[:, :hd], 1),
                 local(wv_hbm.at[:, other], WKVO.at[:, hd:], 2), local(x_hbm, X, 3),
                 local(wo_hbm.at[lanes_of(1 - core, qw), :], WOO, 4)]
        for cp in loads:
            cp.start()

        def finish(t, same):
            ct, st = tile_tables(cos_ref, sin_ref, tile, t)
            g = (DK[t] * scale).astype(BF16).astype(F32)
            gk = (g * ct - pltpu.roll(g, hd // 2, 1) * st).astype(BF16)
            gv = DV[t].astype(BF16)
            DKVT[t, :hd, :] = gk.T
            DKVT[t, hd:, :] = gv.T

            @pl.when(t // 2 == 0)
            def _():
                DKA[t % 2, :, :hd] = gk
                DKA[t % 2, :, hd:] = gv

            @pl.when(t // 2 == 1)
            def _():
                DKS[t % 2, :, :hd] = gk
                DKS[t % 2, :, hd:] = gv

            return same

        lax.fori_loop(0, 4, finish, 0)
        n_k.start()
        lax.fori_loop(4, 8, finish, 0)

        DWK[...] = jnp.zeros_like(DWK)

        def kv_grad(t, _):
            DWK[...] += dot(DKVT[t], H[t, :, lanes_of(chip, 2 * part)])
            return _

        lax.fori_loop(0, 8, kv_grad, 0)
        theirs = lanes_of(1 - core, part)
        mine = lanes_of(core, part)
        for n in range(qw // tile):
            cols = slice(n * tile, (n + 1) * tile)
            DWS[:, cols] = DWT[cols, theirs].T
        DWS[:, qw:] = DWK[:, theirs].T
        n_w.start()
        for n in range(qw // tile):
            cols = slice(n * tile, (n + 1) * tile)
            DWM[:, cols] = DWT[cols, mine].T
        DWM[:, qw:] = DWK[:, mine].T
        outs = [local(DWM.at[:, :qw], dwq_hbm.at[:, lanes_of(core, qw)], 5),
                local(DWM.at[:, qw:qw + hd], dwk_hbm.at[:, lanes_of(core, hd)], 6),
                local(DWM.at[:, qw + hd:], dwv_hbm.at[:, lanes_of(core, hd)], 7)]
        for cp in outs:
            cp.start()

        for cp in loads[:4]:
            cp.wait()
        n_q.wait_recv()
        n_k.wait_recv()

        def rowsum(v):
            return jnp.sum(v, axis=0, keepdims=True)

        VS[0] = jnp.zeros_like(VS[0])
        gain = lnw[...]
        for t in range(2):
            ACC[...] = (dot_nt(DQA[t], WQ[...]) + dot_nt(DQR[t], WQO[...])
                        + dot_nt(DKA[t], WKV[...]) + dot_nt(DKR[t], WKVO[...]))

            def back(r, _):
                rows = pl.ds(pl.multiple_of(r * 64, 64), 64)
                dh = ACC[rows, :].astype(BF16).astype(F32)
                x = X[t, rows, :].astype(F32)
                cen = x - jnp.mean(x, axis=-1, keepdims=True)
                inv = lax.rsqrt(jnp.mean(cen * cen, axis=-1, keepdims=True) + EPS)
                xh = cen * inv
                a = dh * gain
                d = D[t, rows, :].astype(F32)
                dx = inv * (a - jnp.mean(a, axis=-1, keepdims=True) - xh * jnp.mean(a * xh, axis=-1, keepdims=True))
                XB[t, rows, :] = (d + dx).astype(BF16)
                VS[0, 0:1, :] += rowsum(dh * xh)
                VS[0, 1:2, :] += rowsum(dh)
                VS[0, 2:3, :] += rowsum(d)
                return _

            lax.fori_loop(0, tile // 64, back, 0)
            for side, q, k in ((core, DQA, DKA), (1 - core, DQR, DKR)):
                qs = rowsum(q[t].astype(F32))
                ks = rowsum(k[t].astype(F32))
                for h in range(2):
                    @pl.when(side == h)
                    def _():
                        VS[0, 3:4, h * qw:(h + 1) * qw] += qs
                        VS[0, 4:5, h * hd:(h + 1) * hd] += ks[:, :hd]
                        VS[0, 5:6, h * hd:(h + 1) * hd] += ks[:, hd:]
        n_v.start()
        outs.append(local(XB, dx_hbm, 8))
        outs[-1].start()

        loads[4].wait()
        n_o.wait_recv()
        for t in range(2):
            z = dot(ONA[t], WO[...]) + dot(ONR[t], WOO[...])
            YB[t] = (X[t].astype(F32) + (z + bo[...])).astype(BF16)
        outs.append(local(YB, y_hbm, 9))
        outs[-1].start()
        n_v.wait_recv()
        VS[1] = VS[0] + VR[0]
        f_v.start()

        @pl.when(jnp.logical_not(holds))
        def _():
            for t in range(8):
                n_s_in(t).wait_recv()

        tn = 512
        for n in range(width // tn):
            cols = slice(n * tn, (n + 1) * tn)
            acc = dot(AT[0], D[0, :, cols])
            for t in range(1, 8):
                acc += dot(AT[t], D[t, :, cols])
            OUT[:, cols] = acc
        outs.append(local(OUT, dwo_hbm, 10))
        outs[-1].start()
        n_w.wait_recv()
        outs += [local(DWR.at[:, :qw], dwq_hbm.at[:, lanes_of(1 - core, qw)], 11),
                 local(DWR.at[:, qw:qw + hd], dwk_hbm.at[:, lanes_of(1 - core, hd)], 12),
                 local(DWR.at[:, qw + hd:], dwv_hbm.at[:, lanes_of(1 - core, hd)], 13)]
        for cp in outs[-3:]:
            cp.start()
        f_v.wait_recv()
        vec_ref[...] = VS[1] + VR[1]
        for cp in outs:
            cp.wait()
        n_w.wait_send()

    pl.run_scoped(tail_phase,
                  pltpu.VMEM((part, qw + 2 * hd), F32), pltpu.VMEM((2, tile, width), BF16), pltpu.VMEM((width, qw), BF16), pltpu.VMEM((qw, width), BF16),
                  pltpu.VMEM((width, 2 * hd), BF16), pltpu.VMEM((8, 2 * hd, tile), BF16), pltpu.VMEM((2 * hd, 2 * part), F32),
                  pltpu.VMEM((part, qw + 2 * hd), F32), pltpu.VMEM((tile, width), F32),
                  pltpu.VMEM((part, width), F32), pltpu.VMEM((2, tile, width), BF16), pltpu.VMEM((2, tile, width), BF16))

    for cp in (n_h, n_d, f_kv, f_kw, f_h1, f_d1, f_e1, f_h0, f_d0, n_h5, n_d5, n_h4, n_d4, n_o, n_q, n_k, n_v, f_v):
        cp.wait_send()

    @pl.when(holds)
    def _():
        for s in (6, 7):
            n_s(tile_at(s), s).wait_send()


def mega(x, d, wq, wk, wv, wo, small, cos_t, sin_t, nh, hd, scale):
    _, tile, width = x.shape
    qw = nh * hd
    part = width // 4
    anywhere = pl.BlockSpec(memory_space=pltpu.HBM)
    vmem = pl.BlockSpec(memory_space=pltpu.VMEM)
    rows = (2, tile, width)

    def vm(*shape, dtype=BF16):
        return pltpu.VMEM(shape, dtype)

    return pl.pallas_call(
        functools.partial(mega_body, nh, hd, tile, scale),
        in_specs=[anywhere] * 6 + [vmem] * 8,
        out_specs=[anywhere] * 6 + [vmem],
        out_shape=[jax.ShapeDtypeStruct(rows, BF16), jax.ShapeDtypeStruct(rows, BF16),
                   jax.ShapeDtypeStruct((part, 2 * qw), F32), jax.ShapeDtypeStruct((part, 2 * hd), F32),
                   jax.ShapeDtypeStruct((part, 2 * hd), F32), jax.ShapeDtypeStruct((part, width), F32),
                   jax.ShapeDtypeStruct((8, width), F32)],
        scratch_shapes=[
            vm(8, tile, width), vm(8, tile, width), vm(8, tile, 2 * hd), vm(8, hd, tile), vm(8, hd, tile),
            vm(width, qw), vm(qw, width), vm(width, 2 * hd),
            vm(8, tile, hd, dtype=F32), vm(8, tile, hd, dtype=F32),
            vm(8, part, tile), vm(2, part, tile), vm(qw, 2 * part, dtype=F32),
            vm(2, tile, qw), vm(2, tile, qw), vm(2, tile, qw), vm(2, tile, qw), vm(2, tile, qw), vm(2, tile, qw),
            vm(2, tile, 2 * hd), vm(2, tile, 2 * hd), vm(2, tile, 2 * hd),
            vm(part, qw + 2 * hd, dtype=F32),
            vm(2, 8, width, dtype=F32), vm(2, 8, width, dtype=F32), vm(8, width, dtype=F32),
            pltpu.SemaphoreType.DMA((8,)), pltpu.SemaphoreType.DMA((8,)),
            pltpu.SemaphoreType.DMA((19,)), pltpu.SemaphoreType.DMA((19,)), pltpu.SemaphoreType.DMA((14,))],
        compiler_params=pltpu.CompilerParams(collective_id=0, has_side_effects=True, vmem_limit_bytes=67043328),
        name="sublayer",
    )(x, d, wq, wk, wv, wo, *small, cos_t, sin_t)


def solution(mesh):
    groups = mesh.shape['cp']
    row_spec = P('dp', 'cp', None)
    mat_spec = P(('dp', 'cp'), None)
    vec_spec = P('dp')

    def device_fn(x_in, ln_w, ln_b, w_q, b_q, w_k, b_k, w_v, b_v, w_o, b_o, long_factor, dy_out):
        rank = lax.axis_index('cp').astype(jnp.int32)
        tokens, width = x_in.shape[1:]
        piece = tokens // 2
        hd = 2 * long_factor.shape[0]
        kvw = w_k.shape[1]
        nh = w_q.shape[1] // kvw
        blocks = jnp.stack([rank, rank ^ 1, rank ^ 2, rank ^ 3])
        rel = jnp.stack([blocks, 2 * groups - 1 - blocks], axis=1).reshape(2 * groups)
        cos_t, sin_t = rope_tables(rel * piece, piece, long_factor)
        small = (ln_w, ln_b, b_q, b_o, b_k, b_v)
        y, dx, d_wq, d_wk, d_wv, d_wo, vec = mega(
            x_in.reshape(2, piece, width), dy_out.reshape(2, piece, width), w_q, w_k, w_v, w_o,
            small, cos_t, sin_t, nh, hd, hd ** -0.5)
        d_lnw, d_lnb, d_bo, d_bq = (vec[n] for n in range(4))
        d_bk, d_bv = (vec[n, :kvw] for n in (4, 5))
        shape = (1, tokens, width)
        return (y.reshape(shape), dx.reshape(shape), d_wq, d_wk, d_wv, d_wo, d_lnw, d_lnb, d_bq, d_bk, d_bv, d_bo)

    in_specs = (row_spec,) + (P(),) * 11 + (row_spec,)
    out_specs = (row_spec, row_spec) + (mat_spec,) * 4 + (vec_spec,) * 6
    return jax.shard_map(device_fn, mesh=mesh, in_specs=in_specs, out_specs=out_specs, check_vma=False)
```

```python
import functools
import math
import jax
import jax.numpy as jnp
from jax import lax
from jax.experimental import pallas as pl
from jax.experimental.pallas import tpu as pltpu
from jax.sharding import PartitionSpec as P

EPS = 1e-5
THETA = 10000.0
ROPE_SCALE = math.sqrt(1.0 + math.log(32.0) / math.log(4096.0))
LOG2E = math.log2(math.e)
NEG = -1e30
F32 = jnp.float32
BF16 = jnp.bfloat16


def dot(a, b):
    return lax.dot_general(a, b, (((1,), (0,)), ((), ())), preferred_element_type=F32)


def dot_nt(a, b):
    return lax.dot_general(a, b, (((1,), (1,)), ((), ())), preferred_element_type=F32)


def dot_tn(a, b):
    return lax.dot_general(a, b, (((0,), (0,)), ((), ())), preferred_element_type=F32)


def rope_tables(starts, piece, long_factor):
    half_dim = long_factor.shape[0]
    exponent = jnp.arange(half_dim, dtype=F32) * (1.0 / half_dim)
    inv_freq = 1.0 / (long_factor * THETA ** exponent)
    positions = jnp.concatenate([jnp.arange(piece, dtype=jnp.int32), starts])
    angle = positions.astype(F32)[:, None] * inv_freq[None, :]
    cos_t = jnp.cos(angle)
    sin_t = jnp.sin(angle)
    return jnp.concatenate([cos_t, cos_t], axis=1), jnp.concatenate([-sin_t, sin_t], axis=1)


def tile_tables(cos_ref, sin_ref, piece, t):
    ca = cos_ref[pl.ds(piece + t, 1), :] * ROPE_SCALE
    sa = sin_ref[pl.ds(piece + t, 1), :] * ROPE_SCALE
    cb = cos_ref[:piece, :]
    sb = sin_ref[:piece, :]
    return ca * cb - sa * sb, sa * cb + ca * sb


MESH = pl.DeviceIdType.MESH


def mega_body(nh, hd, tile, scale,
              x_hbm, d_hbm, wq_hbm, wk_hbm, wv_hbm, wo_hbm, lnw1, lnb1, bq1, bo1, bk1, bv1, cos_ref, sin_ref,
              y_hbm, dx_hbm, dwm_hbm, DWR, dwo_hbm, vec_ref,
              H, D, KV, KT, VT, WQ, WO, WKV, DK, DV, AT, SEND, DWT, ONA, ONS, ONR, DQA, DQS, DQR, DKA, DKS, DKR,
              VS, VR, SM, fs, fr, ns, nr, ls):
    rank = lax.axis_index('cp')
    core = rank % 2
    chip = rank // 2
    near = rank + 1 - 2 * core
    far = rank + 2 - 4 * chip
    tq = nh * tile
    qw = nh * hd
    width = H.shape[2]
    part = width // 4
    third = nh // 2
    lnw, lnb, bq, bo, bk, bv = (SM.at[n:n + 1, :] for n in range(6))
    for n, r in enumerate((lnw1, lnb1, bq1, bo1, bk1, bv1)):
        SM[n:n + 1, :r.shape[0]] = r[...].astype(F32).reshape(1, r.shape[0])

    def local(src, dst, n):
        return pltpu.make_async_copy(src, dst, ls.at[n])

    def remote(src, dst, send, recv, n, to):
        return pltpu.make_async_remote_copy(src_ref=src, dst_ref=dst, send_sem=send.at[n], recv_sem=recv.at[n],
                                            device_id={'cp': to}, device_id_type=MESH)

    def lanes_of(i, n):
        return pl.ds(pl.multiple_of(i * n, 128), n)

    def piece_of(t):
        k = t // 2
        b = (rank % 2 + k % 2) % 2 + 2 * ((rank // 2 + k // 2) % 2)
        return b + (t % 2) * (7 - 2 * b)

    def tile_of(p):
        up = p // 4
        b = p + up * (7 - 2 * p)
        k = (rank % 2 + b % 2) % 2 + 2 * ((rank // 2 + b // 2) % 2)
        return 2 * k + up

    def start_loads(X):
        mine = lanes_of(core, hd)
        return [local(x_hbm, X, 0), local(wk_hbm.at[:, mine], WKV.at[:, :hd], 1), local(wv_hbm.at[:, mine], WKV.at[:, hd:], 2),
                local(d_hbm, D.at[0:2], 3), local(wq_hbm.at[:, lanes_of(core, qw)], WQ, 4),
                local(wo_hbm.at[lanes_of(core, qw), :], WO, 5)]

    n_h = remote(H.at[0:2], H.at[2:4], ns, nr, 0, near)
    n_d = remote(D.at[0:2], D.at[2:4], ns, nr, 1, near)
    f_kv = remote(KV.at[0:2], KV.at[4:6], fs, fr, 0, far)
    f_kw = remote(KV.at[2:4], KV.at[6:8], fs, fr, 6, far)
    f_h1 = remote(H.at[1], H.at[5], fs, fr, 1, far)
    f_d1 = remote(D.at[1, :tile // 2], D.at[5, :tile // 2], fs, fr, 2, far)
    f_e1 = remote(D.at[1, tile // 2:], D.at[5, tile // 2:], fs, fr, 7, far)
    f_h0 = remote(H.at[0], H.at[4], fs, fr, 3, far)
    f_d0 = remote(D.at[0], D.at[4], fs, fr, 4, far)
    n_h5 = remote(H.at[5], H.at[7], ns, nr, 2, near)
    n_d5 = remote(D.at[5], D.at[7], ns, nr, 3, near)
    n_h4 = remote(H.at[4], H.at[6], ns, nr, 4, near)
    n_d4 = remote(D.at[4], D.at[6], ns, nr, 5, near)
    n_o = remote(ONS, ONR, ns, nr, 6, near)
    n_q = remote(DQS, DQR, ns, nr, 7, near)
    n_k = remote(DKS, DKR, ns, nr, 8, near)
    n_v = remote(VS.at[0], VR.at[0], ns, nr, 10, near)
    f_v = remote(VS.at[1], VR.at[1], fs, fr, 5, far)

    def swapped(t):
        return t + 2 - 4 * ((t // 2) % 2)

    holds = core == chip

    def n_s(t, s):
        return remote(SEND.at[s % 2], AT.at[swapped(t)], ns, nr, 11 + t, near)

    def n_s_in(t):
        return remote(SEND.at[0], AT.at[t], ns, nr, 11 + swapped(t), near)

    def tile_at(s):
        late = s // 4
        u = s % 4
        return (1 - late) * ((u + 2) % 4) + late * (4 + (u % 2) * 2 + 1 - u // 2)

    def head_phase(X):
        loads = start_loads(X)
        for c in loads:
            c.start()
        barrier = pltpu.get_barrier_semaphore()
        for to in (near, far):
            pl.semaphore_signal(barrier, inc=1, device_id={'cp': to}, device_id_type=MESH)
        pl.semaphore_wait(barrier, 2)
        loads[3].wait()
        f_d1.start()
        loads[0].wait()
        gain = lnw[...]
        shift = lnb[...]

        def norm(r, _):
            rows = pl.ds(pl.multiple_of((r % 4) * 64, 64), 64)
            x = X[r // 4, rows, :].astype(F32)
            cen = x - jnp.mean(x, axis=-1, keepdims=True)
            inv = lax.rsqrt(jnp.mean(cen * cen, axis=-1, keepdims=True) + EPS)
            H[r // 4, rows, :] = (cen * inv * gain + shift).astype(BF16)
            return _

        lax.fori_loop(0, 8, norm, 0)
        n_h.start()
        n_d.start()
        loads[1].wait()
        loads[2].wait()
        loads[4].wait()
        loads[5].wait()

    pl.run_scoped(head_phase, pltpu.VMEM((2, tile, width), BF16))

    def attention_phase(Q, DO, PS, DPS, MS, PB, DSB, OT, DQT, DQTT):
        c = scale * LOG2E

        def rope(t, ct, st):
            t = t.astype(BF16).astype(F32)
            return (t * ct + pltpu.roll(t, hd // 2, 1) * st).astype(BF16)

        def kv_tile(t, _):
            ct, st = tile_tables(cos_ref, sin_ref, tile, t)
            kv = dot(H[t], WKV[...])
            KV[t, :, :hd] = rope(kv[:, :hd] + bk[0:1, lanes_of(core, hd)], ct, st)
            KV[t, :, hd:] = (kv[:, hd:] + bv[0:1, lanes_of(core, hd)]).astype(BF16)
            return _

        def project(t, slot):
            ct, st = tile_tables(cos_ref, sin_ref, tile, t)
            q = dot(H[t], WQ[...]) + bq[0:1, lanes_of(core, qw)]
            for n in range(nh):
                Q[slot, n] = rope(q[:, n * hd:(n + 1) * hd], ct, st)
            r = dot_nt(D[t], WO[...]).astype(BF16)
            for n in range(nh):
                DO[slot, n] = r[:, n * hd:(n + 1) * hd]

        def turn(t, _):
            KT[t] = KV[t, :, :hd].T
            VT[t] = KV[t, :, hd:].T
            return _

        lax.fori_loop(0, 2, kv_tile, 0)
        f_kv.start()
        n_h.wait_recv()
        lax.fori_loop(2, 4, kv_tile, 0)
        f_kw.start()
        f_h1.start()
        f_e1.start()
        f_h0.start()
        f_d0.start()
        n_d.wait_recv()

        def first_four(t, _):
            project(t, t)
            return _

        lax.fori_loop(0, 4, first_four, 0)
        lax.fori_loop(0, 4, turn, 0)
        DK[...] = jnp.zeros_like(DK)
        DV[...] = jnp.zeros_like(DV)
        DWT[...] = jnp.zeros_like(DWT)
        f_kv.wait_recv()
        lax.fori_loop(4, 6, turn, 0)
        f_kw.wait_recv()
        lax.fori_loop(6, 8, turn, 0)

        def one_tile(s, same):
            late = s // 4
            u = s % 4
            t = tile_at(s)
            slot = (1 - late) * t + late * u

            @pl.when(s == 4)
            def _():
                f_h1.wait_recv()
                f_d1.wait_recv()
                f_e1.wait_recv()
                n_h5.start()
                n_d5.start()

            @pl.when(s == 5)
            def _():
                n_h5.wait_recv()
                n_d5.wait_recv()

            @pl.when(s == 6)
            def _():
                f_h0.wait_recv()
                f_d0.wait_recv()
                n_h4.start()
                n_d4.start()

            @pl.when(s == 7)
            def _():
                n_h4.wait_recv()
                n_d4.wait_recv()

            @pl.when(late == 1)
            def _():
                project(t, slot)

            i = piece_of(t)

            def first(j, carry, diag):
                m, l, dl = carry
                g = tile_of(j)
                kj = KV[g, :, :hd]
                vj = KV[g, :, hd:]
                m_new, l_new, d_new = [], [], []
                for n in range(nh):
                    lanes = slice(n * tile, (n + 1) * tile)
                    sc = dot_nt(kj, Q[slot, n]) * c
                    if diag:
                        key = lax.broadcasted_iota(jnp.int32, (tile, tile), 0)
                        qry = lax.broadcasted_iota(jnp.int32, (tile, tile), 1)
                        sc = jnp.where(key <= qry, sc, NEG)
                    dpb = dot_nt(vj, DO[slot, n]).astype(BF16)
                    DPS[j, :, lanes] = dpb
                    mo = m[:, lanes]
                    mn = jnp.maximum(mo, jnp.max(sc, axis=0, keepdims=True))
                    p = jnp.exp2(sc - mn)
                    PS[j, :, lanes] = p
                    al = jnp.exp2(mo - mn)
                    m_new.append(mn)
                    l_new.append(l[:, lanes] * al + jnp.sum(p, axis=0, keepdims=True))
                    d_new.append(dl[:, lanes] * al + jnp.sum(p * dpb.astype(F32), axis=0, keepdims=True))
                m = jnp.concatenate(m_new, axis=1)
                MS[j] = m
                return m, jnp.concatenate(l_new, axis=1), jnp.concatenate(d_new, axis=1)

            init = (jnp.full((1, tq), NEG, F32), jnp.zeros((1, tq), F32), jnp.zeros((1, tq), F32))
            carry = lax.fori_loop(0, i // 2, lambda h, cr: first(2 * h + 1, first(2 * h, cr, False), False), init)
            carry = lax.fori_loop(2 * (i // 2), i, lambda j, cr: first(j, cr, False), carry)
            m, l, dl = first(i, carry, True)
            inv = 1.0 / l
            delta = dl * inv
            OT[...] = jnp.zeros_like(OT)
            DQT[...] = jnp.zeros_like(DQT)

            def weigh(j, k):
                f = jnp.exp2(MS[j] - m) * inv
                for n in range(nh):
                    lanes = slice(n * tile, (n + 1) * tile)
                    p = PS[j, :, lanes] * f[:, lanes]
                    PB[k, :, lanes] = p.astype(BF16)
                    DSB[k, :, lanes] = (p * (DPS[j, :, lanes].astype(F32) - delta[:, lanes])).astype(BF16)

            def second(js, carry):
                gs = [tile_of(j) for j in js]
                for k, j in enumerate(js):
                    weigh(j, k)
                o = dot(VT[gs[0]], PB[0])
                dq = dot(KT[gs[0]], DSB[0])
                for k in range(1, len(js)):
                    o += dot(VT[gs[k]], PB[k])
                    dq += dot(KT[gs[k]], DSB[k])
                OT[...] += o
                DQT[...] += dq
                for k, g in enumerate(gs):
                    DV[g] += dot(PB[k], DO[slot].reshape(tq, hd))
                    DK[g] += dot(DSB[k], Q[slot].reshape(tq, hd))
                return carry

            pairs = (i + 1) // 2
            lax.fori_loop(0, pairs, lambda h, cr: second((2 * h, 2 * h + 1), cr), 0)
            lax.fori_loop(2 * pairs, i + 1, lambda j, cr: second((j,), cr), 0)
            ct, st = tile_tables(cos_ref, sin_ref, tile, t)
            cos_t = ct.T[:hd // 2]

            @pl.when(jnp.logical_and(holds, s >= 2))
            def _():
                n_s(tile_at(s - 2), s).wait_send()

            sin_t = st.T[hd // 2:]
            for n in range(nh):
                lanes = slice(n * tile, (n + 1) * tile)
                o_t = OT[:, lanes].astype(BF16)
                rows = slice((n % third) * hd, (n % third + 1) * hd)

                @pl.when(jnp.logical_and(holds, core == n // third))
                def _():
                    AT[t, rows, :] = o_t

                @pl.when(jnp.logical_and(holds, core != n // third))
                def _():
                    SEND[s % 2, rows, :] = o_t

                gr = (DQT[:, lanes] * scale).astype(BF16).astype(F32)
                a = gr[:hd // 2]
                e = gr[hd // 2:]
                gr = jnp.concatenate([a * cos_t + e * sin_t, e * cos_t - a * sin_t], axis=0).astype(BF16)
                cols = slice(n * hd, (n + 1) * hd)
                DQTT[cols, :] = gr

                @pl.when(t // 2 == 0)
                def _():
                    ONA[t % 2, :, cols] = o_t.T
                    DQA[t % 2, :, cols] = gr.T

                @pl.when(t // 2 == 1)
                def _():
                    ONS[t % 2, :, cols] = o_t.T
                    DQS[t % 2, :, cols] = gr.T

            @pl.when(holds)
            def _():
                n_s(t, s).start()

            @pl.when(s == 1)
            def _():
                n_o.start()
                n_q.start()

            DWT[...] += dot(DQTT[...], H[t, :, lanes_of(chip, 2 * part)])
            return same

        lax.fori_loop(0, 8, one_tile, 0)

    pl.run_scoped(attention_phase,
                  pltpu.VMEM((4, nh, tile, hd), BF16), pltpu.VMEM((4, nh, tile, hd), BF16),
                  pltpu.VMEM((8, tile, tq), F32), pltpu.VMEM((8, tile, tq), BF16), pltpu.VMEM((8, 1, tq), F32),
                  pltpu.VMEM((2, tile, tq), BF16), pltpu.VMEM((2, tile, tq), BF16), pltpu.VMEM((hd, tq), F32), pltpu.VMEM((hd, tq), F32),
                  pltpu.VMEM((qw, tile), BF16))

    def tail_phase(DWS, X, WQO, WOO, WKVO, DKVT, DWK, DWM, ACC, OUT, YB, XB):
        n_w = remote(DWS, DWR, ns, nr, 9, near)
        other = lanes_of(1 - core, hd)
        loads = [local(wq_hbm.at[:, lanes_of(1 - core, qw)], WQO, 0), local(wk_hbm.at[:, other], WKVO.at[:, :hd], 1),
                 local(wv_hbm.at[:, other], WKVO.at[:, hd:], 2), local(x_hbm, X, 3),
                 local(wo_hbm.at[lanes_of(1 - core, qw), :], WOO, 4)]
        for cp in loads:
            cp.start()

        def finish(t, same):
            ct, st = tile_tables(cos_ref, sin_ref, tile, t)
            g = (DK[t] * scale).astype(BF16).astype(F32)
            gk = (g * ct - pltpu.roll(g, hd // 2, 1) * st).astype(BF16)
            gv = DV[t].astype(BF16)
            DKVT[t, :hd, :] = gk.T
            DKVT[t, hd:, :] = gv.T

            @pl.when(t // 2 == 0)
            def _():
                DKA[t % 2, :, :hd] = gk
                DKA[t % 2, :, hd:] = gv

            @pl.when(t // 2 == 1)
            def _():
                DKS[t % 2, :, :hd] = gk
                DKS[t % 2, :, hd:] = gv

            return same

        lax.fori_loop(0, 4, finish, 0)
        n_k.start()
        lax.fori_loop(4, 8, finish, 0)

        DWK[...] = jnp.zeros_like(DWK)

        def kv_grad(t, _):
            DWK[...] += dot(DKVT[t], H[t, :, lanes_of(chip, 2 * part)])
            return _

        lax.fori_loop(0, 8, kv_grad, 0)
        theirs = lanes_of(1 - core, part)
        mine = lanes_of(core, part)
        for cp in loads[:4]:
            cp.wait()
        n_q.wait_recv()
        n_k.wait_recv()
        for t in range(2):
            ACC[t * tile:(t + 1) * tile, :] = (dot_nt(DQA[t], WQ[...]) + dot_nt(DQR[t], WQO[...])
                                               + dot_nt(DKA[t], WKV[...]) + dot_nt(DKR[t], WKVO[...]))
        for cols_of, out in ((theirs, DWS), (mine, DWM)):
            for n in range(qw // tile):
                cols = slice(n * tile, (n + 1) * tile)
                out[:, cols] = DWT[cols, cols_of].T
            out[:, qw:] = DWK[:, cols_of].T
        n_w.start()
        outs = [local(DWM, dwm_hbm, 5)]
        outs[0].start()

        @pl.when(jnp.logical_not(holds))
        def _():
            for t in range(8):
                n_s_in(t).wait_recv()

        def rowsum(v):
            return jnp.sum(v, axis=0, keepdims=True)

        VS[0] = jnp.zeros_like(VS[0])
        gain = lnw[...]
        chunk = tile // 2
        tn = width // 4

        def back(r, same):
            lanes = lanes_of(r, tn)
            acc = dot(AT[0], D[0, :, lanes])
            for t in range(1, 8):
                acc += dot(AT[t], D[t, :, lanes])
            OUT[:, lanes] = acc
            rows = pl.ds(pl.multiple_of((r % 2) * chunk, chunk), chunk)
            dh = ACC[pl.ds(pl.multiple_of(r * chunk, chunk), chunk), :].astype(BF16).astype(F32)
            x = X[r // 2, rows, :].astype(F32)
            cen = x - jnp.mean(x, axis=-1, keepdims=True)
            inv = lax.rsqrt(jnp.mean(cen * cen, axis=-1, keepdims=True) + EPS)
            xh = cen * inv
            a = dh * gain
            d = D[r // 2, rows, :].astype(F32)
            dx = inv * (a - jnp.mean(a, axis=-1, keepdims=True) - xh * jnp.mean(a * xh, axis=-1, keepdims=True))
            XB[r // 2, rows, :] = (d + dx).astype(BF16)
            VS[0, 0:1, :] += rowsum(dh * xh)
            VS[0, 1:2, :] += rowsum(dh)
            VS[0, 2:3, :] += rowsum(d)
            return same

        lax.fori_loop(0, 4, back, 0)
        for side, q, k in ((core, DQA, DKA), (1 - core, DQR, DKR)):
            qs = rowsum(q[0].astype(F32)) + rowsum(q[1].astype(F32))
            ks = rowsum(k[0].astype(F32)) + rowsum(k[1].astype(F32))
            VS[0, 3:4, lanes_of(side, qw)] = qs
            VS[0, 4:5, lanes_of(side, hd)] = ks[:, :hd]
            VS[0, 5:6, lanes_of(side, hd)] = ks[:, hd:]
        n_v.start()
        outs += [local(XB, dx_hbm, 8), local(OUT, dwo_hbm, 10)]
        outs[1].start()
        outs[2].start()

        loads[4].wait()
        n_o.wait_recv()

        def y_tile(t):
            z = dot(ONA[t], WO[...]) + dot(ONR[t], WOO[...])
            YB[t] = (X[t].astype(F32) + (z + bo[...])).astype(BF16)

        y_tile(0)
        n_v.wait_recv()
        VS[1] = VS[0] + VR[0]
        f_v.start()
        y_tile(1)
        outs.append(local(YB, y_hbm, 9))
        outs[-1].start()
        n_w.wait_recv()
        f_v.wait_recv()
        vec_ref[...] = VS[1] + VR[1]
        for cp in outs:
            cp.wait()
        n_w.wait_send()

    pl.run_scoped(tail_phase,
                  pltpu.VMEM((part, qw + 2 * hd), F32), pltpu.VMEM((2, tile, width), BF16), pltpu.VMEM((width, qw), BF16), pltpu.VMEM((qw, width), BF16),
                  pltpu.VMEM((width, 2 * hd), BF16), pltpu.VMEM((8, 2 * hd, tile), BF16), pltpu.VMEM((2 * hd, 2 * part), F32),
                  pltpu.VMEM((part, qw + 2 * hd), F32), pltpu.VMEM((2 * tile, width), F32),
                  pltpu.VMEM((part, width), F32), pltpu.VMEM((2, tile, width), BF16), pltpu.VMEM((2, tile, width), BF16))

    for cp in (n_h, n_d, f_kv, f_kw, f_h1, f_d1, f_e1, f_h0, f_d0, n_h5, n_d5, n_h4, n_d4, n_o, n_q, n_k, n_v, f_v):
        cp.wait_send()

    @pl.when(holds)
    def _():
        for s in (6, 7):
            n_s(tile_at(s), s).wait_send()


def mega(x, d, wq, wk, wv, wo, small, cos_t, sin_t, nh, hd, scale):
    _, tile, width = x.shape
    qw = nh * hd
    part = width // 4
    anywhere = pl.BlockSpec(memory_space=pltpu.HBM)
    vmem = pl.BlockSpec(memory_space=pltpu.VMEM)
    rows = (2, tile, width)

    def vm(*shape, dtype=BF16):
        return pltpu.VMEM(shape, dtype)

    return pl.pallas_call(
        functools.partial(mega_body, nh, hd, tile, scale),
        in_specs=[anywhere] * 6 + [vmem] * 8,
        out_specs=[anywhere] * 5 + [vmem],
        out_shape=[jax.ShapeDtypeStruct(rows, BF16), jax.ShapeDtypeStruct(rows, BF16),
                   jax.ShapeDtypeStruct((part, qw + 2 * hd), F32), jax.ShapeDtypeStruct((part, qw + 2 * hd), F32),
                   jax.ShapeDtypeStruct((part, width), F32),
                   jax.ShapeDtypeStruct((8, width), F32)],
        scratch_shapes=[
            vm(8, tile, width), vm(8, tile, width), vm(8, tile, 2 * hd), vm(8, hd, tile), vm(8, hd, tile),
            vm(width, qw), vm(qw, width), vm(width, 2 * hd),
            vm(8, tile, hd, dtype=F32), vm(8, tile, hd, dtype=F32),
            vm(8, part, tile), vm(2, part, tile), vm(qw, 2 * part, dtype=F32),
            vm(2, tile, qw), vm(2, tile, qw), vm(2, tile, qw), vm(2, tile, qw), vm(2, tile, qw), vm(2, tile, qw),
            vm(2, tile, 2 * hd), vm(2, tile, 2 * hd), vm(2, tile, 2 * hd),
            vm(2, 8, width, dtype=F32), vm(2, 8, width, dtype=F32), vm(8, width, dtype=F32),
            pltpu.SemaphoreType.DMA((8,)), pltpu.SemaphoreType.DMA((8,)),
            pltpu.SemaphoreType.DMA((19,)), pltpu.SemaphoreType.DMA((19,)), pltpu.SemaphoreType.DMA((14,))],
        compiler_params=pltpu.CompilerParams(collective_id=0, has_side_effects=True, vmem_limit_bytes=67043328),
        name="sublayer",
    )(x, d, wq, wk, wv, wo, *small, cos_t, sin_t)


def finish_body(hd, c_ref, y_ref, dx_ref, m_ref, t_ref, o_ref, v_ref, y_out, dx_out, q_out, k_out, v_out, o_out, *vecs):
    core = c_ref[0]
    y_out[...] = y_ref[...]
    dx_out[...] = dx_ref[...]
    o_out[...] = o_ref[...]
    qw = q_out.shape[1] // 2
    for side, r in ((core, m_ref), (1 - core, t_ref)):
        q_out[:, pl.ds(pl.multiple_of(side * qw, 128), qw)] = r[:, :qw]
        k_out[:, pl.ds(pl.multiple_of(side * hd, 128), hd)] = r[:, qw:qw + hd]
        v_out[:, pl.ds(pl.multiple_of(side * hd, 128), hd)] = r[:, qw + hd:]

    @pl.when(pl.program_id(0) == 0)
    def _():
        for n, r in enumerate(vecs):
            r[...] = v_ref[n:n + 1, :r.shape[0]].reshape(r.shape[0])


def finish(core, y, dx, mine, theirs, d_wo, vec, hd, kvw, steps=4):
    rows, width = y.shape
    part, cols = mine.shape
    qw = cols - 2 * hd

    def tall(r, c):
        return pl.BlockSpec((r // steps, c), lambda i, s: (i, 0))

    dims = [(rows, width), (rows, width), (part, 2 * qw), (part, 2 * hd), (part, 2 * hd), (part, width)]
    lens = [width] * 4 + [kvw] * 2
    return pl.pallas_call(
        functools.partial(finish_body, hd),
        grid_spec=pltpu.PrefetchScalarGridSpec(
            num_scalar_prefetch=1, grid=(steps,),
            in_specs=[tall(rows, width), tall(rows, width), tall(part, cols), tall(part, cols), tall(part, width),
                      pl.BlockSpec(vec.shape, lambda i, s: (0, 0))],
            out_specs=[tall(*d) for d in dims] + [pl.BlockSpec((n,), lambda i, s: (0,)) for n in lens]),
        out_shape=[jax.ShapeDtypeStruct(d, BF16 if n < 2 else F32) for n, d in enumerate(dims)]
        + [jax.ShapeDtypeStruct((n,), F32) for n in lens],
        compiler_params=pltpu.CompilerParams(dimension_semantics=("arbitrary",), vmem_limit_bytes=67043328),
        name="finish",
    )(core, y, dx, mine, theirs, d_wo, vec)


def solution(mesh):
    groups = mesh.shape['cp']
    row_spec = P('dp', 'cp', None)
    mat_spec = P(('dp', 'cp'), None)
    vec_spec = P('dp')

    def device_fn(x_in, ln_w, ln_b, w_q, b_q, w_k, b_k, w_v, b_v, w_o, b_o, long_factor, dy_out):
        rank = lax.axis_index('cp').astype(jnp.int32)
        tokens, width = x_in.shape[1:]
        piece = tokens // 2
        hd = 2 * long_factor.shape[0]
        kvw = w_k.shape[1]
        nh = w_q.shape[1] // kvw
        blocks = jnp.stack([rank, rank ^ 1, rank ^ 2, rank ^ 3])
        rel = jnp.stack([blocks, 2 * groups - 1 - blocks], axis=1).reshape(2 * groups)
        cos_t, sin_t = rope_tables(rel * piece, piece, long_factor)
        small = (ln_w, ln_b, b_q, b_o, b_k, b_v)
        y, dx, mine, theirs, d_wo, vec = mega(
            x_in.reshape(2, piece, width), dy_out.reshape(2, piece, width), w_q, w_k, w_v, w_o,
            small, cos_t, sin_t, nh, hd, hd ** -0.5)
        y, dx, d_wq, d_wk, d_wv, d_wo, d_lnw, d_lnb, d_bo, d_bq, d_bk, d_bv = finish(
            (rank % 2)[None], y.reshape(tokens, width), dx.reshape(tokens, width), mine, theirs, d_wo, vec, hd, kvw)
        shape = (1, tokens, width)
        return (y.reshape(shape), dx.reshape(shape), d_wq, d_wk, d_wv, d_wo, d_lnw, d_lnb, d_bq, d_bk, d_bv, d_bo)

    in_specs = (row_spec,) + (P(),) * 11 + (row_spec,)
    out_specs = (row_spec, row_spec) + (mat_spec,) * 4 + (vec_spec,) * 6
    return jax.shard_map(device_fn, mesh=mesh, in_specs=in_specs, out_specs=out_specs, check_vma=False)
```

```python
import functools
import math
import jax
import jax.numpy as jnp
from jax import lax
from jax.experimental import pallas as pl
from jax.experimental.pallas import tpu as pltpu
from jax.sharding import PartitionSpec as P

EPS = 1e-5
THETA = 10000.0
ROPE_SCALE = math.sqrt(1.0 + math.log(32.0) / math.log(4096.0))
LOG2E = math.log2(math.e)
NEG = -1e30
F32 = jnp.float32
BF16 = jnp.bfloat16


def dot(a, b):
    return lax.dot_general(a, b, (((1,), (0,)), ((), ())), preferred_element_type=F32)


def dot_nt(a, b):
    return lax.dot_general(a, b, (((1,), (1,)), ((), ())), preferred_element_type=F32)


def dot_tn(a, b):
    return lax.dot_general(a, b, (((0,), (0,)), ((), ())), preferred_element_type=F32)


def rope_tables(starts, piece, long_factor):
    half_dim = long_factor.shape[0]
    exponent = jnp.arange(half_dim, dtype=F32) * (1.0 / half_dim)
    inv_freq = jnp.tile(1.0 / (long_factor * THETA ** exponent), 2)
    sign = jnp.where(jnp.arange(2 * half_dim) < half_dim, -1.0, 1.0)
    positions = jnp.concatenate([jnp.arange(piece, dtype=jnp.int32), starts])
    angle = positions.astype(F32)[:, None] * inv_freq[None, :]
    return jnp.cos(angle), jnp.sin(angle) * sign[None, :]


def tile_tables(cos_ref, sin_ref, piece, t):
    ca = cos_ref[pl.ds(piece + t, 1), :] * ROPE_SCALE
    sa = sin_ref[pl.ds(piece + t, 1), :] * ROPE_SCALE
    cb = cos_ref[:piece, :]
    sb = sin_ref[:piece, :]
    return ca * cb - sa * sb, sa * cb + ca * sb


MESH = pl.DeviceIdType.MESH


def mega_body(nh, hd, tile, scale,
              x_hbm, d_hbm, wq_hbm, wk_hbm, wv_hbm, wo_hbm, lnw1, lnb1, bq1, bo1, bk1, bv1, cos_ref, sin_ref,
              y_hbm, dx_hbm, dwm_hbm, DWR, dwo_hbm, vec_ref,
              H, D, KV, KT, VT, WQ, WO, WKV, DK, DV, AT, SEND, DWT, ONA, ONS, ONR, DQA, DQS, DQR, DKA, DKS, DKR,
              VS, VR, SM, fs, fr, ns, nr, ls):
    rank = lax.axis_index('cp')
    core = rank % 2
    chip = rank // 2
    near = rank + 1 - 2 * core
    far = rank + 2 - 4 * chip
    tq = nh * tile
    qw = nh * hd
    width = H.shape[2]
    part = width // 4
    third = nh // 2
    lnw, lnb, bq, bo, bk, bv = (SM.at[n:n + 1, :] for n in range(6))
    for n, r in enumerate((lnw1, lnb1, bq1, bo1, bk1, bv1)):
        SM[n:n + 1, :r.shape[0]] = r[...].astype(F32).reshape(1, r.shape[0])

    def local(src, dst, n):
        return pltpu.make_async_copy(src, dst, ls.at[n])

    def remote(src, dst, send, recv, n, to):
        return pltpu.make_async_remote_copy(src_ref=src, dst_ref=dst, send_sem=send.at[n], recv_sem=recv.at[n],
                                            device_id={'cp': to}, device_id_type=MESH)

    def lanes_of(i, n):
        return pl.ds(pl.multiple_of(i * n, 128), n)

    def piece_of(t):
        k = t // 2
        b = (rank % 2 + k % 2) % 2 + 2 * ((rank // 2 + k // 2) % 2)
        return b + (t % 2) * (7 - 2 * b)

    def tile_of(p):
        up = p // 4
        b = p + up * (7 - 2 * p)
        k = (rank % 2 + b % 2) % 2 + 2 * ((rank // 2 + b // 2) % 2)
        return 2 * k + up

    def start_loads(X):
        mine = lanes_of(core, hd)
        return [local(x_hbm, X, 0), local(wk_hbm.at[:, mine], WKV.at[:, :hd], 1), local(wv_hbm.at[:, mine], WKV.at[:, hd:], 2),
                local(d_hbm, D.at[0:2], 3), local(wq_hbm.at[:, lanes_of(core, qw)], WQ, 4),
                local(wo_hbm.at[lanes_of(core, qw), :], WO, 5)]

    n_h = remote(H.at[0:2], H.at[2:4], ns, nr, 0, near)
    n_d = remote(D.at[0:2], D.at[2:4], ns, nr, 1, near)
    f_kv = remote(KV.at[0:2], KV.at[4:6], fs, fr, 0, far)
    f_kw = remote(KV.at[2:4], KV.at[6:8], fs, fr, 6, far)
    f_h1 = remote(H.at[1], H.at[5], fs, fr, 1, far)
    f_d1 = remote(D.at[1, :tile // 2], D.at[5, :tile // 2], fs, fr, 2, far)
    f_e1 = remote(D.at[1, tile // 2:], D.at[5, tile // 2:], fs, fr, 7, far)
    f_h0 = remote(H.at[0], H.at[4], fs, fr, 3, far)
    f_d0 = remote(D.at[0], D.at[4], fs, fr, 4, far)
    n_h5 = remote(H.at[5], H.at[7], ns, nr, 2, near)
    n_d5 = remote(D.at[5], D.at[7], ns, nr, 3, near)
    n_h4 = remote(H.at[4], H.at[6], ns, nr, 4, near)
    n_d4 = remote(D.at[4], D.at[6], ns, nr, 5, near)
    n_o = remote(ONS, ONR, ns, nr, 6, near)
    n_q = remote(DQS, DQR, ns, nr, 7, near)
    n_k = remote(DKS, DKR, ns, nr, 8, near)
    n_v = remote(VS.at[0], VR.at[0], ns, nr, 10, near)
    f_v = remote(VS.at[1], VR.at[1], fs, fr, 5, far)

    def swapped(t):
        return t + 2 - 4 * ((t // 2) % 2)

    holds = core == chip

    def n_s(t, s):
        return remote(SEND.at[s % 2], AT.at[swapped(t)], ns, nr, 11 + t, near)

    def n_s_in(t):
        return remote(SEND.at[0], AT.at[t], ns, nr, 11 + swapped(t), near)

    def tile_at(s):
        late = s // 4
        u = s % 4
        return (1 - late) * ((u + 2) % 4) + late * (4 + (u % 2) * 2 + 1 - u // 2)

    def head_phase(X):
        loads = start_loads(X)
        for c in loads:
            c.start()
        barrier = pltpu.get_barrier_semaphore()
        for to in (near, far):
            pl.semaphore_signal(barrier, inc=1, device_id={'cp': to}, device_id_type=MESH)
        pl.semaphore_wait(barrier, 2)
        loads[3].wait()
        f_d1.start()
        loads[0].wait()
        gain = lnw[...]
        shift = lnb[...]

        def norm(r, _):
            rows = pl.ds(pl.multiple_of((r % 4) * 64, 64), 64)
            x = X[r // 4, rows, :].astype(F32)
            cen = x - jnp.mean(x, axis=-1, keepdims=True)
            inv = lax.rsqrt(jnp.mean(cen * cen, axis=-1, keepdims=True) + EPS)
            H[r // 4, rows, :] = (cen * inv * gain + shift).astype(BF16)
            return _

        lax.fori_loop(0, 8, norm, 0)
        n_h.start()
        n_d.start()
        loads[1].wait()
        loads[2].wait()
        loads[4].wait()
        loads[5].wait()

    pl.run_scoped(head_phase, pltpu.VMEM((2, tile, width), BF16))

    def attention_phase(Q, DO, PS, DPS, MS, PB, DSB, OT, DQT, DQTT):
        c = scale * LOG2E

        def rope(t, ct, st):
            t = t.astype(BF16).astype(F32)
            return (t * ct + pltpu.roll(t, hd // 2, 1) * st).astype(BF16)

        def kv_tile(t, _):
            ct, st = tile_tables(cos_ref, sin_ref, tile, t)
            kv = dot(H[t], WKV[...])
            KV[t, :, :hd] = rope(kv[:, :hd] + bk[0:1, lanes_of(core, hd)], ct, st)
            KV[t, :, hd:] = (kv[:, hd:] + bv[0:1, lanes_of(core, hd)]).astype(BF16)
            return _

        def project(t, slot):
            ct, st = tile_tables(cos_ref, sin_ref, tile, t)
            q = dot(H[t], WQ[...]) + bq[0:1, lanes_of(core, qw)]
            for n in range(nh):
                Q[slot, n] = rope(q[:, n * hd:(n + 1) * hd], ct, st)
            r = dot_nt(D[t], WO[...]).astype(BF16)
            for n in range(nh):
                DO[slot, n] = r[:, n * hd:(n + 1) * hd]

        def turn(t, _):
            KT[t] = KV[t, :, :hd].T
            VT[t] = KV[t, :, hd:].T
            return _

        lax.fori_loop(0, 2, kv_tile, 0)
        f_kv.start()
        n_h.wait_recv()
        lax.fori_loop(2, 4, kv_tile, 0)
        f_kw.start()
        f_h1.start()
        f_e1.start()
        f_h0.start()
        f_d0.start()

        def first_four(t, _):
            project(t, t)
            return _

        lax.fori_loop(0, 2, first_four, 0)
        n_d.wait_recv()
        lax.fori_loop(2, 4, first_four, 0)
        lax.fori_loop(0, 4, turn, 0)
        DK[...] = jnp.zeros_like(DK)
        DV[...] = jnp.zeros_like(DV)
        DWT[...] = jnp.zeros_like(DWT)
        f_kv.wait_recv()
        lax.fori_loop(4, 6, turn, 0)
        f_kw.wait_recv()
        lax.fori_loop(6, 8, turn, 0)

        def one_tile(s, same):
            late = s // 4
            u = s % 4
            t = tile_at(s)
            slot = (1 - late) * t + late * u

            @pl.when(s == 4)
            def _():
                f_h1.wait_recv()
                f_d1.wait_recv()
                f_e1.wait_recv()
                n_h5.start()
                n_d5.start()

            @pl.when(s == 5)
            def _():
                n_h5.wait_recv()
                n_d5.wait_recv()

            @pl.when(s == 6)
            def _():
                f_h0.wait_recv()
                f_d0.wait_recv()
                n_h4.start()
                n_d4.start()

            @pl.when(s == 7)
            def _():
                n_h4.wait_recv()
                n_d4.wait_recv()

            @pl.when(late == 1)
            def _():
                project(t, slot)

            i = piece_of(t)

            def first(j, carry, diag):
                m, l, dl = carry
                g = tile_of(j)
                kj = KV[g, :, :hd]
                vj = KV[g, :, hd:]
                m_new, l_new, d_new = [], [], []
                for n in range(nh):
                    lanes = slice(n * tile, (n + 1) * tile)
                    sc = dot_nt(kj, Q[slot, n]) * c
                    if diag:
                        key = lax.broadcasted_iota(jnp.int32, (tile, tile), 0)
                        qry = lax.broadcasted_iota(jnp.int32, (tile, tile), 1)
                        sc = jnp.where(key <= qry, sc, NEG)
                    dpb = dot_nt(vj, DO[slot, n]).astype(BF16)
                    DPS[j, :, lanes] = dpb
                    mo = m[:, lanes]
                    mn = jnp.maximum(mo, jnp.max(sc, axis=0, keepdims=True))
                    p = jnp.exp2(sc - mn)
                    PS[j, :, lanes] = p
                    al = jnp.exp2(mo - mn)
                    m_new.append(mn)
                    l_new.append(l[:, lanes] * al + jnp.sum(p, axis=0, keepdims=True))
                    d_new.append(dl[:, lanes] * al + jnp.sum(p * dpb.astype(F32), axis=0, keepdims=True))
                m = jnp.concatenate(m_new, axis=1)
                MS[j] = m
                return m, jnp.concatenate(l_new, axis=1), jnp.concatenate(d_new, axis=1)

            init = (jnp.full((1, tq), NEG, F32), jnp.zeros((1, tq), F32), jnp.zeros((1, tq), F32))
            carry = lax.fori_loop(0, i // 2, lambda h, cr: first(2 * h + 1, first(2 * h, cr, False), False), init)
            carry = lax.fori_loop(2 * (i // 2), i, lambda j, cr: first(j, cr, False), carry)
            m, l, dl = first(i, carry, True)
            inv = 1.0 / l
            delta = dl * inv
            OT[...] = jnp.zeros_like(OT)
            DQT[...] = jnp.zeros_like(DQT)

            def weigh(j, k):
                f = jnp.exp2(MS[j] - m) * inv
                for n in range(nh):
                    lanes = slice(n * tile, (n + 1) * tile)
                    p = PS[j, :, lanes] * f[:, lanes]
                    PB[k, :, lanes] = p.astype(BF16)
                    DSB[k, :, lanes] = (p * (DPS[j, :, lanes].astype(F32) - delta[:, lanes])).astype(BF16)

            def second(js, carry):
                gs = [tile_of(j) for j in js]
                for k, j in enumerate(js):
                    weigh(j, k)
                o = dot(VT[gs[0]], PB[0])
                dq = dot(KT[gs[0]], DSB[0])
                for k in range(1, len(js)):
                    o += dot(VT[gs[k]], PB[k])
                    dq += dot(KT[gs[k]], DSB[k])
                OT[...] += o
                DQT[...] += dq
                for k, g in enumerate(gs):
                    DV[g] += dot(PB[k], DO[slot].reshape(tq, hd))
                    DK[g] += dot(DSB[k], Q[slot].reshape(tq, hd))
                return carry

            pairs = (i + 1) // 2
            lax.fori_loop(0, pairs, lambda h, cr: second((2 * h, 2 * h + 1), cr), 0)
            lax.fori_loop(2 * pairs, i + 1, lambda j, cr: second((j,), cr), 0)
            ct, st = tile_tables(cos_ref, sin_ref, tile, t)
            cos_t = ct.T[:hd // 2]

            @pl.when(jnp.logical_and(holds, s >= 2))
            def _():
                n_s(tile_at(s - 2), s).wait_send()

            sin_t = st.T[hd // 2:]
            for n in range(nh):
                lanes = slice(n * tile, (n + 1) * tile)
                gr = (DQT[:, lanes] * scale).astype(BF16).astype(F32)
                a = gr[:hd // 2]
                e = gr[hd // 2:]
                gr = jnp.concatenate([a * cos_t + e * sin_t, e * cos_t - a * sin_t], axis=0).astype(BF16)
                DQTT[s % 2, n * hd:(n + 1) * hd, :] = gr

            for h in range(2):
                @pl.when(jnp.logical_and(holds, core == h))
                def _():
                    for n in range(nh):
                        o_t = OT[:, n * tile:(n + 1) * tile].astype(BF16)
                        rows = slice((n % third) * hd, (n % third + 1) * hd)
                        if n // third == h:
                            AT[t, rows, :] = o_t
                        else:
                            SEND[s % 2, rows, :] = o_t

            for h, (o_out, q_out) in enumerate(((ONA, DQA), (ONS, DQS))):
                @pl.when(t // 2 == h)
                def _():
                    for n in range(nh):
                        cols = slice(n * hd, (n + 1) * hd)
                        o_out[t % 2, :, cols] = OT[:, n * tile:(n + 1) * tile].astype(BF16).T
                        q_out[t % 2, :, cols] = DQTT[s % 2, cols, :].T

            @pl.when(holds)
            def _():
                n_s(t, s).start()

            @pl.when(s == 1)
            def _():
                n_o.start()
                n_q.start()

            @pl.when(s % 2 == 1)
            def _():
                cols = lanes_of(chip, 2 * part)
                DWT[...] += dot(DQTT[0], H[tile_at(s - 1), :, cols]) + dot(DQTT[1], H[t, :, cols])

            return same

        lax.fori_loop(0, 8, one_tile, 0)

    pl.run_scoped(attention_phase,
                  pltpu.VMEM((4, nh, tile, hd), BF16), pltpu.VMEM((4, nh, tile, hd), BF16),
                  pltpu.VMEM((8, tile, tq), F32), pltpu.VMEM((8, tile, tq), BF16), pltpu.VMEM((8, 1, tq), F32),
                  pltpu.VMEM((2, tile, tq), BF16), pltpu.VMEM((2, tile, tq), BF16), pltpu.VMEM((hd, tq), F32), pltpu.VMEM((hd, tq), F32),
                  pltpu.VMEM((2, qw, tile), BF16))

    def tail_phase(DWS, X, WQO, WOO, WKVO, DKVT, DWK, DWM, ACC, OUT, YB, XB):
        n_w = remote(DWS, DWR, ns, nr, 9, near)
        other = lanes_of(1 - core, hd)
        loads = [local(wq_hbm.at[:, lanes_of(1 - core, qw)], WQO, 0), local(wk_hbm.at[:, other], WKVO.at[:, :hd], 1),
                 local(wv_hbm.at[:, other], WKVO.at[:, hd:], 2), local(x_hbm, X, 3),
                 local(wo_hbm.at[lanes_of(1 - core, qw), :], WOO, 4)]
        for cp in loads:
            cp.start()

        def finish(t, same):
            ct, st = tile_tables(cos_ref, sin_ref, tile, t)
            g = (DK[t] * scale).astype(BF16).astype(F32)
            gk = (g * ct - pltpu.roll(g, hd // 2, 1) * st).astype(BF16)
            gv = DV[t].astype(BF16)
            DKVT[t, :hd, :] = gk.T
            DKVT[t, hd:, :] = gv.T

            @pl.when(t // 2 == 0)
            def _():
                DKA[t % 2, :, :hd] = gk
                DKA[t % 2, :, hd:] = gv

            @pl.when(t // 2 == 1)
            def _():
                DKS[t % 2, :, :hd] = gk
                DKS[t % 2, :, hd:] = gv

            return same

        lax.fori_loop(0, 4, finish, 0)
        n_k.start()
        lax.fori_loop(4, 8, finish, 0)

        chip_cols = lanes_of(chip, 2 * part)
        acc = dot(DKVT[0], H[0, :, chip_cols])
        for t in range(1, 8):
            acc += dot(DKVT[t], H[t, :, chip_cols])
        DWK[...] = acc
        theirs = lanes_of(1 - core, part)
        mine = lanes_of(core, part)
        for cp in loads[:4]:
            cp.wait()
        n_q.wait_recv()
        n_k.wait_recv()
        for t in range(2):
            ACC[t * tile:(t + 1) * tile, :] = (dot_nt(DQA[t], WQ[...]) + dot_nt(DQR[t], WQO[...])
                                               + dot_nt(DKA[t], WKV[...]) + dot_nt(DKR[t], WKVO[...]))
        for cols_of, out in ((theirs, DWS), (mine, DWM)):
            for n in range(qw // tile):
                cols = slice(n * tile, (n + 1) * tile)
                out[:, cols] = DWT[cols, cols_of].T
            out[:, qw:] = DWK[:, cols_of].T
        n_w.start()
        outs = [local(DWM, dwm_hbm, 5)]
        outs[0].start()

        @pl.when(jnp.logical_not(holds))
        def _():
            for t in range(8):
                n_s_in(t).wait_recv()

        def rowsum(v):
            return jnp.sum(v, axis=0, keepdims=True)

        VS[0] = jnp.zeros_like(VS[0])
        gain = lnw[...]
        chunk = tile // 2
        tn = width // 4

        def back(r, same):
            lanes = lanes_of(r, tn)
            acc = dot(AT[0], D[0, :, lanes])
            for t in range(1, 8):
                acc += dot(AT[t], D[t, :, lanes])
            OUT[:, lanes] = acc
            rows = pl.ds(pl.multiple_of((r % 2) * chunk, chunk), chunk)
            dh = ACC[pl.ds(pl.multiple_of(r * chunk, chunk), chunk), :].astype(BF16).astype(F32)
            x = X[r // 2, rows, :].astype(F32)
            cen = x - jnp.mean(x, axis=-1, keepdims=True)
            inv = lax.rsqrt(jnp.mean(cen * cen, axis=-1, keepdims=True) + EPS)
            xh = cen * inv
            a = dh * gain
            d = D[r // 2, rows, :].astype(F32)
            dx = inv * (a - jnp.mean(a, axis=-1, keepdims=True) - xh * jnp.mean(a * xh, axis=-1, keepdims=True))
            XB[r // 2, rows, :] = (d + dx).astype(BF16)
            VS[0, 0:1, :] += rowsum(dh * xh)
            VS[0, 1:2, :] += rowsum(dh)
            VS[0, 2:3, :] += rowsum(d)
            return same

        lax.fori_loop(0, 4, back, 0)
        for side, q, k in ((core, DQA, DKA), (1 - core, DQR, DKR)):
            qs = rowsum(q[0].astype(F32)) + rowsum(q[1].astype(F32))
            ks = rowsum(k[0].astype(F32)) + rowsum(k[1].astype(F32))
            VS[0, 3:4, lanes_of(side, qw)] = qs
            VS[0, 4:5, lanes_of(side, hd)] = ks[:, :hd]
            VS[0, 5:6, lanes_of(side, hd)] = ks[:, hd:]
        n_v.start()
        outs += [local(XB, dx_hbm, 8), local(OUT, dwo_hbm, 10)]
        outs[1].start()
        outs[2].start()

        loads[4].wait()
        n_o.wait_recv()

        def y_tile(t):
            z = dot(ONA[t], WO[...]) + dot(ONR[t], WOO[...])
            YB[t] = (X[t].astype(F32) + (z + bo[...])).astype(BF16)

        y_tile(0)
        n_v.wait_recv()
        VS[1] = VS[0] + VR[0]
        f_v.start()
        y_tile(1)
        outs.append(local(YB, y_hbm, 9))
        outs[-1].start()
        n_w.wait_recv()
        f_v.wait_recv()
        vec_ref[...] = VS[1] + VR[1]
        for cp in outs:
            cp.wait()
        n_w.wait_send()

    pl.run_scoped(tail_phase,
                  pltpu.VMEM((part, qw + 2 * hd), F32), pltpu.VMEM((2, tile, width), BF16), pltpu.VMEM((width, qw), BF16), pltpu.VMEM((qw, width), BF16),
                  pltpu.VMEM((width, 2 * hd), BF16), pltpu.VMEM((8, 2 * hd, tile), BF16), pltpu.VMEM((2 * hd, 2 * part), F32),
                  pltpu.VMEM((part, qw + 2 * hd), F32), pltpu.VMEM((2 * tile, width), F32),
                  pltpu.VMEM((part, width), F32), pltpu.VMEM((2, tile, width), BF16), pltpu.VMEM((2, tile, width), BF16))

    for cp in (n_h, n_d, f_kv, f_kw, f_h1, f_d1, f_e1, f_h0, f_d0, n_h5, n_d5, n_h4, n_d4, n_o, n_q, n_k, n_v, f_v):
        cp.wait_send()

    @pl.when(holds)
    def _():
        for s in (6, 7):
            n_s(tile_at(s), s).wait_send()


def mega(x, d, wq, wk, wv, wo, small, cos_t, sin_t, nh, hd, scale):
    _, tile, width = x.shape
    qw = nh * hd
    part = width // 4
    anywhere = pl.BlockSpec(memory_space=pltpu.HBM)
    vmem = pl.BlockSpec(memory_space=pltpu.VMEM)
    rows = (2, tile, width)

    def vm(*shape, dtype=BF16):
        return pltpu.VMEM(shape, dtype)

    return pl.pallas_call(
        functools.partial(mega_body, nh, hd, tile, scale),
        in_specs=[anywhere] * 6 + [vmem] * 8,
        out_specs=[anywhere] * 5 + [vmem],
        out_shape=[jax.ShapeDtypeStruct(rows, BF16), jax.ShapeDtypeStruct(rows, BF16),
                   jax.ShapeDtypeStruct((part, qw + 2 * hd), F32), jax.ShapeDtypeStruct((part, qw + 2 * hd), F32),
                   jax.ShapeDtypeStruct((part, width), F32),
                   jax.ShapeDtypeStruct((8, width), F32)],
        scratch_shapes=[
            vm(8, tile, width), vm(8, tile, width), vm(8, tile, 2 * hd), vm(8, hd, tile), vm(8, hd, tile),
            vm(width, qw), vm(qw, width), vm(width, 2 * hd),
            vm(8, tile, hd, dtype=F32), vm(8, tile, hd, dtype=F32),
            vm(8, part, tile), vm(2, part, tile), vm(qw, 2 * part, dtype=F32),
            vm(2, tile, qw), vm(2, tile, qw), vm(2, tile, qw), vm(2, tile, qw), vm(2, tile, qw), vm(2, tile, qw),
            vm(2, tile, 2 * hd), vm(2, tile, 2 * hd), vm(2, tile, 2 * hd),
            vm(2, 8, width, dtype=F32), vm(2, 8, width, dtype=F32), vm(8, width, dtype=F32),
            pltpu.SemaphoreType.DMA((8,)), pltpu.SemaphoreType.DMA((8,)),
            pltpu.SemaphoreType.DMA((19,)), pltpu.SemaphoreType.DMA((19,)), pltpu.SemaphoreType.DMA((14,))],
        compiler_params=pltpu.CompilerParams(collective_id=0, has_side_effects=True, vmem_limit_bytes=67043328),
        name="sublayer",
    )(x, d, wq, wk, wv, wo, *small, cos_t, sin_t)


def finish_body(hd, c_ref, y_ref, dx_ref, m_ref, t_ref, o_ref, v_ref, y_out, dx_out, q_out, k_out, v_out, o_out, *vecs):
    core = c_ref[0]
    y_out[...] = y_ref[...]
    dx_out[...] = dx_ref[...]
    o_out[...] = o_ref[...]
    qw = q_out.shape[1] // 2
    for side, r in ((core, m_ref), (1 - core, t_ref)):
        q_out[:, pl.ds(pl.multiple_of(side * qw, 128), qw)] = r[:, :qw]
        k_out[:, pl.ds(pl.multiple_of(side * hd, 128), hd)] = r[:, qw:qw + hd]
        v_out[:, pl.ds(pl.multiple_of(side * hd, 128), hd)] = r[:, qw + hd:]

    @pl.when(pl.program_id(0) == 0)
    def _():
        for n, r in enumerate(vecs):
            r[...] = v_ref[n:n + 1, :r.shape[0]].reshape(r.shape[0])


def finish(core, y, dx, mine, theirs, d_wo, vec, hd, kvw, steps=2):
    rows, width = y.shape
    part, cols = mine.shape
    qw = cols - 2 * hd

    def tall(r, c):
        return pl.BlockSpec((r // steps, c), lambda i, s: (i, 0))

    dims = [(rows, width), (rows, width), (part, 2 * qw), (part, 2 * hd), (part, 2 * hd), (part, width)]
    lens = [width] * 4 + [kvw] * 2
    return pl.pallas_call(
        functools.partial(finish_body, hd),
        grid_spec=pltpu.PrefetchScalarGridSpec(
            num_scalar_prefetch=1, grid=(steps,),
            in_specs=[tall(rows, width), tall(rows, width), tall(part, cols), tall(part, cols), tall(part, width),
                      pl.BlockSpec(vec.shape, lambda i, s: (0, 0))],
            out_specs=[tall(*d) for d in dims] + [pl.BlockSpec((n,), lambda i, s: (0,)) for n in lens]),
        out_shape=[jax.ShapeDtypeStruct(d, BF16 if n < 2 else F32) for n, d in enumerate(dims)]
        + [jax.ShapeDtypeStruct((n,), F32) for n in lens],
        compiler_params=pltpu.CompilerParams(dimension_semantics=("arbitrary",), vmem_limit_bytes=67043328),
        name="finish",
    )(core, y, dx, mine, theirs, d_wo, vec)


def solution(mesh):
    groups = mesh.shape['cp']
    row_spec = P('dp', 'cp', None)
    mat_spec = P(('dp', 'cp'), None)
    vec_spec = P('dp')

    def device_fn(x_in, ln_w, ln_b, w_q, b_q, w_k, b_k, w_v, b_v, w_o, b_o, long_factor, dy_out):
        rank = lax.axis_index('cp').astype(jnp.int32)
        tokens, width = x_in.shape[1:]
        piece = tokens // 2
        hd = 2 * long_factor.shape[0]
        kvw = w_k.shape[1]
        nh = w_q.shape[1] // kvw
        blocks = jnp.stack([rank, rank ^ 1, rank ^ 2, rank ^ 3])
        rel = jnp.stack([blocks, 2 * groups - 1 - blocks], axis=1).reshape(2 * groups)
        cos_t, sin_t = rope_tables(rel * piece, piece, long_factor)
        small = (ln_w, ln_b, b_q, b_o, b_k, b_v)
        y, dx, mine, theirs, d_wo, vec = mega(
            x_in.reshape(2, piece, width), dy_out.reshape(2, piece, width), w_q, w_k, w_v, w_o,
            small, cos_t, sin_t, nh, hd, hd ** -0.5)
        y, dx, d_wq, d_wk, d_wv, d_wo, d_lnw, d_lnb, d_bo, d_bq, d_bk, d_bv = finish(
            (rank % 2)[None], y.reshape(tokens, width), dx.reshape(tokens, width), mine, theirs, d_wo, vec, hd, kvw)
        shape = (1, tokens, width)
        return (y.reshape(shape), dx.reshape(shape), d_wq, d_wk, d_wv, d_wo, d_lnw, d_lnb, d_bq, d_bk, d_bv, d_bo)

    in_specs = (row_spec,) + (P(),) * 11 + (row_spec,)
    out_specs = (row_spec, row_spec) + (mat_spec,) * 4 + (vec_spec,) * 6
    return jax.shard_map(device_fn, mesh=mesh, in_specs=in_specs, out_specs=out_specs, check_vma=False)
```

```python
import functools
import math
import jax
import jax.numpy as jnp
from jax import lax
from jax.experimental import pallas as pl
from jax.experimental.pallas import tpu as pltpu
from jax.sharding import PartitionSpec as P

EPS = 1e-5
THETA = 10000.0
ROPE_SCALE = math.sqrt(1.0 + math.log(32.0) / math.log(4096.0))
LOG2E = math.log2(math.e)
NEG = -1e30
F32 = jnp.float32
BF16 = jnp.bfloat16


def dot(a, b):
    return lax.dot_general(a, b, (((1,), (0,)), ((), ())), preferred_element_type=F32)


def dot_nt(a, b):
    return lax.dot_general(a, b, (((1,), (1,)), ((), ())), preferred_element_type=F32)


def dot_tn(a, b):
    return lax.dot_general(a, b, (((0,), (0,)), ((), ())), preferred_element_type=F32)


def rope_tables(starts, piece, long_factor):
    half_dim = long_factor.shape[0]
    exponent = jnp.arange(half_dim, dtype=F32) * (1.0 / half_dim)
    inv_freq = jnp.tile(1.0 / (long_factor * THETA ** exponent), 2)
    sign = jnp.where(jnp.arange(2 * half_dim) < half_dim, -1.0, 1.0)
    positions = jnp.concatenate([jnp.arange(piece, dtype=jnp.int32), starts])
    angle = positions.astype(F32)[:, None] * inv_freq[None, :]
    return jnp.cos(angle), jnp.sin(angle) * sign[None, :]


def tile_tables(cos_ref, sin_ref, piece, t):
    ca = cos_ref[pl.ds(piece + t, 1), :] * ROPE_SCALE
    sa = sin_ref[pl.ds(piece + t, 1), :] * ROPE_SCALE
    cb = cos_ref[:piece, :]
    sb = sin_ref[:piece, :]
    return ca * cb - sa * sb, sa * cb + ca * sb


MESH = pl.DeviceIdType.MESH


def mega_body(nh, hd, tile, scale,
              x_hbm, d_hbm, wq_hbm, wk_hbm, wv_hbm, wo_hbm, lnw1, lnb1, bq1, bo1, bk1, bv1, cos_ref, sin_ref,
              y_hbm, dx_hbm, dwm_hbm, DWR, dwo_hbm, vec_ref,
              H, D, KV, KT, VT, WQ, WO, WKV, DK, DV, AT, SEND, DWT, ONA, ONS, ONR, DQA, DQS, DQR, DKA, DKS, DKR,
              VS, VR, SM, fs, fr, ns, nr, ls):
    rank = lax.axis_index('cp')
    core = rank % 2
    chip = rank // 2
    near = rank + 1 - 2 * core
    far = rank + 2 - 4 * chip
    tq = nh * tile
    qw = nh * hd
    width = H.shape[2]
    part = width // 4
    third = nh // 2
    lnw, lnb, bq, bo, bk, bv = (SM.at[n:n + 1, :] for n in range(6))
    for n, r in enumerate((lnw1, lnb1, bq1, bo1, bk1, bv1)):
        SM[n:n + 1, :r.shape[0]] = r[...].astype(F32).reshape(1, r.shape[0])

    def local(src, dst, n):
        return pltpu.make_async_copy(src, dst, ls.at[n])

    def remote(src, dst, send, recv, n, to):
        return pltpu.make_async_remote_copy(src_ref=src, dst_ref=dst, send_sem=send.at[n], recv_sem=recv.at[n],
                                            device_id={'cp': to}, device_id_type=MESH)

    def lanes_of(i, n):
        return pl.ds(pl.multiple_of(i * n, 128), n)

    def piece_of(t):
        k = t // 2
        b = (rank % 2 + k % 2) % 2 + 2 * ((rank // 2 + k // 2) % 2)
        return b + (t % 2) * (7 - 2 * b)

    def tile_of(p):
        up = p // 4
        b = p + up * (7 - 2 * p)
        k = (rank % 2 + b % 2) % 2 + 2 * ((rank // 2 + b // 2) % 2)
        return 2 * k + up

    def start_loads(X):
        mine = lanes_of(core, hd)
        return [local(x_hbm, X, 0), local(wk_hbm.at[:, mine], WKV.at[:, :hd], 1), local(wv_hbm.at[:, mine], WKV.at[:, hd:], 2),
                local(d_hbm, D.at[0:2], 3), local(wq_hbm.at[:, lanes_of(core, qw)], WQ, 4),
                local(wo_hbm.at[lanes_of(core, qw), :], WO, 5)]

    n_h = remote(H.at[0:2], H.at[2:4], ns, nr, 0, near)
    n_d = remote(D.at[0:2], D.at[2:4], ns, nr, 1, near)
    f_kv = remote(KV.at[0:2], KV.at[4:6], fs, fr, 0, far)
    f_kw = remote(KV.at[2:4], KV.at[6:8], fs, fr, 6, far)
    f_h1 = remote(H.at[1], H.at[5], fs, fr, 1, far)
    f_d1 = remote(D.at[1, :tile // 4], D.at[5, :tile // 4], fs, fr, 2, far)
    f_e1 = remote(D.at[1, tile // 4:], D.at[5, tile // 4:], fs, fr, 7, far)
    f_h0 = remote(H.at[0], H.at[4], fs, fr, 3, far)
    f_d0 = remote(D.at[0], D.at[4], fs, fr, 4, far)
    n_h5 = remote(H.at[5], H.at[7], ns, nr, 2, near)
    n_d5 = remote(D.at[5], D.at[7], ns, nr, 3, near)
    n_h4 = remote(H.at[4], H.at[6], ns, nr, 4, near)
    n_d4 = remote(D.at[4], D.at[6], ns, nr, 5, near)
    n_o = remote(ONS, ONR, ns, nr, 6, near)
    n_q = remote(DQS, DQR, ns, nr, 7, near)
    n_k = remote(DKS, DKR, ns, nr, 8, near)
    n_v = remote(VS.at[0], VR.at[0], ns, nr, 10, near)
    f_v = remote(VS.at[1], VR.at[1], fs, fr, 5, far)

    def swapped(t):
        return t + 2 - 4 * ((t // 2) % 2)

    holds = core == chip

    def n_s(t, s):
        return remote(SEND.at[s % 2], AT.at[swapped(t)], ns, nr, 11 + t, near)

    def n_s_in(t):
        return remote(SEND.at[0], AT.at[t], ns, nr, 11 + swapped(t), near)

    def tile_at(s):
        late = s // 4
        u = s % 4
        return (1 - late) * ((u + 2) % 4) + late * (4 + (u % 2) * 2 + 1 - u // 2)

    def head_phase(X):
        loads = start_loads(X)
        for c in loads:
            c.start()
        barrier = pltpu.get_barrier_semaphore()
        for to in (near, far):
            pl.semaphore_signal(barrier, inc=1, device_id={'cp': to}, device_id_type=MESH)
        pl.semaphore_wait(barrier, 2)
        loads[3].wait()
        f_d1.start()
        loads[0].wait()
        gain = lnw[...]
        shift = lnb[...]

        def norm(r, _):
            rows = pl.ds(pl.multiple_of((r % 4) * 64, 64), 64)
            x = X[r // 4, rows, :].astype(F32)
            cen = x - jnp.mean(x, axis=-1, keepdims=True)
            inv = lax.rsqrt(jnp.mean(cen * cen, axis=-1, keepdims=True) + EPS)
            H[r // 4, rows, :] = (cen * inv * gain + shift).astype(BF16)
            return _

        lax.fori_loop(0, 8, norm, 0)
        n_h.start()
        n_d.start()
        loads[1].wait()
        loads[2].wait()
        loads[4].wait()
        loads[5].wait()

    pl.run_scoped(head_phase, pltpu.VMEM((2, tile, width), BF16))

    def attention_phase(Q, DO, PS, DPS, MS, PB, DSB, OT, DQT, DQTT):
        c = scale * LOG2E

        def rope(t, ct, st):
            t = t.astype(BF16).astype(F32)
            return (t * ct + pltpu.roll(t, hd // 2, 1) * st).astype(BF16)

        def kv_tile(t, _):
            ct, st = tile_tables(cos_ref, sin_ref, tile, t)
            kv = dot(H[t], WKV[...])
            KV[t, :, :hd] = rope(kv[:, :hd] + bk[0:1, lanes_of(core, hd)], ct, st)
            KV[t, :, hd:] = (kv[:, hd:] + bv[0:1, lanes_of(core, hd)]).astype(BF16)
            return _

        def project(t, slot):
            ct, st = tile_tables(cos_ref, sin_ref, tile, t)
            q = dot(H[t], WQ[...]) + bq[0:1, lanes_of(core, qw)]
            for n in range(nh):
                Q[slot, n] = rope(q[:, n * hd:(n + 1) * hd], ct, st)
            r = dot_nt(D[t], WO[...]).astype(BF16)
            for n in range(nh):
                DO[slot, n] = r[:, n * hd:(n + 1) * hd]

        def turn(t, _):
            KT[t] = KV[t, :, :hd].T
            VT[t] = KV[t, :, hd:].T
            return _

        lax.fori_loop(0, 2, kv_tile, 0)
        f_kv.start()
        n_h.wait_recv()
        lax.fori_loop(2, 4, kv_tile, 0)
        f_kw.start()
        f_h1.start()
        f_e1.start()
        f_h0.start()
        f_d0.start()

        def first_four(t, _):
            project(t, t)
            return _

        lax.fori_loop(0, 2, first_four, 0)
        n_d.wait_recv()
        lax.fori_loop(2, 4, first_four, 0)
        lax.fori_loop(0, 4, turn, 0)
        DK[...] = jnp.zeros_like(DK)
        DV[...] = jnp.zeros_like(DV)
        DWT[...] = jnp.zeros_like(DWT)
        f_kv.wait_recv()
        lax.fori_loop(4, 6, turn, 0)
        f_kw.wait_recv()
        lax.fori_loop(6, 8, turn, 0)

        def one_tile(s, same):
            late = s // 4
            u = s % 4
            t = tile_at(s)
            slot = (1 - late) * t + late * u

            @pl.when(s == 4)
            def _():
                f_h1.wait_recv()
                f_d1.wait_recv()
                f_e1.wait_recv()
                n_h5.start()
                n_d5.start()

            @pl.when(s == 5)
            def _():
                n_h5.wait_recv()
                n_d5.wait_recv()

            @pl.when(s == 6)
            def _():
                f_h0.wait_recv()
                f_d0.wait_recv()
                n_h4.start()
                n_d4.start()

            @pl.when(s == 7)
            def _():
                n_h4.wait_recv()
                n_d4.wait_recv()

            @pl.when(late == 1)
            def _():
                project(t, slot)

            i = piece_of(t)

            def first(j, carry, diag):
                m, l, dl = carry
                g = tile_of(j)
                kj = KV[g, :, :hd]
                vj = KV[g, :, hd:]
                m_new, l_new, d_new = [], [], []
                for n in range(nh):
                    lanes = slice(n * tile, (n + 1) * tile)
                    sc = dot_nt(kj, Q[slot, n]) * c
                    if diag:
                        key = lax.broadcasted_iota(jnp.int32, (tile, tile), 0)
                        qry = lax.broadcasted_iota(jnp.int32, (tile, tile), 1)
                        sc = jnp.where(key <= qry, sc, NEG)
                    dpb = dot_nt(vj, DO[slot, n]).astype(BF16)
                    DPS[j, :, lanes] = dpb
                    mo = m[:, lanes]
                    mn = jnp.maximum(mo, jnp.max(sc, axis=0, keepdims=True))
                    p = jnp.exp2(sc - mn)
                    PS[j, :, lanes] = p
                    al = jnp.exp2(mo - mn)
                    m_new.append(mn)
                    l_new.append(l[:, lanes] * al + jnp.sum(p, axis=0, keepdims=True))
                    d_new.append(dl[:, lanes] * al + jnp.sum(p * dpb.astype(F32), axis=0, keepdims=True))
                m = jnp.concatenate(m_new, axis=1)
                MS[j] = m
                return m, jnp.concatenate(l_new, axis=1), jnp.concatenate(d_new, axis=1)

            init = (jnp.full((1, tq), NEG, F32), jnp.zeros((1, tq), F32), jnp.zeros((1, tq), F32))
            carry = lax.fori_loop(0, i // 2, lambda h, cr: first(2 * h + 1, first(2 * h, cr, False), False), init)
            carry = lax.fori_loop(2 * (i // 2), i, lambda j, cr: first(j, cr, False), carry)
            m, l, dl = first(i, carry, True)
            inv = 1.0 / l
            delta = dl * inv
            OT[...] = jnp.zeros_like(OT)
            DQT[...] = jnp.zeros_like(DQT)

            def weigh(j, k):
                f = jnp.exp2(MS[j] - m) * inv
                for n in range(nh):
                    lanes = slice(n * tile, (n + 1) * tile)
                    p = PS[j, :, lanes] * f[:, lanes]
                    PB[k, :, lanes] = p.astype(BF16)
                    DSB[k, :, lanes] = (p * (DPS[j, :, lanes].astype(F32) - delta[:, lanes])).astype(BF16)

            def second(js, carry):
                gs = [tile_of(j) for j in js]
                for k, j in enumerate(js):
                    weigh(j, k)
                o = dot(VT[gs[0]], PB[0])
                dq = dot(KT[gs[0]], DSB[0])
                for k in range(1, len(js)):
                    o += dot(VT[gs[k]], PB[k])
                    dq += dot(KT[gs[k]], DSB[k])
                OT[...] += o
                DQT[...] += dq
                for k, g in enumerate(gs):
                    DV[g] += dot(PB[k], DO[slot].reshape(tq, hd))
                    DK[g] += dot(DSB[k], Q[slot].reshape(tq, hd))
                return carry

            pairs = (i + 1) // 2
            lax.fori_loop(0, pairs, lambda h, cr: second((2 * h, 2 * h + 1), cr), 0)
            lax.fori_loop(2 * pairs, i + 1, lambda j, cr: second((j,), cr), 0)
            ct, st = tile_tables(cos_ref, sin_ref, tile, t)
            cos_t = ct.T[:hd // 2]

            @pl.when(jnp.logical_and(holds, s >= 2))
            def _():
                n_s(tile_at(s - 2), s).wait_send()

            sin_t = st.T[hd // 2:]
            for n in range(nh):
                lanes = slice(n * tile, (n + 1) * tile)
                gr = (DQT[:, lanes] * scale).astype(BF16).astype(F32)
                a = gr[:hd // 2]
                e = gr[hd // 2:]
                gr = jnp.concatenate([a * cos_t + e * sin_t, e * cos_t - a * sin_t], axis=0).astype(BF16)
                DQTT[s % 2, n * hd:(n + 1) * hd, :] = gr

            for h in range(2):
                @pl.when(jnp.logical_and(holds, core == h))
                def _():
                    for n in range(nh):
                        o_t = OT[:, n * tile:(n + 1) * tile].astype(BF16)
                        rows = slice((n % third) * hd, (n % third + 1) * hd)
                        if n // third == h:
                            AT[t, rows, :] = o_t
                        else:
                            SEND[s % 2, rows, :] = o_t

            for h, (o_out, q_out) in enumerate(((ONA, DQA), (ONS, DQS))):
                @pl.when(t // 2 == h)
                def _():
                    for n in range(nh):
                        cols = slice(n * hd, (n + 1) * hd)
                        o_out[t % 2, :, cols] = OT[:, n * tile:(n + 1) * tile].astype(BF16).T
                        q_out[t % 2, :, cols] = DQTT[s % 2, cols, :].T

            @pl.when(holds)
            def _():
                n_s(t, s).start()

            @pl.when(s == 1)
            def _():
                n_o.start()
                n_q.start()

            @pl.when(s % 2 == 1)
            def _():
                cols = lanes_of(chip, 2 * part)
                DWT[...] += dot(DQTT[0], H[tile_at(s - 1), :, cols]) + dot(DQTT[1], H[t, :, cols])

            return same

        lax.fori_loop(0, 8, one_tile, 0)

    pl.run_scoped(attention_phase,
                  pltpu.VMEM((4, nh, tile, hd), BF16), pltpu.VMEM((4, nh, tile, hd), BF16),
                  pltpu.VMEM((8, tile, tq), F32), pltpu.VMEM((8, tile, tq), BF16), pltpu.VMEM((8, 1, tq), F32),
                  pltpu.VMEM((2, tile, tq), BF16), pltpu.VMEM((2, tile, tq), BF16), pltpu.VMEM((hd, tq), F32), pltpu.VMEM((hd, tq), F32),
                  pltpu.VMEM((2, qw, tile), BF16))

    def tail_phase(DWS, X, WQO, WOO, WKVO, DKVT, DWK, DWM, ACC, OUT, YB, XB):
        n_w = remote(DWS, DWR, ns, nr, 9, near)
        other = lanes_of(1 - core, hd)
        loads = [local(wq_hbm.at[:, lanes_of(1 - core, qw)], WQO, 0), local(wk_hbm.at[:, other], WKVO.at[:, :hd], 1),
                 local(wv_hbm.at[:, other], WKVO.at[:, hd:], 2), local(x_hbm, X, 3),
                 local(wo_hbm.at[lanes_of(1 - core, qw), :], WOO, 4)]
        for cp in loads:
            cp.start()

        def finish(t, same):
            ct, st = tile_tables(cos_ref, sin_ref, tile, t)
            g = (DK[t] * scale).astype(BF16).astype(F32)
            gk = (g * ct - pltpu.roll(g, hd // 2, 1) * st).astype(BF16)
            gv = DV[t].astype(BF16)
            DKVT[t, :hd, :] = gk.T
            DKVT[t, hd:, :] = gv.T

            @pl.when(t // 2 == 0)
            def _():
                DKA[t % 2, :, :hd] = gk
                DKA[t % 2, :, hd:] = gv

            @pl.when(t // 2 == 1)
            def _():
                DKS[t % 2, :, :hd] = gk
                DKS[t % 2, :, hd:] = gv

            return same

        lax.fori_loop(0, 4, finish, 0)
        n_k.start()
        lax.fori_loop(4, 8, finish, 0)

        chip_cols = lanes_of(chip, 2 * part)
        acc = dot(DKVT[0], H[0, :, chip_cols])
        for t in range(1, 8):
            acc += dot(DKVT[t], H[t, :, chip_cols])
        DWK[...] = acc
        theirs = lanes_of(1 - core, part)
        mine = lanes_of(core, part)
        for cp in loads[:4]:
            cp.wait()
        n_q.wait_recv()
        n_k.wait_recv()
        for t in range(2):
            ACC[t * tile:(t + 1) * tile, :] = (dot_nt(DQA[t], WQ[...]) + dot_nt(DQR[t], WQO[...])
                                               + dot_nt(DKA[t], WKV[...]) + dot_nt(DKR[t], WKVO[...]))
        for cols_of, out in ((theirs, DWS), (mine, DWM)):
            for n in range(qw // tile):
                cols = slice(n * tile, (n + 1) * tile)
                out[:, cols] = DWT[cols, cols_of].T
            out[:, qw:] = DWK[:, cols_of].T
        n_w.start()
        outs = [local(DWM, dwm_hbm, 5)]
        outs[0].start()

        @pl.when(jnp.logical_not(holds))
        def _():
            for t in range(8):
                n_s_in(t).wait_recv()

        def rowsum(v):
            return jnp.sum(v, axis=0, keepdims=True)

        VS[0] = jnp.zeros_like(VS[0])
        gain = lnw[...]
        chunk = tile // 2
        tn = width // 4

        def back(r, same):
            lanes = lanes_of(r, tn)
            acc = dot(AT[0], D[0, :, lanes])
            for t in range(1, 8):
                acc += dot(AT[t], D[t, :, lanes])
            OUT[:, lanes] = acc
            rows = pl.ds(pl.multiple_of((r % 2) * chunk, chunk), chunk)
            dh = ACC[pl.ds(pl.multiple_of(r * chunk, chunk), chunk), :].astype(BF16).astype(F32)
            x = X[r // 2, rows, :].astype(F32)
            cen = x - jnp.mean(x, axis=-1, keepdims=True)
            inv = lax.rsqrt(jnp.mean(cen * cen, axis=-1, keepdims=True) + EPS)
            xh = cen * inv
            a = dh * gain
            d = D[r // 2, rows, :].astype(F32)
            dx = inv * (a - jnp.mean(a, axis=-1, keepdims=True) - xh * jnp.mean(a * xh, axis=-1, keepdims=True))
            XB[r // 2, rows, :] = (d + dx).astype(BF16)
            VS[0, 0:1, :] += rowsum(dh * xh)
            VS[0, 1:2, :] += rowsum(dh)
            VS[0, 2:3, :] += rowsum(d)
            return same

        lax.fori_loop(0, 4, back, 0)
        for side, q, k in ((core, DQA, DKA), (1 - core, DQR, DKR)):
            qs = rowsum(q[0].astype(F32)) + rowsum(q[1].astype(F32))
            ks = rowsum(k[0].astype(F32)) + rowsum(k[1].astype(F32))
            VS[0, 3:4, lanes_of(side, qw)] = qs
            VS[0, 4:5, lanes_of(side, hd)] = ks[:, :hd]
            VS[0, 5:6, lanes_of(side, hd)] = ks[:, hd:]
        n_v.start()
        outs += [local(XB, dx_hbm, 8), local(OUT, dwo_hbm, 10)]
        outs[1].start()
        outs[2].start()

        loads[4].wait()
        n_o.wait_recv()

        def y_tile(t):
            z = dot(ONA[t], WO[...]) + dot(ONR[t], WOO[...])
            YB[t] = (X[t].astype(F32) + (z + bo[...])).astype(BF16)

        y_tile(0)
        n_v.wait_recv()
        VS[1] = VS[0] + VR[0]
        f_v.start()
        y_tile(1)
        outs.append(local(YB, y_hbm, 9))
        outs[-1].start()
        n_w.wait_recv()
        f_v.wait_recv()
        vec_ref[...] = VS[1] + VR[1]
        for cp in outs:
            cp.wait()
        n_w.wait_send()

    pl.run_scoped(tail_phase,
                  pltpu.VMEM((part, qw + 2 * hd), F32), pltpu.VMEM((2, tile, width), BF16), pltpu.VMEM((width, qw), BF16), pltpu.VMEM((qw, width), BF16),
                  pltpu.VMEM((width, 2 * hd), BF16), pltpu.VMEM((8, 2 * hd, tile), BF16), pltpu.VMEM((2 * hd, 2 * part), F32),
                  pltpu.VMEM((part, qw + 2 * hd), F32), pltpu.VMEM((2 * tile, width), F32),
                  pltpu.VMEM((part, width), F32), pltpu.VMEM((2, tile, width), BF16), pltpu.VMEM((2, tile, width), BF16))

    for cp in (n_h, n_d, f_kv, f_kw, f_h1, f_d1, f_e1, f_h0, f_d0, n_h5, n_d5, n_h4, n_d4, n_o, n_q, n_k, n_v, f_v):
        cp.wait_send()

    @pl.when(holds)
    def _():
        for s in (6, 7):
            n_s(tile_at(s), s).wait_send()


def mega(x, d, wq, wk, wv, wo, small, cos_t, sin_t, nh, hd, scale):
    _, tile, width = x.shape
    qw = nh * hd
    part = width // 4
    anywhere = pl.BlockSpec(memory_space=pltpu.HBM)
    vmem = pl.BlockSpec(memory_space=pltpu.VMEM)
    rows = (2, tile, width)

    def vm(*shape, dtype=BF16):
        return pltpu.VMEM(shape, dtype)

    return pl.pallas_call(
        functools.partial(mega_body, nh, hd, tile, scale),
        in_specs=[anywhere] * 6 + [vmem] * 8,
        out_specs=[anywhere] * 5 + [vmem],
        out_shape=[jax.ShapeDtypeStruct(rows, BF16), jax.ShapeDtypeStruct(rows, BF16),
                   jax.ShapeDtypeStruct((part, qw + 2 * hd), F32), jax.ShapeDtypeStruct((part, qw + 2 * hd), F32),
                   jax.ShapeDtypeStruct((part, width), F32),
                   jax.ShapeDtypeStruct((8, width), F32)],
        scratch_shapes=[
            vm(8, tile, width), vm(8, tile, width), vm(8, tile, 2 * hd), vm(8, hd, tile), vm(8, hd, tile),
            vm(width, qw), vm(qw, width), vm(width, 2 * hd),
            vm(8, tile, hd, dtype=F32), vm(8, tile, hd, dtype=F32),
            vm(8, part, tile), vm(2, part, tile), vm(qw, 2 * part, dtype=F32),
            vm(2, tile, qw), vm(2, tile, qw), vm(2, tile, qw), vm(2, tile, qw), vm(2, tile, qw), vm(2, tile, qw),
            vm(2, tile, 2 * hd), vm(2, tile, 2 * hd), vm(2, tile, 2 * hd),
            vm(2, 8, width, dtype=F32), vm(2, 8, width, dtype=F32), vm(8, width, dtype=F32),
            pltpu.SemaphoreType.DMA((8,)), pltpu.SemaphoreType.DMA((8,)),
            pltpu.SemaphoreType.DMA((19,)), pltpu.SemaphoreType.DMA((19,)), pltpu.SemaphoreType.DMA((14,))],
        compiler_params=pltpu.CompilerParams(collective_id=0, has_side_effects=True, vmem_limit_bytes=67043328),
        name="sublayer",
    )(x, d, wq, wk, wv, wo, *small, cos_t, sin_t)


def finish_body(hd, c_ref, y_ref, dx_ref, m_ref, t_ref, o_ref, v_ref, y_out, dx_out, q_out, k_out, v_out, o_out, *vecs):
    core = c_ref[0]
    y_out[...] = y_ref[...]
    dx_out[...] = dx_ref[...]
    o_out[...] = o_ref[...]
    qw = q_out.shape[1] // 2
    for side, r in ((core, m_ref), (1 - core, t_ref)):
        q_out[:, pl.ds(pl.multiple_of(side * qw, 128), qw)] = r[:, :qw]
        k_out[:, pl.ds(pl.multiple_of(side * hd, 128), hd)] = r[:, qw:qw + hd]
        v_out[:, pl.ds(pl.multiple_of(side * hd, 128), hd)] = r[:, qw + hd:]

    @pl.when(pl.program_id(0) == 0)
    def _():
        for n, r in enumerate(vecs):
            r[...] = v_ref[n:n + 1, :r.shape[0]].reshape(r.shape[0])


def finish(core, y, dx, mine, theirs, d_wo, vec, hd, kvw, steps=2):
    rows, width = y.shape
    part, cols = mine.shape
    qw = cols - 2 * hd

    def tall(r, c):
        return pl.BlockSpec((r // steps, c), lambda i, s: (i, 0))

    dims = [(rows, width), (rows, width), (part, 2 * qw), (part, 2 * hd), (part, 2 * hd), (part, width)]
    lens = [width] * 4 + [kvw] * 2
    return pl.pallas_call(
        functools.partial(finish_body, hd),
        grid_spec=pltpu.PrefetchScalarGridSpec(
            num_scalar_prefetch=1, grid=(steps,),
            in_specs=[tall(rows, width), tall(rows, width), tall(part, cols), tall(part, cols), tall(part, width),
                      pl.BlockSpec(vec.shape, lambda i, s: (0, 0))],
            out_specs=[tall(*d) for d in dims] + [pl.BlockSpec((n,), lambda i, s: (0,)) for n in lens]),
        out_shape=[jax.ShapeDtypeStruct(d, BF16 if n < 2 else F32) for n, d in enumerate(dims)]
        + [jax.ShapeDtypeStruct((n,), F32) for n in lens],
        compiler_params=pltpu.CompilerParams(dimension_semantics=("arbitrary",), vmem_limit_bytes=67043328),
        name="finish",
    )(core, y, dx, mine, theirs, d_wo, vec)


def solution(mesh):
    groups = mesh.shape['cp']
    row_spec = P('dp', 'cp', None)
    mat_spec = P(('dp', 'cp'), None)
    vec_spec = P('dp')

    def device_fn(x_in, ln_w, ln_b, w_q, b_q, w_k, b_k, w_v, b_v, w_o, b_o, long_factor, dy_out):
        rank = lax.axis_index('cp').astype(jnp.int32)
        tokens, width = x_in.shape[1:]
        piece = tokens // 2
        hd = 2 * long_factor.shape[0]
        kvw = w_k.shape[1]
        nh = w_q.shape[1] // kvw
        blocks = jnp.stack([rank, rank ^ 1, rank ^ 2, rank ^ 3])
        rel = jnp.stack([blocks, 2 * groups - 1 - blocks], axis=1).reshape(2 * groups)
        cos_t, sin_t = rope_tables(rel * piece, piece, long_factor)
        small = (ln_w, ln_b, b_q, b_o, b_k, b_v)
        y, dx, mine, theirs, d_wo, vec = mega(
            x_in.reshape(2, piece, width), dy_out.reshape(2, piece, width), w_q, w_k, w_v, w_o,
            small, cos_t, sin_t, nh, hd, hd ** -0.5)
        y, dx, d_wq, d_wk, d_wv, d_wo, d_lnw, d_lnb, d_bo, d_bq, d_bk, d_bv = finish(
            (rank % 2)[None], y.reshape(tokens, width), dx.reshape(tokens, width), mine, theirs, d_wo, vec, hd, kvw)
        shape = (1, tokens, width)
        return (y.reshape(shape), dx.reshape(shape), d_wq, d_wk, d_wv, d_wo, d_lnw, d_lnb, d_bq, d_bk, d_bv, d_bo)

    in_specs = (row_spec,) + (P(),) * 11 + (row_spec,)
    out_specs = (row_spec, row_spec) + (mat_spec,) * 4 + (vec_spec,) * 6
    return jax.shard_map(device_fn, mesh=mesh, in_specs=in_specs, out_specs=out_specs, check_vma=False)
```
